32 devices in a mesh: dp: 8 (over y, x, core), expert: 4 (over z).
Axes of the slice: x: 2, y: 2, z: 4, core: 2. Of those that a mesh axis runs over, the one named last changes fastest.
Arguments:
- tokens: bfloat16 [4096, 2048], P(('dp', 'expert')), may hold values from -6 to 6
- out_grad: bfloat16 [4096, 2048], P(('dp', 'expert')), may hold values from -6 to 6
- gate_prob: float32 [4096, 1], P(('dp', 'expert')), may hold values from 0.2 to 1
- routing: int32 [4096, 1], P(('dp', 'expert')), may hold values from 0 to 3; in each aligned block of 128 rows (0 to 127, 128 to 255, ...) at most 64 rows name the same one
- expert_weights: bfloat16 [4, 2048, 1152], P('expert'), may hold values from -0.125 to 0.125
Outputs:
- input_grad: bfloat16 [4096, 2048], P(('dp', 'expert'))
- weight_grad: float32 [4, 2048, 1152], P('expert', 'dp')
The draws below stay inside these ranges and needn't reach their ends.
Inputs may be any that keep to these rules, and one draw needn't show every extreme that they name: `routing`: among the tokens of one device at most 64 go to any one expert; in some devices' tokens an expert gets exactly 64.
All inputs are finite; a program needn't handle non-finite values.
Results may differ from the reference program's by a relative error of at most 0.014.
Values may be sent and summed in bfloat16 or wider, within the bound.
A program may use at most 64 MiB of HBM per device.

```python
import math
from functools import partial
import jax
import jax.numpy as jnp
import numpy as np
from jax import lax

D = 2048
FF = 384
TOK_DEV = 128
TOKENS = 4096
EXPERTS_TURN = 4
CAP = 64
GROUP_ROWS = 1024
N_DP = 8
N_EXPERT = 4


def block_levels(key, shape, shards, smallest, high):
    level, own = 1.0, jax.random.fold_in(key, 6)
    for axis_at, shards_of in shards:
        heights = jnp.exp(jax.random.uniform(jax.random.fold_in(own, axis_at), (shards_of,), jnp.float32, smallest / len(shards), high / len(shards)))
        level = level * jnp.repeat(heights, shape[axis_at] // shards_of).reshape([-1 if axis == axis_at else 1 for axis in range(len(shape))])
    return level


def shared_out(stream_key, own, number, rows, number_of, top, most, slope):
    order = jax.random.permutation(stream_key, number_of)
    heavy_load, common = shares(number_of, rows * top, most, slope, True), shares(number_of, rows * top, most, slope, False)
    places = jnp.arange(number_of)

    def named(sizes, rotation):
        used = int((sizes > 0).sum())
        fixed = max(1, used // 4)
        moved = fixed + (places - fixed + rotation * (used - fixed)) % max(1, number_of - fixed)
        return jnp.zeros((number_of,), jnp.int32).at[order[jnp.where(places < fixed, places, moved)]].set(jnp.asarray(sizes, jnp.int32))

    sizes = jnp.where(number % 4 == 0, named(heavy_load, number // 4), named(common, number - number // 4 - 1))
    mixed = jax.random.permutation(jax.random.fold_in(own, 3), number_of)
    giver, receiver = mixed[0:number_of // 2 * 2:2], mixed[1:number_of // 2 * 2:2]
    slack = jnp.minimum(sizes[giver] - 1, most - sizes[receiver]) // 2
    slack = jnp.where((giver == order[0]) | (receiver == order[0]) | (sizes[receiver] == 0), 0, jnp.maximum(slack, 0))
    moved = jax.random.randint(jax.random.fold_in(own, 4), (number_of // 2,), 0, 1 << 20) % (slack + 1)
    sizes = sizes.at[giver].add(-moved).at[receiver].add(moved)
    labels = jnp.searchsorted(jnp.cumsum(sizes), jnp.arange(rows * top), side="right").astype(jnp.int32)
    grid = labels.reshape(top, rows).T
    grid = grid[jax.random.permutation(jax.random.fold_in(own, 1), rows)]
    rotation = jax.random.randint(jax.random.fold_in(own, 2), (rows, 1), 0, top)
    return jnp.take_along_axis(grid, (jnp.arange(top)[None, :] + rotation) % top, axis=1)


def shares(number_of, total, reach, slope, full):
    loads = [(1 << 20) // math.isqrt(standing ** slope) + 1 for standing in range(1, number_of + 1)]
    largest = reach if full else min(reach, max(-(-total // number_of), total * loads[0] // sum(loads)))
    least = 1 if total - largest >= number_of - 1 else 0
    counts, rest = [largest] + [least] * (number_of - 1), total - largest - least * (number_of - 1)
    while rest > 0:
        candidates = [i for i in range(1, number_of) if counts[i] < largest] or [i for i in range(1, number_of) if counts[i] < reach]
        whole, left = sum([loads[i] for i in candidates]), rest
        for i in candidates:
            more = min(reach - counts[i], max(1, left * loads[i] // whole), rest)
            counts[i] = counts[i] + more
            rest = rest - more
    return np.array(counts)


def noise(rng, extent, width, reach, pieces=(), kind=jnp.bfloat16):
    drawn = jax.random.normal(rng, extent, jnp.float32) * width
    if len(pieces) > 0:
        drawn = block_levels(rng, extent, pieces, -0.22, 0.18) * drawn
    return jnp.clip(drawn, min=-reach, max=reach).astype(kind)


def setup_inputs(seed: int = 0) -> dict:
    streams_of = jax.random.split(jax.random.key(seed), 6)
    tokens = noise(streams_of[0], (TOKENS, D), 1.0, 6.0, ((0, 32),))
    out_grad = noise(streams_of[1], (TOKENS, D), 1.0, 6.0, ((0, 32),))
    gate_prob = jnp.clip(0.2 + 0.8 * jax.random.uniform(streams_of[2], (TOKENS, 1), jnp.float32) ** block_levels(streams_of[2], (TOKENS, 1), ((0, 32),), -0.2, 0.2), 0.2, 1.0)
    routing_keys = jax.random.split(jax.random.fold_in(streams_of[3], 1), TOKENS // TOK_DEV)
    routing_turns = jax.random.permutation(jax.random.fold_in(streams_of[3], 3), TOKENS // TOK_DEV)
    routing = jax.vmap(lambda own, number: shared_out(jax.random.fold_in(streams_of[3], 2), own, number, TOK_DEV, N_EXPERT, 1, CAP, 2))(routing_keys, routing_turns).reshape((TOKENS, 1))
    expert_weights = noise(streams_of[4], (EXPERTS_TURN, D, 3 * FF), D ** -0.5, 0.125, ((0, 4),))
    return {"tokens": tokens, "out_grad": out_grad, "gate_prob": gate_prob, "routing": routing, "expert_weights": expert_weights}


def slot_of(route_block, capacity, experts):
    onehot = (route_block[:, None] == jnp.arange(experts, dtype=jnp.int32)[None, :]).astype(jnp.int32)
    before = jnp.cumsum(onehot, axis=0) - onehot
    position = jnp.sum(before * onehot, axis=1).astype(jnp.int32)
    return (route_block * capacity + position).astype(jnp.int32)


def expert_rows(weights, rows_in, grad_in):
    hidden_width = weights.shape[1] // 3
    pair_weights = weights[:, :2 * hidden_width]
    down_weights = weights[:, 2 * hidden_width:]
    pre_act = jnp.dot(rows_in, pair_weights, preferred_element_type=jnp.float32)
    pre_gate = pre_act[:, :hidden_width]
    pre_up = pre_act[:, hidden_width:]
    sigmoid_gate = jax.nn.sigmoid(pre_gate)
    active = pre_gate * sigmoid_gate
    hidden = (active * pre_up).astype(jnp.bfloat16)
    grad_hidden = jnp.dot(grad_in, down_weights, preferred_element_type=jnp.float32)
    grad_gate = grad_hidden * pre_up * (sigmoid_gate * (1.0 + pre_gate * (1.0 - sigmoid_gate)))
    grad_up = grad_hidden * active
    grad_pair = jnp.concatenate([grad_gate.astype(jnp.bfloat16), grad_up.astype(jnp.bfloat16)], axis=1)
    returned = lax.dot_general(grad_pair, pair_weights, (((1,), (1,)), ((), ())), preferred_element_type=jnp.float32)
    return returned.astype(jnp.bfloat16), hidden, grad_pair


def weight_term(rows_in, grad_in, hidden, grad_pair, grad_scale):
    contract = (((0,), (0,)), ((), ()))
    first_part = lax.dot_general(rows_in, grad_pair, contract, preferred_element_type=jnp.float32)
    second = lax.dot_general(grad_in, hidden, contract, preferred_element_type=jnp.float32)
    return grad_scale * jnp.concatenate([first_part, second], axis=1)


def reference(tokens, out_grad, gate_prob, routing, expert_weights):
    model_width = tokens.shape[1]
    grad_scale = float(GROUP_ROWS) ** -0.5
    scaled = (gate_prob * out_grad.astype(jnp.float32)).astype(jnp.bfloat16)
    tok_x = tokens.reshape(N_DP, N_EXPERT, TOK_DEV, model_width)
    tok_g = scaled.reshape(N_DP, N_EXPERT, TOK_DEV, model_width)
    routes = routing.reshape(N_DP, N_EXPERT, TOK_DEV)
    slotter = jax.vmap(partial(slot_of, capacity=CAP, experts=N_EXPERT))

    def one_expert(operands):
        weights, rows_in, grad_in = operands
        returned, hidden, grad_pair = expert_rows(weights, rows_in, grad_in)
        rounded = weight_term(rows_in, grad_in, hidden, grad_pair, grad_scale).astype(jnp.bfloat16)
        rounded = lax.optimization_barrier(rounded)
        return returned, rounded.astype(jnp.float32)

    def replica(running, blocks):
        block_x, block_g, block_r = blocks
        slot_index = slotter(block_r)
        source = jnp.broadcast_to(jnp.arange(N_EXPERT, dtype=jnp.int32)[:, None], slot_index.shape)
        buf_x = jnp.zeros((N_EXPERT, N_EXPERT * CAP, model_width), jnp.bfloat16).at[source, slot_index].set(block_x)
        buf_g = jnp.zeros((N_EXPERT, N_EXPERT * CAP, model_width), jnp.bfloat16).at[source, slot_index].set(block_g)
        buf_x = buf_x.reshape(N_EXPERT, N_EXPERT, CAP, model_width).transpose(1, 0, 2, 3).reshape(N_EXPERT, N_EXPERT * CAP, model_width)
        buf_g = buf_g.reshape(N_EXPERT, N_EXPERT, CAP, model_width).transpose(1, 0, 2, 3).reshape(N_EXPERT, N_EXPERT * CAP, model_width)
        returned, terms = lax.map(one_expert, (expert_weights, buf_x, buf_g))
        returned = returned.reshape(N_EXPERT, N_EXPERT, CAP, model_width).transpose(1, 0, 2, 3).reshape(N_EXPERT, N_EXPERT * CAP, model_width)
        return running + terms, returned[source, slot_index]

    initial = jnp.zeros((N_EXPERT, model_width, expert_weights.shape[2]), jnp.float32)
    totals, input_grads = lax.scan(replica, initial, (tok_x, tok_g, routes))
    return input_grads.reshape(TOKENS, model_width), totals
```

```python
import functools
import math
import jax
import jax.numpy as jnp
from jax import lax
from jax.experimental import pallas as pl
from jax.experimental.pallas import tpu as pltpu
from jax.sharding import PartitionSpec as P

MESH = pl.DeviceIdType.MESH
F32 = jnp.float32
BF16 = jnp.bfloat16
SUBS = 2
PIECES = 4


def xor(value, step):
    total, bit = 0, 1
    result = value
    while bit <= step:
        if step & bit:
            result = result + bit - 2 * bit * (lax.rem(lax.div(value, bit), 2))
        bit *= 2
    return result


def plan(n_expert, n_dp):
    half, quarter = n_expert // 2, n_expert // 4
    near = list(range(1, half))
    across = list(range(n_expert - 1, half + quarter - 1, -1))
    last = list(range(half + quarter - 1, half - 1, -1))
    chips = n_dp // 2
    side = math.isqrt(chips)
    while chips % side:
        side -= 1
    return near, across, last, chips // side, side


def can_exchange(width, n_expert, n_dp):
    return n_expert == 4 and (width // n_dp) % 128 == 0


def body(
    n_expert,
    n_dp,
    cap,
    tokens_ref,
    out_grad_ref,
    gate_ref,
    route_ref,
    w_hbm,
    in_grad_ref,
    w_grad_ref,
    w_ref,
    send_x,
    send_g,
    recv_x,
    recv_g,
    ret,
    arrived,
    pair,
    hidden,
    part,
    recv_a,
    send_b,
    recv_b,
    send_c,
    recv_c,
    w_sem,
    dx_s,
    dx_r,
    dg_s,
    dg_r,
    rt_s,
    rt_r,
    a_s,
    a_r,
    b_s,
    b_r,
    c_s,
    c_r,
    band_x=None,
    band_g=None,
    terms=None,
    bx_s=None,
    bx_r=None,
    bg_s=None,
    bg_r=None,
    tm_s=None,
    tm_r=None,
    fw_s=None,
    fw_r=None,
):
    near, across, last, na, nb = plan(n_expert, n_dp)
    far = across + last
    order = [0] + near + far
    place = {k: p for p, k in enumerate(order)}
    me = lax.axis_index("expert")
    dp = lax.axis_index("dp")
    tok, width = tokens_ref.shape
    hid = w_ref.shape[1] // 3
    slots = n_expert * cap
    quarter_rows = slots // 4
    share = width // n_dp
    sub = share // SUBS
    exchange = can_exchange(width, n_expert, n_dp)
    early_rows = 3 * quarter_rows if exchange else slots
    grad_scale = float(tok * n_dp) ** (-0.5)
    core = lax.rem(dp, 2)
    chip = lax.div(dp, 2)
    pos_hi, pos_lo = lax.div(chip, na), lax.rem(chip, na)
    if na == nb:
        a = jnp.where(core == 0, pos_lo, pos_hi)
        b = jnp.where(core == 0, pos_hi, pos_lo)
    else:
        a, b = pos_lo, pos_hi

    def chip_of(a_at, b_at):
        plain = b_at * na + a_at
        if na == nb:
            return jnp.where(core == 0, plain, a_at * na + b_at)
        return plain

    def dp_of(a_at, b_at):
        return chip_of(a_at, b_at) * 2 + core

    w_copy = pltpu.make_async_copy(w_hbm.at[0], w_ref, w_sem)
    w_copy.start()

    barrier = pltpu.get_barrier_semaphore()
    partner = dp + 1 - 2 * core
    greeted = 0
    for k in near + far:
        pl.semaphore_signal(barrier, inc=1, device_id={"expert": xor(me, k)}, device_id_type=MESH)
        greeted += 1
    if exchange:
        dp_peers = [lax.rem(dp + j, n_dp) for j in range(1, n_dp)]
    else:
        dp_peers = [partner]
        dp_peers += [dp_of(lax.rem(a + s, na), b) for s in range(1, na)]
        dp_peers += [dp_of(a, lax.rem(b + t, nb)) for t in range(1, nb)]
    for peer in dp_peers:
        pl.semaphore_signal(barrier, inc=1, device_id={"dp": peer}, device_id_type=MESH)
        greeted += 1

    row_i = lax.broadcasted_iota(jnp.int32, (tok, tok), 0)
    col_i = lax.broadcasted_iota(jnp.int32, (tok, tok), 1)

    def column(row):
        return jnp.sum(jnp.where(row_i == col_i, row, 0.0), axis=1, keepdims=True)

    offset = jnp.bitwise_xor(route_ref[...], me)
    block = jnp.zeros_like(offset)
    for p, k in enumerate(order):
        block = jnp.where(offset == k, p, block)
    route_row = block.astype(F32)
    route_col = column(route_row)
    same = route_col == route_row
    pos_row = jnp.sum(jnp.where(same & (row_i < col_i), 1.0, 0.0), axis=0, keepdims=True)
    pos_col = jnp.sum(jnp.where(same & (col_i < row_i), 1.0, 0.0), axis=1, keepdims=True)
    slot_row = route_row * cap + pos_row
    slot_col = route_col * cap + pos_col
    slot_at = lax.broadcasted_iota(jnp.int32, (slots, tok), 0).astype(F32)
    table = jnp.where(slot_at == slot_row, 1.0, 0.0).astype(BF16)
    slot_of = lax.broadcasted_iota(jnp.int32, (tok, slots), 1).astype(F32)
    table_t = jnp.where(slot_of == slot_col, 1.0, 0.0).astype(BF16)

    send_x[...] = jnp.dot(table, tokens_ref[...], preferred_element_type=F32).astype(BF16)
    scaled = (column(gate_ref[...]) * out_grad_ref[...].astype(F32)).astype(BF16)
    send_g[...] = jnp.dot(table, scaled, preferred_element_type=F32).astype(BF16)

    def rows_of(k):
        return pl.ds(place[k] * cap, cap)

    pl.semaphore_wait(barrier, greeted)

    def dispatch(k, src, dst, s_sem, r_sem):
        peer = xor(me, k)
        return pltpu.make_async_remote_copy(
            src_ref=src.at[rows_of(k)],
            dst_ref=dst.at[rows_of(k)],
            send_sem=s_sem.at[k],
            recv_sem=r_sem.at[k],
            device_id={"expert": peer},
            device_id_type=MESH,
        )

    x_copies = {k: dispatch(k, send_x, recv_x, dx_s, dx_r) for k in near + far}
    g_copies = {k: dispatch(k, send_g, recv_g, dg_s, dg_r) for k in near + far}
    returns = {k: dispatch(k, ret, arrived, rt_s, rt_r) for k in near + far}
    for k in near + far:
        x_copies[k].start()
        g_copies[k].start()

    recv_x[rows_of(0)] = send_x[rows_of(0)]
    recv_g[rows_of(0)] = send_g[rows_of(0)]
    w_copy.wait()

    def forward(start, size):
        rows = pl.ds(start, size)
        x = recv_x[rows]
        pre_gate = jnp.dot(x, w_ref[:, :hid], preferred_element_type=F32)
        pre_up = jnp.dot(x, w_ref[:, hid : 2 * hid], preferred_element_type=F32)
        grad_hidden = jnp.dot(recv_g[rows], w_ref[:, 2 * hid :], preferred_element_type=F32)
        sig = jax.nn.sigmoid(pre_gate)
        active = pre_gate * sig
        hidden[rows] = (active * pre_up).astype(BF16)
        grad_gate = grad_hidden * pre_up * (sig * (1.0 + pre_gate * (1.0 - sig)))
        pair[rows, :hid] = grad_gate.astype(BF16)
        pair[rows, hid:] = (grad_hidden * active).astype(BF16)

    def backward(start, size):
        rows = pl.ds(start, size)
        tile = min(512, width)

        @pl.loop(0, width // tile)
        def _(j):
            at = pl.ds(pl.multiple_of(j * tile, tile), tile)
            ret[rows, at] = lax.dot_general(
                pair[rows],
                w_ref[at, : 2 * hid],
                (((1,), (1,)), ((), ())),
                preferred_element_type=F32,
            ).astype(BF16)

    near_half = (0, 2 * quarter_rows)
    across_quarter = (2 * quarter_rows, quarter_rows)
    last_quarter = (3 * quarter_rows, quarter_rows)
    late = pl.ds(3 * quarter_rows, quarter_rows)

    def rows_from(index):
        return pl.ds(pl.multiple_of(index * quarter_rows, quarter_rows), quarter_rows)

    def columns_of(index):
        return pl.ds(pl.multiple_of(index * share, share), share)

    def band_copy(j, src, dst, s_sem, r_sem):
        peer = lax.rem(dp + j, n_dp)
        return pltpu.make_async_remote_copy(
            src_ref=src.at[late, columns_of(peer)],
            dst_ref=dst.at[rows_from(dp)],
            send_sem=s_sem.at[j],
            recv_sem=r_sem.at[j],
            device_id={"dp": peer},
            device_id_type=MESH,
        )

    def term_copy(c):
        return pltpu.make_async_remote_copy(
            src_ref=terms.at[rows_from(dp)],
            dst_ref=terms.at[rows_from(dp)],
            send_sem=tm_s.at[c],
            recv_sem=tm_r.at[c],
            device_id={"dp": lax.rem(chip + c, n_dp // 2) * 2 + core},
            device_id_type=MESH,
        )

    def forward_copy(c):
        source = lax.rem(chip + n_dp // 2 - c, n_dp // 2) * 2 + core
        return pltpu.make_async_remote_copy(
            src_ref=terms.at[rows_from(source)],
            dst_ref=terms.at[rows_from(source)],
            send_sem=fw_s.at[c],
            recv_sem=fw_r.at[c],
            device_id={"dp": partner},
            device_id_type=MESH,
        )

    def last_step():
        for k in last:
            x_copies[k].wait_recv()
            g_copies[k].wait_recv()
        if exchange:
            for j in range(1, n_dp):
                band_copy(j, recv_x, band_x, bx_s, bx_r).start()
                band_copy(j, recv_g, band_g, bg_s, bg_r).start()
        for k in across:
            returns[k].start()
        forward(*last_quarter)
        if exchange:
            terms[rows_from(dp), : 2 * hid] = pair[late]
            terms[rows_from(dp), 2 * hid :] = hidden[late]
            for c in range(1, n_dp // 2):
                term_copy(c).start()
            forward_copy(0).start()
            band_x[rows_from(dp)] = recv_x[late, columns_of(dp)]
            band_g[rows_from(dp)] = recv_g[late, columns_of(dp)]
            backward(*last_quarter)
            for k in last:
                returns[k].start()

    def forward_terms():
        for c in range(1, n_dp // 2):
            term_copy(c).wait_recv()
            forward_copy(c).start()

    for k in near:
        x_copies[k].wait_recv()
        g_copies[k].wait_recv()
    forward(*near_half)
    backward(*near_half)
    for k in near:
        returns[k].start()
    arrived[rows_of(0)] = ret[rows_of(0)]
    for k in across:
        x_copies[k].wait_recv()
        g_copies[k].wait_recv()
    forward(*across_quarter)
    backward(*across_quarter)
    if exchange:
        first = (me > 0) & (me < n_expert - 1)
        pl.when(first)(last_step)
    else:
        last_step()

    def weight_rows(start, size):
        at = pl.ds(pl.multiple_of(start, size), size)
        contract = (((0,), (0,)), ((), ()))
        part[at, : 2 * hid] = (
            grad_scale
            * lax.dot_general(
                recv_x[:early_rows, at], pair[:early_rows], contract, preferred_element_type=F32
            )
        ).astype(BF16)
        part[at, 2 * hid :] = (
            grad_scale
            * lax.dot_general(
                recv_g[:early_rows, at], hidden[:early_rows], contract, preferred_element_type=F32
            )
        ).astype(BF16)

    def band(chip_at, core_at, g):
        return pl.ds(pl.multiple_of((chip_at * 2 + core_at) * share + g * sub, sub), sub)

    bands = [(s, t) for s in range(1, na) for t in list(range(1, nb)) + [0]]
    bands += [(0, t) for t in list(range(1, nb)) + [0]]
    items = [(s, t, g) for s, t in bands for g in range(SUBS)]

    def item_chip(s, t):
        return chip_of(lax.rem(a + s, na), lax.rem(b + t, nb))

    banded = share % 128 == 0
    if not banded:

        @pl.loop(0, width // 256)
        def _(j):
            weight_rows(j * 256, 256)

    def pair_copy(index, chip_at, g):
        rows = band(chip_at, 1 - core, g)
        return pltpu.make_async_remote_copy(
            src_ref=part.at[rows],
            dst_ref=recv_a.at[pl.ds(pl.multiple_of(chip_at * share + g * sub, sub), sub)],
            send_sem=a_s.at[index],
            recv_sem=a_r.at[index],
            device_id={"dp": partner},
            device_id_type=MESH,
        )

    def partner_chip(s, t):
        if na == nb:
            a_at, b_at = lax.rem(b + s, na), lax.rem(a + t, nb)
            return jnp.where(core == 1, b_at * na + a_at, a_at * na + b_at)
        return item_chip(s, t)

    a_copies = []
    for index, (s, t, g) in enumerate(items):
        chip_at = partner_chip(s, t)
        if banded and g == 0:
            weight_rows((chip_at * 2 + 1 - core) * share, share)
        copy = pair_copy(index, chip_at, g)
        copy.start()
        a_copies.append(copy)

    if not exchange:
        backward(*last_quarter)
        for k in last:
            returns[k].start()

    def pair_sum(index, s, t, g):
        chip_at = item_chip(s, t)
        a_copies[index].wait_recv()
        return (
            part[band(chip_at, core, g)].astype(F32)
            + recv_a[pl.ds(pl.multiple_of(chip_at * share + g * sub, sub), sub)].astype(F32)
        )

    if banded:
        for s, t in bands:
            weight_rows((item_chip(s, t) * 2 + core) * share, share)

    b_copies = {}
    for index, (s, t, g) in enumerate(items):
        if s == 0:
            continue
        at = ((s - 1) * nb + t) * SUBS + g
        send_b[at] = pair_sum(index, s, t, g).astype(BF16)
        copy = pltpu.make_async_remote_copy(
            src_ref=send_b.at[at],
            dst_ref=recv_b.at[at],
            send_sem=b_s.at[at],
            recv_sem=b_r.at[at],
            device_id={"dp": dp_of(lax.rem(a + s, na), b)},
            device_id_type=MESH,
        )
        copy.start()
        b_copies[s, t, g] = copy
    if exchange:
        pl.when(first)(forward_terms)
    c_copies = {}
    for index, (s, t, g) in enumerate(items):
        if s > 0:
            continue
        total = pair_sum(index, s, t, g)
        for s_from in range(1, na):
            b_copies[s_from, t, g].wait_recv()
            total = total + recv_b[((s_from - 1) * nb + t) * SUBS + g].astype(F32)
        if t > 0:
            at = (t - 1) * SUBS + g
            send_c[at] = total.astype(BF16)
            copy = pltpu.make_async_remote_copy(
                src_ref=send_c.at[at],
                dst_ref=recv_c.at[at],
                send_sem=c_s.at[at],
                recv_sem=c_r.at[at],
                device_id={"dp": dp_of(a, lax.rem(b + t, nb))},
                device_id_type=MESH,
            )
            copy.start()
            c_copies[t, g] = copy
        else:
            w_grad_ref[0, pl.ds(g * sub, sub)] = total
    for t in range(1, nb):
        for g in range(SUBS):
            c_copies[t, g].wait_recv()
            w_grad_ref[0, pl.ds(g * sub, sub)] += recv_c[(t - 1) * SUBS + g].astype(F32)

    if exchange:

        @pl.when(jnp.logical_not(first))
        def _():
            last_step()
            forward_terms()

        for j in range(1, n_dp):
            band_copy(j, recv_x, band_x, bx_s, bx_r).wait_recv()
            band_copy(j, recv_g, band_g, bg_s, bg_r).wait_recv()
        for c in range(n_dp // 2):
            forward_copy(c).wait_recv()
        contract = (((0,), (0,)), ((), ()))
        w_grad_ref[0, :, : 2 * hid] += grad_scale * lax.dot_general(
            band_x[...], terms[:, : 2 * hid], contract, preferred_element_type=F32
        )
        w_grad_ref[0, :, 2 * hid :] += grad_scale * lax.dot_general(
            band_g[...], terms[:, 2 * hid :], contract, preferred_element_type=F32
        )

    for k in near + far:
        returns[k].wait_recv()
    in_grad_ref[...] = jnp.dot(table_t, arrived[...], preferred_element_type=F32).astype(BF16)

    for k in near + far:
        x_copies[k].wait_send()
        g_copies[k].wait_send()
        returns[k].wait_send()
    if exchange:
        for j in range(1, n_dp):
            band_copy(j, recv_x, band_x, bx_s, bx_r).wait_send()
            band_copy(j, recv_g, band_g, bg_s, bg_r).wait_send()
        for c in range(n_dp // 2):
            if c > 0:
                term_copy(c).wait_send()
            forward_copy(c).wait_send()
    for copy in a_copies + list(b_copies.values()) + list(c_copies.values()):
        copy.wait_send()


def local(n_expert, n_dp, tokens, out_grad, gate_prob, routing, expert_weights):
    tok, width = tokens.shape
    full = expert_weights.shape[2]
    hid = full // 3
    cap = max(16, 2 * tok // n_expert)
    slots = n_expert * cap
    share = width // n_dp
    _, _, _, na, nb = plan(n_expert, n_dp)
    sub = share // SUBS
    chips = na * nb
    n_b, n_c = max(1, (na - 1) * nb) * SUBS, max(1, nb - 1) * SUBS
    dma = pltpu.SemaphoreType.DMA
    vmem = pl.BlockSpec(memory_space=pltpu.VMEM)
    extra = []
    if can_exchange(width, n_expert, n_dp):
        rows = n_dp * slots // 4
        extra = [
            pltpu.VMEM((rows, share), BF16),
            pltpu.VMEM((rows, share), BF16),
            pltpu.VMEM((rows, full), BF16),
        ]
        extra += [dma((n_dp,))] * 4 + [dma((chips,))] * 4
    early = pl.pallas_call(
        functools.partial(body, n_expert, n_dp, cap),
        out_shape=(
            jax.ShapeDtypeStruct((tok, width), BF16),
            jax.ShapeDtypeStruct((1, share, full), F32),
        ),
        in_specs=[vmem] * 4 + [pl.BlockSpec(memory_space=pl.ANY)],
        out_specs=(vmem, vmem),
        scratch_shapes=[
            pltpu.VMEM((width, full), BF16),
            pltpu.VMEM((slots, width), BF16),
            pltpu.VMEM((slots, width), BF16),
            pltpu.VMEM((slots, width), BF16),
            pltpu.VMEM((slots, width), BF16),
            pltpu.VMEM((slots, width), BF16),
            pltpu.VMEM((slots, width), BF16),
            pltpu.VMEM((slots, 2 * hid), BF16),
            pltpu.VMEM((slots, hid), BF16),
            pltpu.VMEM((width, full), BF16),
            pltpu.VMEM((chips * share, full), BF16),
            pltpu.VMEM((n_b, sub, full), BF16),
            pltpu.VMEM((n_b, sub, full), BF16),
            pltpu.VMEM((n_c, sub, full), BF16),
            pltpu.VMEM((n_c, sub, full), BF16),
            dma,
            dma((n_expert,)),
            dma((n_expert,)),
            dma((n_expert,)),
            dma((n_expert,)),
            dma((n_expert,)),
            dma((n_expert,)),
            dma((chips * SUBS,)),
            dma((chips * SUBS,)),
            dma((n_b,)),
            dma((n_b,)),
            dma((n_c,)),
            dma((n_c,)),
        ]
        + extra,
        compiler_params=pltpu.CompilerParams(
            collective_id=0, has_side_effects=True, vmem_limit_bytes=60 * 1024 * 1024
        ),
        name="moe_backward",
    )(tokens, out_grad, gate_prob.reshape(1, tok), routing.reshape(1, tok), expert_weights)
    return pl.pallas_call(
        write_out,
        out_shape=(
            jax.ShapeDtypeStruct((tok, width), BF16),
            jax.ShapeDtypeStruct((1, share, full), F32),
        ),
        in_specs=[pl.BlockSpec(memory_space=pl.ANY)] * 2,
        out_specs=(pl.BlockSpec(memory_space=pl.ANY),) * 2,
        scratch_shapes=[
            pltpu.VMEM((tok, width), BF16),
            pltpu.VMEM((1, share, full), F32),
            dma((2 * PIECES,)),
            dma((2 * PIECES,)),
        ],
        name="write_out",
    )(*early)


def write_out(in_grad_ref, w_grad_ref, in_grad_out, w_grad_out, x_held, w_held, in_s, out_s):
    moves = []
    for p in range(PIECES):
        for src, mid, dst in (
            (in_grad_ref, x_held, in_grad_out),
            (w_grad_ref.at[0], w_held.at[0], w_grad_out.at[0]),
        ):
            rows = src.shape[0] // PIECES
            at = pl.ds(p * rows, rows)
            n = len(moves)
            moves.append(
                (
                    pltpu.make_async_copy(src.at[at], mid.at[at], in_s.at[n]),
                    pltpu.make_async_copy(mid.at[at], dst.at[at], out_s.at[n]),
                )
            )
    for take, _ in moves:
        take.start()
    for take, put in moves:
        take.wait()
        put.start()
    for _, put in moves:
        put.wait()


def solution(mesh):
    tokens_spec = P(("dp", "expert"), None)
    return jax.shard_map(
        functools.partial(local, mesh.shape["expert"], mesh.shape["dp"]),
        mesh=mesh,
        in_specs=(tokens_spec, tokens_spec, tokens_spec, tokens_spec, P("expert", None, None)),
        out_specs=(tokens_spec, P("expert", "dp", None)),
        check_vma=False,
    )
```

```python
import functools
import math
import jax
import jax.numpy as jnp
from jax import lax
from jax.experimental import pallas as pl
from jax.experimental.pallas import tpu as pltpu
from jax.sharding import PartitionSpec as P

MESH = pl.DeviceIdType.MESH
F32 = jnp.float32
BF16 = jnp.bfloat16
SUBS = 2
PIECES = 4


def xor(value, step):
    total, bit = 0, 1
    result = value
    while bit <= step:
        if step & bit:
            result = result + bit - 2 * bit * (lax.rem(lax.div(value, bit), 2))
        bit *= 2
    return result


def plan(n_expert, n_dp):
    half, quarter = n_expert // 2, n_expert // 4
    near = list(range(1, half))
    across = list(range(n_expert - 1, half + quarter - 1, -1))
    last = list(range(half + quarter - 1, half - 1, -1))
    chips = n_dp // 2
    side = math.isqrt(chips)
    while chips % side:
        side -= 1
    return near, across, last, chips // side, side


def body(
    n_expert,
    n_dp,
    cap,
    tokens_ref,
    out_grad_ref,
    gate_ref,
    route_ref,
    w_hbm,
    in_grad_ref,
    w_grad_ref,
    w_ref,
    send_x,
    send_g,
    recv_x,
    recv_g,
    ret,
    arrived,
    pair,
    hidden,
    part,
    recv_a,
    send_b,
    recv_b,
    send_c,
    recv_c,
    w_sem,
    dx_s,
    dx_r,
    dg_s,
    dg_r,
    rt_s,
    rt_r,
    a_s,
    a_r,
    b_s,
    b_r,
    c_s,
    c_r,
):
    near, across, last, na, nb = plan(n_expert, n_dp)
    far = across + last
    me = lax.axis_index("expert")
    dp = lax.axis_index("dp")
    tok, width = tokens_ref.shape
    hid = w_ref.shape[1] // 3
    slots = n_expert * cap
    quarter_rows = slots // 4
    share = width // n_dp
    sub = share // SUBS
    grad_scale = float(tok * n_dp) ** (-0.5)
    core = lax.rem(dp, 2)
    chip = lax.div(dp, 2)
    pos_hi, pos_lo = lax.div(chip, na), lax.rem(chip, na)
    if na == nb:
        a = jnp.where(core == 0, pos_lo, pos_hi)
        b = jnp.where(core == 0, pos_hi, pos_lo)
    else:
        a, b = pos_lo, pos_hi

    def chip_of(a_at, b_at):
        plain = b_at * na + a_at
        if na == nb:
            return jnp.where(core == 0, plain, a_at * na + b_at)
        return plain

    def dp_of(a_at, b_at):
        return chip_of(a_at, b_at) * 2 + core

    w_copy = pltpu.make_async_copy(w_hbm.at[0], w_ref, w_sem)
    w_copy.start()

    barrier = pltpu.get_barrier_semaphore()
    partner = dp + 1 - 2 * core
    greeted = 0
    for k in near + far:
        pl.semaphore_signal(barrier, inc=1, device_id={"expert": xor(me, k)}, device_id_type=MESH)
        greeted += 1
    pl.semaphore_signal(barrier, inc=1, device_id={"dp": partner}, device_id_type=MESH)
    greeted += 1
    for s in range(1, na):
        pl.semaphore_signal(
            barrier, inc=1, device_id={"dp": dp_of(lax.rem(a + s, na), b)}, device_id_type=MESH
        )
        greeted += 1
    for t in range(1, nb):
        pl.semaphore_signal(
            barrier, inc=1, device_id={"dp": dp_of(a, lax.rem(b + t, nb))}, device_id_type=MESH
        )
        greeted += 1

    row_i = lax.broadcasted_iota(jnp.int32, (tok, tok), 0)
    col_i = lax.broadcasted_iota(jnp.int32, (tok, tok), 1)

    def column(row):
        return jnp.sum(jnp.where(row_i == col_i, row, 0.0), axis=1, keepdims=True)

    route_row = route_ref[...].astype(F32)
    route_col = column(route_row)
    same = route_col == route_row
    pos_row = jnp.sum(jnp.where(same & (row_i < col_i), 1.0, 0.0), axis=0, keepdims=True)
    pos_col = jnp.sum(jnp.where(same & (col_i < row_i), 1.0, 0.0), axis=1, keepdims=True)
    slot_row = route_row * cap + pos_row
    slot_col = route_col * cap + pos_col
    slot_at = lax.broadcasted_iota(jnp.int32, (slots, tok), 0).astype(F32)
    table = jnp.where(slot_at == slot_row, 1.0, 0.0).astype(BF16)
    slot_of = lax.broadcasted_iota(jnp.int32, (tok, slots), 1).astype(F32)
    table_t = jnp.where(slot_of == slot_col, 1.0, 0.0).astype(BF16)

    send_x[...] = jnp.dot(table, tokens_ref[...], preferred_element_type=F32).astype(BF16)
    scaled = (column(gate_ref[...]) * out_grad_ref[...].astype(F32)).astype(BF16)
    send_g[...] = jnp.dot(table, scaled, preferred_element_type=F32).astype(BF16)

    def rows_of(index):
        return pl.ds(pl.multiple_of(index * cap, cap), cap)

    pl.semaphore_wait(barrier, greeted)

    def dispatch(k, src, dst, s_sem, r_sem):
        peer = xor(me, k)
        return pltpu.make_async_remote_copy(
            src_ref=src.at[rows_of(peer)],
            dst_ref=dst.at[rows_of(me)],
            send_sem=s_sem.at[k],
            recv_sem=r_sem.at[k],
            device_id={"expert": peer},
            device_id_type=MESH,
        )

    x_copies = {k: dispatch(k, send_x, recv_x, dx_s, dx_r) for k in near + far}
    g_copies = {k: dispatch(k, send_g, recv_g, dg_s, dg_r) for k in near + far}
    returns = {k: dispatch(k, ret, arrived, rt_s, rt_r) for k in near + far}
    for k in near + far:
        x_copies[k].start()
        g_copies[k].start()

    recv_x[rows_of(me)] = send_x[rows_of(me)]
    recv_g[rows_of(me)] = send_g[rows_of(me)]
    w_copy.wait()

    mine = lax.div(me, n_expert // 4)

    def forward(start, size):
        rows = pl.ds(pl.multiple_of(start, cap), size)
        x = recv_x[rows]
        pre_gate = jnp.dot(x, w_ref[:, :hid], preferred_element_type=F32)
        pre_up = jnp.dot(x, w_ref[:, hid : 2 * hid], preferred_element_type=F32)
        grad_hidden = jnp.dot(recv_g[rows], w_ref[:, 2 * hid :], preferred_element_type=F32)
        sig = jax.nn.sigmoid(pre_gate)
        active = pre_gate * sig
        hidden[rows] = (active * pre_up).astype(BF16)
        grad_gate = grad_hidden * pre_up * (sig * (1.0 + pre_gate * (1.0 - sig)))
        pair[rows, :hid] = grad_gate.astype(BF16)
        pair[rows, hid:] = (grad_hidden * active).astype(BF16)

    def backward(start, size):
        rows = pl.ds(pl.multiple_of(start, cap), size)
        tile = min(512, width)

        @pl.loop(0, width // tile)
        def _(j):
            at = pl.ds(pl.multiple_of(j * tile, tile), tile)
            ret[rows, at] = lax.dot_general(
                pair[rows],
                w_ref[at, : 2 * hid],
                (((1,), (1,)), ((), ())),
                preferred_element_type=F32,
            ).astype(BF16)

    near_half = (lax.div(mine, 2) * 2 * quarter_rows, 2 * quarter_rows)
    across_quarter = (xor(mine, 3) * quarter_rows, quarter_rows)
    last_quarter = (xor(mine, 2) * quarter_rows, quarter_rows)
    for k in near:
        x_copies[k].wait_recv()
        g_copies[k].wait_recv()
    forward(*near_half)
    backward(*near_half)
    for k in near:
        returns[k].start()
    arrived[rows_of(me)] = ret[rows_of(me)]
    for k in across:
        x_copies[k].wait_recv()
        g_copies[k].wait_recv()
    forward(*across_quarter)
    backward(*across_quarter)
    for k in last:
        x_copies[k].wait_recv()
        g_copies[k].wait_recv()
    for k in across:
        returns[k].start()
    forward(*last_quarter)

    def weight_rows(start, size):
        at = pl.ds(pl.multiple_of(start, size), size)
        contract = (((0,), (0,)), ((), ()))
        part[at, : 2 * hid] = (
            grad_scale
            * lax.dot_general(recv_x[:, at], pair[...], contract, preferred_element_type=F32)
        ).astype(BF16)
        part[at, 2 * hid :] = (
            grad_scale
            * lax.dot_general(recv_g[:, at], hidden[...], contract, preferred_element_type=F32)
        ).astype(BF16)

    def band(chip_at, core_at, g):
        return pl.ds(pl.multiple_of((chip_at * 2 + core_at) * share + g * sub, sub), sub)

    bands = [(s, t) for s in range(1, na) for t in list(range(1, nb)) + [0]]
    bands += [(0, t) for t in list(range(1, nb)) + [0]]
    items = [(s, t, g) for s, t in bands for g in range(SUBS)]

    def item_chip(s, t):
        return chip_of(lax.rem(a + s, na), lax.rem(b + t, nb))

    banded = share % 128 == 0
    if not banded:

        @pl.loop(0, width // 256)
        def _(j):
            weight_rows(j * 256, 256)

    def pair_copy(index, chip_at, g):
        rows = band(chip_at, 1 - core, g)
        return pltpu.make_async_remote_copy(
            src_ref=part.at[rows],
            dst_ref=recv_a.at[pl.ds(pl.multiple_of(chip_at * share + g * sub, sub), sub)],
            send_sem=a_s.at[index],
            recv_sem=a_r.at[index],
            device_id={"dp": partner},
            device_id_type=MESH,
        )

    def partner_chip(s, t):
        if na == nb:
            a_at, b_at = lax.rem(b + s, na), lax.rem(a + t, nb)
            return jnp.where(core == 1, b_at * na + a_at, a_at * na + b_at)
        return item_chip(s, t)

    a_copies = []
    for index, (s, t, g) in enumerate(items):
        chip_at = partner_chip(s, t)
        if banded and g == 0:
            weight_rows((chip_at * 2 + 1 - core) * share, share)
        copy = pair_copy(index, chip_at, g)
        copy.start()
        a_copies.append(copy)

    backward(*last_quarter)
    for k in last:
        returns[k].start()

    def pair_sum(index, s, t, g):
        chip_at = item_chip(s, t)
        a_copies[index].wait_recv()
        return (
            part[band(chip_at, core, g)].astype(F32)
            + recv_a[pl.ds(pl.multiple_of(chip_at * share + g * sub, sub), sub)].astype(F32)
        )

    if banded:
        for s, t in bands:
            weight_rows((item_chip(s, t) * 2 + core) * share, share)

    b_copies = {}
    for index, (s, t, g) in enumerate(items):
        if s == 0:
            continue
        at = ((s - 1) * nb + t) * SUBS + g
        send_b[at] = pair_sum(index, s, t, g).astype(BF16)
        copy = pltpu.make_async_remote_copy(
            src_ref=send_b.at[at],
            dst_ref=recv_b.at[at],
            send_sem=b_s.at[at],
            recv_sem=b_r.at[at],
            device_id={"dp": dp_of(lax.rem(a + s, na), b)},
            device_id_type=MESH,
        )
        copy.start()
        b_copies[s, t, g] = copy
    c_copies = {}
    for index, (s, t, g) in enumerate(items):
        if s > 0:
            continue
        total = pair_sum(index, s, t, g)
        for s_from in range(1, na):
            b_copies[s_from, t, g].wait_recv()
            total = total + recv_b[((s_from - 1) * nb + t) * SUBS + g].astype(F32)
        if t > 0:
            at = (t - 1) * SUBS + g
            send_c[at] = total.astype(BF16)
            copy = pltpu.make_async_remote_copy(
                src_ref=send_c.at[at],
                dst_ref=recv_c.at[at],
                send_sem=c_s.at[at],
                recv_sem=c_r.at[at],
                device_id={"dp": dp_of(a, lax.rem(b + t, nb))},
                device_id_type=MESH,
            )
            copy.start()
            c_copies[t, g] = copy
        else:
            w_grad_ref[0, pl.ds(g * sub, sub)] = total
    for t in range(1, nb):
        for g in range(SUBS):
            c_copies[t, g].wait_recv()
            w_grad_ref[0, pl.ds(g * sub, sub)] += recv_c[(t - 1) * SUBS + g].astype(F32)

    for k in near + far:
        returns[k].wait_recv()
    in_grad_ref[...] = jnp.dot(table_t, arrived[...], preferred_element_type=F32).astype(BF16)

    for k in near + far:
        x_copies[k].wait_send()
        g_copies[k].wait_send()
        returns[k].wait_send()
    for copy in a_copies + list(b_copies.values()) + list(c_copies.values()):
        copy.wait_send()


def paired(width, hid, n_expert, n_dp):
    chips_a, chips_b = plan(n_expert, n_dp)[3:]
    return n_expert == 4 and chips_a == chips_b == 2 and width % (128 * n_dp) == hid % 128 == 0


def paired_body(
    n_expert,
    n_dp,
    cap,
    tokens_ref,
    out_grad_ref,
    gate_ref,
    route_ref,
    w_hbm,
    in_grad_ref,
    w_grad_ref,
    w_ref,
    w2_ref,
    send_x,
    send_g,
    recv_x,
    recv_g,
    ret,
    arrived,
    pair,
    hidden,
    part,
    recv_a,
    send_b,
    recv_b,
    send_c,
    recv_c,
    stage,
    band_x,
    band_g,
    terms,
    held_d,
    send_d,
    near_d,
    far_d,
    w_sem,
    st_sem,
    dx_s,
    dx_r,
    dg_s,
    dg_r,
    rt_s,
    rt_r,
    a_s,
    a_r,
    b_s,
    b_r,
    c_s,
    c_r,
    bx_s,
    bx_r,
    bg_s,
    bg_r,
    tm_s,
    tm_r,
    fw_s,
    fw_r,
    w_s,
    w_r,
    wz_s,
    ag_s,
    ag_r,
    pf_s,
    pf_r,
    d_s,
    d_r,
    f_r,
):
    _, _, _, na, nb = plan(n_expert, n_dp)
    chips = na * nb
    me = lax.axis_index("expert")
    dp = lax.axis_index("dp")
    half = lax.div(me, 2)
    inner = (me == 1) | (me == n_expert - 2)
    outer = jnp.logical_not(inner)
    near = me + 1 - 2 * lax.rem(me, 2)
    mirror = n_expert - 1 - me
    inner_far = 2 - half
    outer_far = 3 - 3 * half
    tok, width = tokens_ref.shape
    hid = w_ref.shape[1] // 3
    slots = n_expert * cap
    share = width // n_dp
    sub = share // SUBS
    grad_scale = float(tok * n_dp) ** (-0.5)
    core = lax.rem(dp, 2)
    chip = lax.div(dp, 2)
    partner = dp + 1 - 2 * core
    pos_hi, pos_lo = lax.div(chip, na), lax.rem(chip, na)
    if na == nb:
        a = jnp.where(core == 0, pos_lo, pos_hi)
        b = jnp.where(core == 0, pos_hi, pos_lo)
    else:
        a, b = pos_lo, pos_hi

    def chip_of(a_at, b_at):
        plain = b_at * na + a_at
        if na == nb:
            return jnp.where(core == 0, plain, a_at * na + b_at)
        return plain

    def dp_of(a_at, b_at):
        return chip_of(a_at, b_at) * 2 + core

    def columns_of(index):
        return pl.ds(pl.multiple_of(index * share, share), share)

    w_copy = pltpu.make_async_copy(w_hbm.at[0], w_ref, w_sem)
    slices = w2_ref.shape[0]
    unit = hid // slices

    def stage_copy(q, third):
        return pltpu.make_async_copy(
            w_hbm.at[0, columns_of(dp), pl.ds(third * hid + q * unit, unit)],
            stage.at[q, :, pl.ds(third * unit, unit)],
            st_sem.at[q * 3 + third],
        )

    @pl.when(outer)
    def _():
        for q in range(slices):
            for third in range(3):
                stage_copy(q, third).start()

    w_copy.start()

    barrier = pltpu.get_barrier_semaphore()
    for k in range(1, n_expert):
        peer = lax.rem(me + k, n_expert)
        pl.semaphore_signal(barrier, inc=1, device_id={"expert": peer}, device_id_type=MESH)
    for j in range(1, n_dp):
        peer = lax.rem(dp + j, n_dp)
        pl.semaphore_signal(barrier, inc=1, device_id={"dp": peer}, device_id_type=MESH)

    row_i = lax.broadcasted_iota(jnp.int32, (tok, tok), 0)
    col_i = lax.broadcasted_iota(jnp.int32, (tok, tok), 1)

    def column(row):
        return jnp.sum(jnp.where(row_i == col_i, row, 0.0), axis=1, keepdims=True)

    route = route_ref[...]
    block = jnp.where(route == near, 1, jnp.where(route == inner_far, 2, 3))
    route_row = jnp.where(route == me, 0, block).astype(F32)
    route_col = column(route_row)
    same = route_col == route_row
    pos_row = jnp.sum(jnp.where(same & (row_i < col_i), 1.0, 0.0), axis=0, keepdims=True)
    pos_col = jnp.sum(jnp.where(same & (col_i < row_i), 1.0, 0.0), axis=1, keepdims=True)
    slot_row = route_row * cap + pos_row
    slot_col = route_col * cap + pos_col
    slot_at = lax.broadcasted_iota(jnp.int32, (slots, tok), 0).astype(F32)
    table = jnp.where(slot_at == slot_row, 1.0, 0.0).astype(BF16)
    slot_of = lax.broadcasted_iota(jnp.int32, (tok, slots), 1).astype(F32)
    table_t = jnp.where(slot_of == slot_col, 1.0, 0.0).astype(BF16)

    send_x[...] = jnp.dot(table, tokens_ref[...], preferred_element_type=F32).astype(BF16)
    scaled = (column(gate_ref[...]) * out_grad_ref[...].astype(F32)).astype(BF16)
    send_g[...] = jnp.dot(table, scaled, preferred_element_type=F32).astype(BF16)

    def rows_of(index):
        return pl.ds(index * cap, cap)

    kept = rows_of(3)

    def rows_from(index):
        return pl.ds(pl.multiple_of(index * cap, cap), cap)

    def remote(src, dst, s_sem, r_sem, device):
        return pltpu.make_async_remote_copy(
            src_ref=src,
            dst_ref=dst,
            send_sem=s_sem,
            recv_sem=r_sem,
            device_id=device,
            device_id_type=MESH,
        )

    pl.semaphore_wait(barrier, n_expert - 1 + n_dp - 1)

    cross_at = jnp.where(inner, 2, 3)

    def near_copy(src, dst, s_sem, r_sem):
        return remote(
            src.at[rows_of(1)], dst.at[rows_of(1)], s_sem.at[1], r_sem.at[1], {"expert": near}
        )

    def cross_copy(src, dst, s_sem, r_sem):
        return remote(
            src.at[rows_of(2)],
            dst.at[rows_from(cross_at)],
            s_sem.at[2],
            r_sem.at[cross_at],
            {"expert": inner_far},
        )

    def cross_arrival(index, dst, s_sem, r_sem):
        return remote(
            dst.at[rows_of(index)],
            dst.at[rows_of(index)],
            s_sem.at[2],
            r_sem.at[index],
            {"expert": mirror},
        )

    x_args = (send_x, recv_x, dx_s, dx_r)
    g_args = (send_g, recv_g, dg_s, dg_r)

    def return_copy(index):
        peer = {1: near, 2: mirror, 3: outer_far}[index]
        home = rows_of(min(index, 2))
        return remote(
            ret.at[rows_of(index)],
            arrived.at[home],
            rt_s.at[index],
            rt_r.at[min(index, 2)],
            {"expert": peer},
        )

    first = jnp.where(core == 0, 1, 2)

    def beside(c):
        return xor(chip, c)

    chip_first = jnp.where(core == 0, beside(1), beside(2))
    chip_second = jnp.where(core == 0, beside(2), beside(1))

    def weight_out(q):
        dst = w2_ref.at[q, columns_of(dp)]
        return remote(stage.at[q], dst, w_s.at[q], w_r.at[q], {"expert": inner_far})

    def weight_on(q):
        at = w2_ref.at[q, columns_of(dp)]
        return remote(at, at, wz_s.at[q], w_r.at[q], {"expert": near})

    def spread(c, q):
        at = w2_ref.at[q, columns_of(dp)]
        n = c * slices + q
        return remote(at, at, ag_s.at[n], ag_r.at[n], {"dp": beside(c) * 2 + core})

    def relay(q):
        at = w2_ref.at[q, columns_of(chip_first * 2 + core)]
        n = 3 * slices + q
        return remote(at, at, ag_s.at[n], ag_r.at[n], {"dp": chip_second * 2 + core})

    def hand_over(c, q):
        at = w2_ref.at[q, columns_of(beside(c) * 2 + core)]
        n = c * slices + q
        return remote(at, at, pf_s.at[n], pf_r.at[n], {"dp": partner})

    def band_copy(j, src, dst, s_sem, r_sem):
        peer = lax.rem(dp + j, n_dp)
        return remote(
            src.at[kept, columns_of(peer)],
            dst.at[rows_from(dp)],
            s_sem.at[j],
            r_sem.at[j],
            {"dp": peer},
        )

    bx_args = (send_x, band_x, bx_s, bx_r)
    bg_args = (send_g, band_g, bg_s, bg_r)

    def term_copy(c, q):
        at = terms.at[q, rows_from(dp)]
        n = c * slices + q
        return remote(at, at, tm_s.at[n], tm_r.at[n], {"dp": beside(c) * 2 + core})

    def term_over(c, q):
        at = terms.at[q, rows_from(beside(c) * 2 + core)]
        n = c * slices + q
        return remote(at, at, fw_s.at[n], fw_r.at[n], {"dp": partner})

    @pl.when(outer)
    def _():
        for q in range(slices):
            for third in range(3):
                stage_copy(q, third).wait()
            weight_out(q).start()

    near_copy(*x_args).start()
    pl.when(outer)(lambda: near_copy(*g_args).start())
    cross_copy(*x_args).start()
    cross_copy(*g_args).start()
    for j in range(1, n_dp):
        band_copy(j, *bx_args).start()
        band_copy(j, *bg_args).start()

    recv_x[rows_of(0)] = send_x[rows_of(0)]
    recv_g[rows_of(0)] = send_g[rows_of(0)]
    band_x[rows_from(dp)] = send_x[kept, columns_of(dp)]
    band_g[rows_from(dp)] = send_g[kept, columns_of(dp)]

    @pl.when(outer)
    def _():
        rest = pl.ds(2 * cap, 2 * cap)
        recv_x[rest] = jnp.zeros((2 * cap, width), BF16)
        recv_g[rest] = jnp.zeros((2 * cap, width), BF16)
        pair[rest] = jnp.zeros((2 * cap, 2 * hid), BF16)
        hidden[rest] = jnp.zeros((2 * cap, hid), BF16)

    def forward(x, g, weights):
        third = weights.shape[1] // 3
        pre_gate = jnp.dot(x, weights[:, :third], preferred_element_type=F32)
        pre_up = jnp.dot(x, weights[:, third : 2 * third], preferred_element_type=F32)
        grad_hidden = jnp.dot(g, weights[:, 2 * third :], preferred_element_type=F32)
        sig = jax.nn.sigmoid(pre_gate)
        active = pre_gate * sig
        grad_gate = grad_hidden * pre_up * (sig * (1.0 + pre_gate * (1.0 - sig)))
        return (
            grad_gate.astype(BF16),
            (grad_hidden * active).astype(BF16),
            (active * pre_up).astype(BF16),
        )

    def forward_rows(start, size):
        rows = pl.ds(start, size)
        grad_gate, grad_up, kept_hidden = forward(recv_x[rows], recv_g[rows], w_ref)
        pair[rows, :hid] = grad_gate
        pair[rows, hid:] = grad_up
        hidden[rows] = kept_hidden

    def columns(pieces, dst, rows):
        tile = min(512, width)

        @pl.loop(0, width // tile)
        def _(j):
            at = pl.ds(pl.multiple_of(j * tile, tile), tile)
            total = 0.0
            for grads, weights in pieces:
                total = total + lax.dot_general(
                    grads(), weights(at), (((1,), (1,)), ((), ())), preferred_element_type=F32
                )
            dst[rows, at] = total.astype(BF16)

    def backward_rows(start, size):
        rows = pl.ds(start, size)
        columns([(lambda: pair[rows], lambda at: w_ref[at, : 2 * hid])], ret, rows)

    contract = (((0,), (0,)), ((), ()))
    mine = rows_from(dp)

    def kept_forward(q):
        grad_gate, grad_up, kept_hidden = forward(send_x[kept], send_g[kept], w2_ref.at[q])
        terms[q, mine, :unit] = grad_gate
        terms[q, mine, unit : 2 * unit] = grad_up
        terms[q, mine, 2 * unit :] = kept_hidden

    def kept_grad(q):
        first = lax.dot_general(
            band_x[...], terms[q, :, : 2 * unit], contract, preferred_element_type=F32
        )
        second = lax.dot_general(
            band_g[...], terms[q, :, 2 * unit :], contract, preferred_element_type=F32
        )
        return grad_scale * jnp.concatenate([first, second], axis=1)

    def near_hop(q):
        return remote(send_d.at[q], near_d.at[q], d_s.at[q], d_r.at[q], {"expert": near})

    def far_hop(q):
        return remote(send_d.at[q], far_d.at[q], d_s.at[q], f_r.at[q], {"expert": outer_far})

    def take(q):
        weight_on(q).wait_recv()
        pl.when(inner)(lambda: weight_on(q).start())
        for c in (1, 2):
            spread(c, q).start()
        hand_over(0, q).start()

    def pass_on(q):
        for c in (1, 2):
            spread(c, q).wait_recv()
        relay(q).start()
        for c in (1, 2):
            hand_over(c, q).start()

    def pass_last(q):
        relay(q).wait_recv()
        hand_over(3, q).start()

    def kept_terms(q):
        for c in range(4):
            hand_over(c, q).wait_recv()
        kept_forward(q)
        for c in range(1, 4):
            term_copy(c, q).start()
        term_over(0, q).start()

    def pass_terms(q):
        for c in range(1, 4):
            term_copy(c, q).wait_recv()
            term_over(c, q).start()

    def kept_band(q):
        if q == 0:
            for j in range(1, n_dp):
                band_copy(j, *bx_args).wait_recv()
                band_copy(j, *bg_args).wait_recv()
        for c in range(4):
            term_over(c, q).wait_recv()
        held_d[q] = kept_grad(q)

        @pl.when(outer)
        def _():
            send_d[q] = held_d[q].astype(BF16)
            near_hop(q).start()

    def near_rows():
        near_copy(*x_args).wait_recv()
        near_copy(*g_args).wait_recv()
        forward_rows(0, 2 * cap)
        backward_rows(0, 2 * cap)
        return_copy(1).start()
        arrived[rows_of(0)] = ret[rows_of(0)]

        @pl.when(inner)
        def _():
            cross_arrival(2, *x_args[1:]).wait_recv()
            cross_arrival(2, *g_args[1:]).wait_recv()
            forward_rows(2 * cap, cap)
            backward_rows(2 * cap, cap)
            return_copy(2).start()

    def late_near():
        @pl.when(inner)
        def _():
            near_copy(*g_args).start()
            w_copy.wait()

        pl.when(outer)(w_copy.wait)

    take(0)
    take(1)
    pass_on(0)
    take(2)
    late_near()
    pass_on(1)
    pass_last(0)
    kept_terms(0)
    pass_on(2)
    pass_last(1)
    kept_terms(1)
    pass_terms(0)
    pass_last(2)
    kept_terms(2)
    kept_band(0)
    pass_terms(1)
    near_rows()
    kept_band(1)
    pass_terms(2)
    kept_pieces = [
        (lambda q=q: terms[q, mine, : 2 * unit], lambda at, q=q: w2_ref[q, at, : 2 * unit])
        for q in range(slices)
    ]
    columns(kept_pieces, arrived, kept)
    kept_band(2)

    @pl.when(inner)
    def _():
        cross_arrival(3, *x_args[1:]).wait_recv()
        cross_arrival(3, *g_args[1:]).wait_recv()
        forward_rows(3 * cap, cap)

    def weight_rows(start, size):
        at = pl.ds(pl.multiple_of(start, size), size)
        part[at, : 2 * hid] = (
            grad_scale
            * lax.dot_general(recv_x[:, at], pair[...], contract, preferred_element_type=F32)
        ).astype(BF16)
        part[at, 2 * hid :] = (
            grad_scale
            * lax.dot_general(recv_g[:, at], hidden[...], contract, preferred_element_type=F32)
        ).astype(BF16)

    def band(chip_at, core_at, g):
        return pl.ds(pl.multiple_of((chip_at * 2 + core_at) * share + g * sub, sub), sub)

    bands = [(s, t) for s in range(1, na) for t in list(range(1, nb)) + [0]]
    bands += [(0, t) for t in list(range(1, nb)) + [0]]
    items = [(s, t, g) for s, t in bands for g in range(SUBS)]

    def item_chip(s, t):
        return chip_of(lax.rem(a + s, na), lax.rem(b + t, nb))

    def pair_copy(index, chip_at, g):
        return remote(
            part.at[band(chip_at, 1 - core, g)],
            recv_a.at[pl.ds(pl.multiple_of(chip_at * share + g * sub, sub), sub)],
            a_s.at[index],
            a_r.at[index],
            {"dp": partner},
        )

    def partner_chip(s, t):
        if na == nb:
            a_at, b_at = lax.rem(b + s, na), lax.rem(a + t, nb)
            return jnp.where(core == 1, b_at * na + a_at, a_at * na + b_at)
        return item_chip(s, t)

    a_copies = []
    for index, (s, t, g) in enumerate(items):
        chip_at = partner_chip(s, t)
        if g == 0:
            weight_rows((chip_at * 2 + 1 - core) * share, share)
        copy = pair_copy(index, chip_at, g)
        copy.start()
        a_copies.append(copy)

    def pair_sum(index, s, t, g):
        chip_at = item_chip(s, t)
        a_copies[index].wait_recv()
        return (
            part[band(chip_at, core, g)].astype(F32)
            + recv_a[pl.ds(pl.multiple_of(chip_at * share + g * sub, sub), sub)].astype(F32)
        )

    b_copies = {}
    for index, (s, t, g) in enumerate(items):
        if g == 0:
            weight_rows((item_chip(s, t) * 2 + core) * share, share)
        if s == 0:
            continue
        at = ((s - 1) * nb + t) * SUBS + g
        send_b[at] = pair_sum(index, s, t, g).astype(BF16)
        copy = remote(
            send_b.at[at],
            recv_b.at[at],
            b_s.at[at],
            b_r.at[at],
            {"dp": dp_of(lax.rem(a + s, na), b)},
        )
        copy.start()
        b_copies[s, t, g] = copy

    @pl.when(inner)
    def _():
        backward_rows(3 * cap, cap)
        return_copy(3).start()
        for q in range(slices):
            near_hop(q).wait_recv()
            send_d[q] = (held_d[q] + near_d[q].astype(F32)).astype(BF16)
            far_hop(q).start()

    c_copies = {}
    for index, (s, t, g) in enumerate(items):
        if s > 0:
            continue
        total = pair_sum(index, s, t, g)
        for s_from in range(1, na):
            b_copies[s_from, t, g].wait_recv()
            total = total + recv_b[((s_from - 1) * nb + t) * SUBS + g].astype(F32)
        if t > 0:
            at = (t - 1) * SUBS + g
            send_c[at] = total.astype(BF16)
            copy = remote(
                send_c.at[at],
                recv_c.at[at],
                c_s.at[at],
                c_r.at[at],
                {"dp": dp_of(a, lax.rem(b + t, nb))},
            )
            copy.start()
            c_copies[t, g] = copy
        else:
            w_grad_ref[0, pl.ds(g * sub, sub)] = total
    for t in range(1, nb):
        for g in range(SUBS):
            c_copies[t, g].wait_recv()
            w_grad_ref[0, pl.ds(g * sub, sub)] += recv_c[(t - 1) * SUBS + g].astype(F32)

    @pl.when(outer)
    def _():
        for q in range(slices):
            far_hop(q).wait_recv()
            for third in range(3):
                at = pl.ds(third * hid + q * unit, unit)
                w_grad_ref[0, :, at] += far_d[q, :, third * unit : (third + 1) * unit].astype(F32)

    return_copy(1).wait_recv()
    return_copy(2).wait_recv()
    in_grad_ref[...] = jnp.dot(table_t, arrived[...], preferred_element_type=F32).astype(BF16)

    for args in (x_args, g_args):
        near_copy(*args).wait_send()
        cross_copy(*args).wait_send()
    return_copy(1).wait_send()
    for j in range(1, n_dp):
        band_copy(j, *bx_args).wait_send()
        band_copy(j, *bg_args).wait_send()
    for q in range(slices):
        for c in range(4):
            if c > 0:
                term_copy(c, q).wait_send()
            term_over(c, q).wait_send()
            hand_over(c, q).wait_send()
        for c in (1, 2):
            spread(c, q).wait_send()
        relay(q).wait_send()

    @pl.when(inner)
    def _():
        return_copy(2).wait_send()
        return_copy(3).wait_send()
        for q in range(slices):
            weight_on(q).wait_send()
            far_hop(q).wait_send()

    @pl.when(outer)
    def _():
        for q in range(slices):
            weight_out(q).wait_send()
            near_hop(q).wait_send()

    for copy in a_copies + list(b_copies.values()) + list(c_copies.values()):
        copy.wait_send()


def local(n_expert, n_dp, tokens, out_grad, gate_prob, routing, expert_weights):
    tok, width = tokens.shape
    full = expert_weights.shape[2]
    hid = full // 3
    cap = max(16, 2 * tok // n_expert)
    slots = n_expert * cap
    share = width // n_dp
    _, _, _, na, nb = plan(n_expert, n_dp)
    sub = share // SUBS
    chips = na * nb
    n_b, n_c = max(1, (na - 1) * nb) * SUBS, max(1, nb - 1) * SUBS
    dma = pltpu.SemaphoreType.DMA
    vmem = pl.BlockSpec(memory_space=pltpu.VMEM)
    weights, rows = pltpu.VMEM((width, full), BF16), pltpu.VMEM((slots, width), BF16)
    scratch = [weights] + [rows] * 6
    scratch += [
        pltpu.VMEM((slots, 2 * hid), BF16),
        pltpu.VMEM((slots, hid), BF16),
        pltpu.VMEM((width, full), BF16),
        pltpu.VMEM((chips * share, full), BF16),
        pltpu.VMEM((n_b, sub, full), BF16),
        pltpu.VMEM((n_b, sub, full), BF16),
        pltpu.VMEM((n_c, sub, full), BF16),
        pltpu.VMEM((n_c, sub, full), BF16),
    ]
    sems = [dma] + [dma((n_expert,))] * 6 + [dma((chips * SUBS,))] * 2
    sems += [dma((n_b,))] * 2 + [dma((n_c,))] * 2
    kernel = body
    if paired(width, hid, n_expert, n_dp):
        kernel = paired_body
        slices = hid // 128
        third = full // slices
        scratch.insert(1, pltpu.VMEM((slices, width, third), BF16))
        scratch += [pltpu.VMEM((slices, share, third), BF16)]
        scratch += [pltpu.VMEM((n_dp * cap, share), BF16)] * 2
        scratch += [pltpu.VMEM((slices, n_dp * cap, third), BF16)]
        scratch += [pltpu.VMEM((slices, share, third), F32)]
        scratch += [pltpu.VMEM((slices, share, third), BF16)] * 3
        sems.insert(1, dma((slices * 3,)))
        sems += [dma((n_dp,))] * 4 + [dma((chips * slices,))] * 4 + [dma((slices,))] * 3
        sems += [dma((chips * slices,))] * 4 + [dma((slices,))] * 3
    early = pl.pallas_call(
        functools.partial(kernel, n_expert, n_dp, cap),
        out_shape=(
            jax.ShapeDtypeStruct((tok, width), BF16),
            jax.ShapeDtypeStruct((1, share, full), F32),
        ),
        in_specs=[vmem] * 4 + [pl.BlockSpec(memory_space=pl.ANY)],
        out_specs=(vmem, vmem),
        scratch_shapes=scratch + sems,
        compiler_params=pltpu.CompilerParams(
            collective_id=0, has_side_effects=True, vmem_limit_bytes=60 * 1024 * 1024
        ),
        name="moe_backward",
    )(tokens, out_grad, gate_prob.reshape(1, tok), routing.reshape(1, tok), expert_weights)
    return pl.pallas_call(
        write_out,
        out_shape=(
            jax.ShapeDtypeStruct((tok, width), BF16),
            jax.ShapeDtypeStruct((1, share, full), F32),
        ),
        in_specs=[pl.BlockSpec(memory_space=pl.ANY)] * 2,
        out_specs=(pl.BlockSpec(memory_space=pl.ANY),) * 2,
        scratch_shapes=[
            pltpu.VMEM((tok, width), BF16),
            pltpu.VMEM((1, share, full), F32),
            dma((2 * PIECES,)),
            dma((2 * PIECES,)),
        ],
        name="write_out",
    )(*early)


def write_out(in_grad_ref, w_grad_ref, in_grad_out, w_grad_out, x_held, w_held, in_s, out_s):
    moves = []
    for p in range(PIECES):
        for src, mid, dst in (
            (in_grad_ref, x_held, in_grad_out),
            (w_grad_ref.at[0], w_held.at[0], w_grad_out.at[0]),
        ):
            rows = src.shape[0] // PIECES
            at = pl.ds(p * rows, rows)
            n = len(moves)
            moves.append(
                (
                    pltpu.make_async_copy(src.at[at], mid.at[at], in_s.at[n]),
                    pltpu.make_async_copy(mid.at[at], dst.at[at], out_s.at[n]),
                )
            )
    for take, _ in moves:
        take.start()
    for take, put in moves:
        take.wait()
        put.start()
    for _, put in moves:
        put.wait()


def solution(mesh):
    tokens_spec = P(("dp", "expert"), None)
    return jax.shard_map(
        functools.partial(local, mesh.shape["expert"], mesh.shape["dp"]),
        mesh=mesh,
        in_specs=(tokens_spec, tokens_spec, tokens_spec, tokens_spec, P("expert", None, None)),
        out_specs=(tokens_spec, P("expert", "dp", None)),
        check_vma=False,
    )
```

```python
import functools
import math
import jax
import jax.numpy as jnp
from jax import lax
from jax.experimental import pallas as pl
from jax.experimental.pallas import tpu as pltpu
from jax.sharding import PartitionSpec as P

MESH = pl.DeviceIdType.MESH
F32 = jnp.float32
BF16 = jnp.bfloat16
SUBS = 2
SLICES = 3
PIECES = 4


def xor(value, step):
    total, bit = 0, 1
    result = value
    while bit <= step:
        if step & bit:
            result = result + bit - 2 * bit * (lax.rem(lax.div(value, bit), 2))
        bit *= 2
    return result


def plan(n_expert, n_dp):
    half, quarter = n_expert // 2, n_expert // 4
    near = list(range(1, half))
    across = list(range(n_expert - 1, half + quarter - 1, -1))
    last = list(range(half + quarter - 1, half - 1, -1))
    chips = n_dp // 2
    side = math.isqrt(chips)
    while chips % side:
        side -= 1
    return near, across, last, chips // side, side


def body(
    n_expert,
    n_dp,
    cap,
    tokens_ref,
    out_grad_ref,
    gate_ref,
    route_ref,
    w_hbm,
    in_grad_ref,
    w_grad_ref,
    w_ref,
    send_x,
    send_g,
    recv_x,
    recv_g,
    ret,
    arrived,
    pair,
    hidden,
    part,
    recv_a,
    send_b,
    recv_b,
    send_c,
    recv_c,
    w_sem,
    dx_s,
    dx_r,
    dg_s,
    dg_r,
    rt_s,
    rt_r,
    a_s,
    a_r,
    b_s,
    b_r,
    c_s,
    c_r,
):
    near, across, last, na, nb = plan(n_expert, n_dp)
    far = across + last
    me = lax.axis_index("expert")
    dp = lax.axis_index("dp")
    tok, width = tokens_ref.shape
    hid = w_ref.shape[1] // 3
    slots = n_expert * cap
    quarter_rows = slots // 4
    share = width // n_dp
    sub = share // SUBS
    grad_scale = float(tok * n_dp) ** (-0.5)
    core = lax.rem(dp, 2)
    chip = lax.div(dp, 2)
    pos_hi, pos_lo = lax.div(chip, na), lax.rem(chip, na)
    if na == nb:
        a = jnp.where(core == 0, pos_lo, pos_hi)
        b = jnp.where(core == 0, pos_hi, pos_lo)
    else:
        a, b = pos_lo, pos_hi

    def chip_of(a_at, b_at):
        plain = b_at * na + a_at
        if na == nb:
            return jnp.where(core == 0, plain, a_at * na + b_at)
        return plain

    def dp_of(a_at, b_at):
        return chip_of(a_at, b_at) * 2 + core

    w_copy = pltpu.make_async_copy(w_hbm.at[0], w_ref, w_sem)
    w_copy.start()

    barrier = pltpu.get_barrier_semaphore()
    partner = dp + 1 - 2 * core
    greeted = 0
    for k in near + far:
        pl.semaphore_signal(barrier, inc=1, device_id={"expert": xor(me, k)}, device_id_type=MESH)
        greeted += 1
    pl.semaphore_signal(barrier, inc=1, device_id={"dp": partner}, device_id_type=MESH)
    greeted += 1
    for s in range(1, na):
        pl.semaphore_signal(
            barrier, inc=1, device_id={"dp": dp_of(lax.rem(a + s, na), b)}, device_id_type=MESH
        )
        greeted += 1
    for t in range(1, nb):
        pl.semaphore_signal(
            barrier, inc=1, device_id={"dp": dp_of(a, lax.rem(b + t, nb))}, device_id_type=MESH
        )
        greeted += 1

    row_i = lax.broadcasted_iota(jnp.int32, (tok, tok), 0)
    col_i = lax.broadcasted_iota(jnp.int32, (tok, tok), 1)

    def column(row):
        return jnp.sum(jnp.where(row_i == col_i, row, 0.0), axis=1, keepdims=True)

    route_row = route_ref[...].astype(F32)
    route_col = column(route_row)
    same = route_col == route_row
    pos_row = jnp.sum(jnp.where(same & (row_i < col_i), 1.0, 0.0), axis=0, keepdims=True)
    pos_col = jnp.sum(jnp.where(same & (col_i < row_i), 1.0, 0.0), axis=1, keepdims=True)
    slot_row = route_row * cap + pos_row
    slot_col = route_col * cap + pos_col
    slot_at = lax.broadcasted_iota(jnp.int32, (slots, tok), 0).astype(F32)
    table = jnp.where(slot_at == slot_row, 1.0, 0.0).astype(BF16)
    slot_of = lax.broadcasted_iota(jnp.int32, (tok, slots), 1).astype(F32)
    table_t = jnp.where(slot_of == slot_col, 1.0, 0.0).astype(BF16)

    send_x[...] = jnp.dot(table, tokens_ref[...], preferred_element_type=F32).astype(BF16)
    scaled = (column(gate_ref[...]) * out_grad_ref[...].astype(F32)).astype(BF16)
    send_g[...] = jnp.dot(table, scaled, preferred_element_type=F32).astype(BF16)

    def rows_of(index):
        return pl.ds(pl.multiple_of(index * cap, cap), cap)

    pl.semaphore_wait(barrier, greeted)

    def dispatch(k, src, dst, s_sem, r_sem):
        peer = xor(me, k)
        return pltpu.make_async_remote_copy(
            src_ref=src.at[rows_of(peer)],
            dst_ref=dst.at[rows_of(me)],
            send_sem=s_sem.at[k],
            recv_sem=r_sem.at[k],
            device_id={"expert": peer},
            device_id_type=MESH,
        )

    x_copies = {k: dispatch(k, send_x, recv_x, dx_s, dx_r) for k in near + far}
    g_copies = {k: dispatch(k, send_g, recv_g, dg_s, dg_r) for k in near + far}
    returns = {k: dispatch(k, ret, arrived, rt_s, rt_r) for k in near + far}
    for k in near + far:
        x_copies[k].start()
        g_copies[k].start()

    recv_x[rows_of(me)] = send_x[rows_of(me)]
    recv_g[rows_of(me)] = send_g[rows_of(me)]
    w_copy.wait()

    mine = lax.div(me, n_expert // 4)

    def forward(start, size):
        rows = pl.ds(pl.multiple_of(start, cap), size)
        x = recv_x[rows]
        pre_gate = jnp.dot(x, w_ref[:, :hid], preferred_element_type=F32)
        pre_up = jnp.dot(x, w_ref[:, hid : 2 * hid], preferred_element_type=F32)
        grad_hidden = jnp.dot(recv_g[rows], w_ref[:, 2 * hid :], preferred_element_type=F32)
        sig = jax.nn.sigmoid(pre_gate)
        active = pre_gate * sig
        hidden[rows] = (active * pre_up).astype(BF16)
        grad_gate = grad_hidden * pre_up * (sig * (1.0 + pre_gate * (1.0 - sig)))
        pair[rows, :hid] = grad_gate.astype(BF16)
        pair[rows, hid:] = (grad_hidden * active).astype(BF16)

    def backward(start, size):
        rows = pl.ds(pl.multiple_of(start, cap), size)
        tile = min(512, width)

        @pl.loop(0, width // tile)
        def _(j):
            at = pl.ds(pl.multiple_of(j * tile, tile), tile)
            ret[rows, at] = lax.dot_general(
                pair[rows],
                w_ref[at, : 2 * hid],
                (((1,), (1,)), ((), ())),
                preferred_element_type=F32,
            ).astype(BF16)

    near_half = (lax.div(mine, 2) * 2 * quarter_rows, 2 * quarter_rows)
    across_quarter = (xor(mine, 3) * quarter_rows, quarter_rows)
    last_quarter = (xor(mine, 2) * quarter_rows, quarter_rows)
    for k in near:
        x_copies[k].wait_recv()
        g_copies[k].wait_recv()
    forward(*near_half)
    backward(*near_half)
    for k in near:
        returns[k].start()
    arrived[rows_of(me)] = ret[rows_of(me)]
    for k in across:
        x_copies[k].wait_recv()
        g_copies[k].wait_recv()
    forward(*across_quarter)
    backward(*across_quarter)
    for k in last:
        x_copies[k].wait_recv()
        g_copies[k].wait_recv()
    for k in across:
        returns[k].start()
    forward(*last_quarter)

    def weight_rows(start, size):
        at = pl.ds(pl.multiple_of(start, size), size)
        contract = (((0,), (0,)), ((), ()))
        part[at, : 2 * hid] = (
            grad_scale
            * lax.dot_general(recv_x[:, at], pair[...], contract, preferred_element_type=F32)
        ).astype(BF16)
        part[at, 2 * hid :] = (
            grad_scale
            * lax.dot_general(recv_g[:, at], hidden[...], contract, preferred_element_type=F32)
        ).astype(BF16)

    def band(chip_at, core_at, g):
        return pl.ds(pl.multiple_of((chip_at * 2 + core_at) * share + g * sub, sub), sub)

    bands = [(s, t) for s in range(1, na) for t in list(range(1, nb)) + [0]]
    bands += [(0, t) for t in list(range(1, nb)) + [0]]
    items = [(s, t, g) for s, t in bands for g in range(SUBS)]

    def item_chip(s, t):
        return chip_of(lax.rem(a + s, na), lax.rem(b + t, nb))

    banded = share % 128 == 0
    if not banded:

        @pl.loop(0, width // 256)
        def _(j):
            weight_rows(j * 256, 256)

    def pair_copy(index, chip_at, g):
        rows = band(chip_at, 1 - core, g)
        return pltpu.make_async_remote_copy(
            src_ref=part.at[rows],
            dst_ref=recv_a.at[pl.ds(pl.multiple_of(chip_at * share + g * sub, sub), sub)],
            send_sem=a_s.at[index],
            recv_sem=a_r.at[index],
            device_id={"dp": partner},
            device_id_type=MESH,
        )

    def partner_chip(s, t):
        if na == nb:
            a_at, b_at = lax.rem(b + s, na), lax.rem(a + t, nb)
            return jnp.where(core == 1, b_at * na + a_at, a_at * na + b_at)
        return item_chip(s, t)

    a_copies = []
    for index, (s, t, g) in enumerate(items):
        chip_at = partner_chip(s, t)
        if banded and g == 0:
            weight_rows((chip_at * 2 + 1 - core) * share, share)
        copy = pair_copy(index, chip_at, g)
        copy.start()
        a_copies.append(copy)

    backward(*last_quarter)
    for k in last:
        returns[k].start()

    def pair_sum(index, s, t, g):
        chip_at = item_chip(s, t)
        a_copies[index].wait_recv()
        return (
            part[band(chip_at, core, g)].astype(F32)
            + recv_a[pl.ds(pl.multiple_of(chip_at * share + g * sub, sub), sub)].astype(F32)
        )

    if banded:
        for s, t in bands:
            weight_rows((item_chip(s, t) * 2 + core) * share, share)

    b_copies = {}
    for index, (s, t, g) in enumerate(items):
        if s == 0:
            continue
        at = ((s - 1) * nb + t) * SUBS + g
        send_b[at] = pair_sum(index, s, t, g).astype(BF16)
        copy = pltpu.make_async_remote_copy(
            src_ref=send_b.at[at],
            dst_ref=recv_b.at[at],
            send_sem=b_s.at[at],
            recv_sem=b_r.at[at],
            device_id={"dp": dp_of(lax.rem(a + s, na), b)},
            device_id_type=MESH,
        )
        copy.start()
        b_copies[s, t, g] = copy
    c_copies = {}
    for index, (s, t, g) in enumerate(items):
        if s > 0:
            continue
        total = pair_sum(index, s, t, g)
        for s_from in range(1, na):
            b_copies[s_from, t, g].wait_recv()
            total = total + recv_b[((s_from - 1) * nb + t) * SUBS + g].astype(F32)
        if t > 0:
            at = (t - 1) * SUBS + g
            send_c[at] = total.astype(BF16)
            copy = pltpu.make_async_remote_copy(
                src_ref=send_c.at[at],
                dst_ref=recv_c.at[at],
                send_sem=c_s.at[at],
                recv_sem=c_r.at[at],
                device_id={"dp": dp_of(a, lax.rem(b + t, nb))},
                device_id_type=MESH,
            )
            copy.start()
            c_copies[t, g] = copy
        else:
            w_grad_ref[0, pl.ds(g * sub, sub)] = total
    for t in range(1, nb):
        for g in range(SUBS):
            c_copies[t, g].wait_recv()
            w_grad_ref[0, pl.ds(g * sub, sub)] += recv_c[(t - 1) * SUBS + g].astype(F32)

    for k in near + far:
        returns[k].wait_recv()
    in_grad_ref[...] = jnp.dot(table_t, arrived[...], preferred_element_type=F32).astype(BF16)

    for k in near + far:
        x_copies[k].wait_send()
        g_copies[k].wait_send()
        returns[k].wait_send()
    for copy in a_copies + list(b_copies.values()) + list(c_copies.values()):
        copy.wait_send()


def paired(width, hid, n_expert, n_dp):
    chips_a, chips_b = plan(n_expert, n_dp)[3:]
    return n_expert == 4 and chips_a == chips_b == 2 and width % (128 * n_dp) == hid % (128 * SLICES) == 0


def paired_body(
    n_expert,
    n_dp,
    cap,
    tokens_hbm,
    out_grad_hbm,
    gate_hbm,
    route_hbm,
    w_hbm,
    in_grad_ref,
    w_grad_ref,
    w_ref,
    w2_ref,
    send_x,
    send_g,
    recv_x,
    recv_g,
    ret,
    arrived,
    pair,
    hidden,
    part,
    recv_a,
    send_b,
    recv_b,
    send_c,
    recv_c,
    stage,
    band_x,
    band_g,
    terms,
    held_d,
    send_d,
    near_d,
    far_d,
    tokens_ref,
    out_grad_ref,
    gate_ref,
    route_ref,
    w_sem,
    in_sem,
    st_sem,
    to_s,
    near_r,
    cross_r,
    rt_s,
    rt_r,
    a_s,
    a_r,
    b_s,
    b_r,
    c_s,
    c_r,
    bd_s,
    bd_r,
    tm_s,
    tm_r,
    fw_s,
    fw_r,
    w_s,
    w_r,
    ag_s,
    ag_r,
    rl_r,
    pf_s,
    pf_r,
    d_s,
    d_r,
):
    _, _, _, na, nb = plan(n_expert, n_dp)
    chips = na * nb
    me = lax.axis_index("expert")
    dp = lax.axis_index("dp")
    half = lax.div(me, 2)
    inner = (me == 1) | (me == n_expert - 2)
    outer = jnp.logical_not(inner)
    near = me + 1 - 2 * lax.rem(me, 2)
    mirror = n_expert - 1 - me
    inner_far = 2 - half
    outer_far = 3 - 3 * half
    tok, width = tokens_hbm.shape
    hid = w_ref.shape[1] // 3
    slots = n_expert * cap
    share = width // n_dp
    sub = share // SUBS
    grad_scale = float(tok * n_dp) ** (-0.5)
    core = lax.rem(dp, 2)
    chip = lax.div(dp, 2)
    partner = dp + 1 - 2 * core
    pos_hi, pos_lo = lax.div(chip, na), lax.rem(chip, na)
    if na == nb:
        a = jnp.where(core == 0, pos_lo, pos_hi)
        b = jnp.where(core == 0, pos_hi, pos_lo)
    else:
        a, b = pos_lo, pos_hi

    def chip_of(a_at, b_at):
        plain = b_at * na + a_at
        if na == nb:
            return jnp.where(core == 0, plain, a_at * na + b_at)
        return plain

    def dp_of(a_at, b_at):
        return chip_of(a_at, b_at) * 2 + core

    def columns_of(index):
        return pl.ds(pl.multiple_of(index * share, share), share)

    w_copy = pltpu.make_async_copy(w_hbm.at[0], w_ref, w_sem)
    slices = w2_ref.shape[0]
    unit = hid // slices

    def stage_copy(q, third):
        return pltpu.make_async_copy(
            w_hbm.at[0, columns_of(dp), pl.ds(third * hid + q * unit, unit)],
            stage.at[q, :, pl.ds(third * unit, unit)],
            st_sem.at[q],
        )

    barrier = pltpu.get_barrier_semaphore()
    for k in range(1, n_expert):
        peer = lax.rem(me + k, n_expert)
        pl.semaphore_signal(barrier, inc=1, device_id={"expert": peer}, device_id_type=MESH)
    for j in range(1, n_dp):
        peer = lax.rem(dp + j, n_dp)
        pl.semaphore_signal(barrier, inc=1, device_id={"dp": peer}, device_id_type=MESH)

    @pl.when(outer)
    def _():
        for q in range(slices):
            for third in range(3):
                stage_copy(q, third).start()

    loads = [
        pltpu.make_async_copy(src, dst, in_sem.at[n])
        for n, (src, dst) in enumerate(
            (
                (route_hbm, route_ref),
                (gate_hbm, gate_ref),
                (tokens_hbm, tokens_ref),
                (out_grad_hbm, out_grad_ref),
            )
        )
    ]
    for load in loads:
        load.start()
    w_copy.start()

    def rows_of(index):
        return pl.ds(index * cap, cap)

    kept = rows_of(3)

    def rows_from(index):
        return pl.ds(pl.multiple_of(index * cap, cap), cap)

    def remote(src, dst, s_sem, r_sem, device):
        return pltpu.make_async_remote_copy(
            src_ref=src,
            dst_ref=dst,
            send_sem=s_sem,
            recv_sem=r_sem,
            device_id=device,
            device_id_type=MESH,
        )

    pl.semaphore_wait(barrier, n_expert - 1 + n_dp - 1)

    def weight_out(q):
        dst = w2_ref.at[q, columns_of(dp)]
        return remote(stage.at[q], dst, w_s, w_r.at[q], {"expert": inner_far})

    @pl.when(outer)
    def _():
        for q in range(slices):
            pltpu.make_async_copy(stage.at[q], stage.at[q], st_sem.at[q]).wait()
            weight_out(q).start()

    row_i = lax.broadcasted_iota(jnp.int32, (tok, tok), 0)
    col_i = lax.broadcasted_iota(jnp.int32, (tok, tok), 1)

    def column(row):
        return jnp.sum(jnp.where(row_i == col_i, row, 0.0), axis=1, keepdims=True)

    loads[0].wait()
    route = route_ref[...]
    block = jnp.where(route == near, 1, jnp.where(route == inner_far, 2, 3))
    route_row = jnp.where(route == me, 0, block).astype(F32)
    route_col = column(route_row)
    same = route_col == route_row
    pos_row = jnp.sum(jnp.where(same & (row_i < col_i), 1.0, 0.0), axis=0, keepdims=True)
    pos_col = jnp.sum(jnp.where(same & (col_i < row_i), 1.0, 0.0), axis=1, keepdims=True)
    slot_row = route_row * cap + pos_row
    slot_col = route_col * cap + pos_col
    slot_at = lax.broadcasted_iota(jnp.int32, (slots, tok), 0).astype(F32)
    table = jnp.where(slot_at == slot_row, 1.0, 0.0).astype(BF16)
    slot_of = lax.broadcasted_iota(jnp.int32, (tok, slots), 1).astype(F32)
    table_t = jnp.where(slot_of == slot_col, 1.0, 0.0).astype(BF16)

    loads[2].wait()
    send_x[...] = jnp.dot(table, tokens_ref[...], preferred_element_type=F32).astype(BF16)
    loads[1].wait()
    loads[3].wait()
    scaled = (column(gate_ref[...]) * out_grad_ref[...].astype(F32)).astype(BF16)
    send_g[...] = jnp.dot(table, scaled, preferred_element_type=F32).astype(BF16)

    def run(is_inner):
        cross_at = 2 if is_inner else 3

        def near_copy(src, dst):
            return remote(
                src.at[rows_of(1)], dst.at[rows_of(1)], to_s, near_r, {"expert": near}
            )

        def cross_copy(src, dst):
            return remote(
                src.at[rows_of(2)],
                dst.at[rows_of(cross_at)],
                to_s,
                cross_r.at[cross_at - 2],
                {"expert": inner_far},
            )

        def bytes_of(ref, s_sem, r_sem):
            return remote(ref, ref, s_sem, r_sem, {"expert": near})

        both = pl.ds(0, 2 * cap)
        x_args = (send_x, recv_x)
        g_args = (send_g, recv_g)

        def return_copy(index):
            peer = {1: near, 2: mirror, 3: outer_far}[index]
            home = rows_of(min(index, 2))
            return remote(
                ret.at[rows_of(index)],
                arrived.at[home],
                rt_s,
                rt_r,
                {"expert": peer},
            )

        first = jnp.where(core == 0, 1, 2)

        def beside(c):
            return xor(chip, c)

        chip_first = jnp.where(core == 0, beside(1), beside(2))
        chip_second = jnp.where(core == 0, beside(2), beside(1))

        def weight_on(q):
            at = w2_ref.at[q, columns_of(dp)]
            return remote(at, at, w_s, w_r.at[q], {"expert": near})

        def spread(c, q):
            at = w2_ref.at[q, columns_of(dp)]
            return remote(at, at, ag_s, ag_r.at[q], {"dp": beside(c) * 2 + core})

        def relay(q):
            at = w2_ref.at[q, columns_of(chip_first * 2 + core)]
            return remote(at, at, ag_s, rl_r.at[q], {"dp": chip_second * 2 + core})

        def hand_over(c, q):
            at = w2_ref.at[q, columns_of(beside(c) * 2 + core)]
            return remote(at, at, pf_s, pf_r.at[q], {"dp": partner})

        def band_copy(j, src, dst):
            peer = lax.rem(dp + j, n_dp)
            return remote(
                src.at[kept, columns_of(peer)], dst.at[rows_from(dp)], bd_s, bd_r, {"dp": peer}
            )

        bands_in = bytes_of(recv_x.at[pl.ds(0, 2 * (n_dp - 1) * cap // n_dp)], bd_s, bd_r)

        def term_copy(c, q):
            at = terms.at[q, rows_from(dp)]
            return remote(at, at, tm_s, tm_r.at[q], {"dp": beside(c) * 2 + core})

        def term_over(c, q):
            at = terms.at[q, rows_from(beside(c) * 2 + core)]
            return remote(at, at, fw_s, fw_r.at[q], {"dp": partner})

        near_copy(*x_args).start()
        if not is_inner:
            near_copy(*g_args).start()
        cross_copy(*x_args).start()
        cross_copy(*g_args).start()
        for j in range(1, n_dp):
            band_copy(j, send_x, band_x).start()
            band_copy(j, send_g, band_g).start()

        recv_x[rows_of(0)] = send_x[rows_of(0)]
        recv_g[rows_of(0)] = send_g[rows_of(0)]
        band_x[rows_from(dp)] = send_x[kept, columns_of(dp)]
        band_g[rows_from(dp)] = send_g[kept, columns_of(dp)]

        def forward(x, g, weights):
            third = weights.shape[1] // 3
            pre_gate = jnp.dot(x, weights[:, :third], preferred_element_type=F32)
            pre_up = jnp.dot(x, weights[:, third : 2 * third], preferred_element_type=F32)
            grad_hidden = jnp.dot(g, weights[:, 2 * third :], preferred_element_type=F32)
            sig = jax.nn.sigmoid(pre_gate)
            active = pre_gate * sig
            grad_gate = grad_hidden * pre_up * (sig * (1.0 + pre_gate * (1.0 - sig)))
            return (
                grad_gate.astype(BF16),
                (grad_hidden * active).astype(BF16),
                (active * pre_up).astype(BF16),
            )

        def forward_rows(start, size):
            rows = pl.ds(start, size)
            grad_gate, grad_up, kept_hidden = forward(recv_x[rows], recv_g[rows], w_ref)
            pair[rows, :hid] = grad_gate
            pair[rows, hid:] = grad_up
            hidden[rows] = kept_hidden

        def columns(pieces, dst, rows):
            tile = min(512, width)

            @pl.loop(0, width // tile)
            def _(j):
                at = pl.ds(pl.multiple_of(j * tile, tile), tile)
                total = 0.0
                for grads, weights in pieces:
                    total = total + lax.dot_general(
                        grads(), weights(at), (((1,), (1,)), ((), ())), preferred_element_type=F32
                    )
                dst[rows, at] = total.astype(BF16)

        def backward_rows(start, size):
            rows = pl.ds(start, size)
            columns([(lambda: pair[rows], lambda at: w_ref[at, : 2 * hid])], ret, rows)

        contract = (((0,), (0,)), ((), ()))
        mine = rows_from(dp)

        def kept_forward(q):
            grad_gate, grad_up, kept_hidden = forward(send_x[kept], send_g[kept], w2_ref.at[q])
            terms[q, mine, :unit] = grad_gate
            terms[q, mine, unit : 2 * unit] = grad_up
            terms[q, mine, 2 * unit :] = kept_hidden

        def kept_grad(q):
            first = lax.dot_general(
                band_x[...], terms[q, :, : 2 * unit], contract, preferred_element_type=F32
            )
            second = lax.dot_general(
                band_g[...], terms[q, :, 2 * unit :], contract, preferred_element_type=F32
            )
            return grad_scale * jnp.concatenate([first, second], axis=1)

        def near_hop(q):
            return remote(send_d.at[q], near_d.at[q], d_s, d_r.at[q], {"expert": near})

        def far_hop(q):
            return remote(send_d.at[q], far_d.at[q], d_s, d_r.at[q], {"expert": outer_far})

        def take(q):
            weight_on(q).wait_recv()
            if is_inner:
                weight_on(q).start()
            for c in (1, 2):
                spread(c, q).start()
            hand_over(0, q).start()

        def pass_on(q):
            bytes_of(w2_ref.at[q, pl.ds(0, 2 * share)], ag_s, ag_r.at[q]).wait_recv()
            relay(q).start()
            for c in (1, 2):
                hand_over(c, q).start()

        def pass_last(q):
            relay(q).wait_recv()
            hand_over(3, q).start()

        def kept_terms(q):
            bytes_of(w2_ref.at[q, pl.ds(0, 4 * share)], pf_s, pf_r.at[q]).wait_recv()
            kept_forward(q)
            for c in range(1, 4):
                term_copy(c, q).start()
            term_over(0, q).start()

        def pass_terms(q):
            bytes_of(terms.at[q, pl.ds(0, 3 * cap)], tm_s, tm_r.at[q]).wait_recv()
            for c in range(1, 4):
                term_over(c, q).start()

        def kept_band(q):
            if q == 0:
                bands_in.wait_recv()
            bytes_of(terms.at[q, pl.ds(0, 4 * cap)], fw_s, fw_r.at[q]).wait_recv()
            held_d[q] = kept_grad(q)
            if not is_inner:
                send_d[q] = held_d[q].astype(BF16)
                near_hop(q).start()

        def own_rows():
            w_copy.wait()
            forward_rows(0, cap)
            backward_rows(0, cap)
            arrived[rows_of(0)] = ret[rows_of(0)]

        def near_forward():
            bytes_of(recv_x.at[both], to_s, near_r).wait_recv()
            forward_rows(cap, cap)

        def near_backward():
            backward_rows(cap, cap)
            return_copy(1).start()

        def cross_forward(index):
            bytes_of(recv_x.at[both], to_s, cross_r.at[index - 2]).wait_recv()
            forward_rows(index * cap, cap)

        def cross_backward(index):
            backward_rows(index * cap, cap)
            return_copy(index).start()

        def kept_backward():
            pieces = [
                (lambda q=q: terms[q, mine, : 2 * unit], lambda at, q=q: w2_ref[q, at, : 2 * unit])
                for q in range(slices)
            ]
            columns(pieces, arrived, kept)

        def add_hop(q):
            near_hop(q).wait_recv()
            send_d[q] = (held_d[q] + near_d[q].astype(F32)).astype(BF16)
            far_hop(q).start()

        rows_in = slots if is_inner else 2 * cap

        def weight_rows(start, size):
            at = pl.ds(pl.multiple_of(start, size), size)
            part[at, : 2 * hid] = (
                grad_scale
                * lax.dot_general(
                    recv_x[:rows_in, at], pair[:rows_in], contract, preferred_element_type=F32
                )
            ).astype(BF16)
            part[at, 2 * hid :] = (
                grad_scale
                * lax.dot_general(
                    recv_g[:rows_in, at], hidden[:rows_in], contract, preferred_element_type=F32
                )
            ).astype(BF16)

        def band(chip_at, core_at, g):
            return pl.ds(pl.multiple_of((chip_at * 2 + core_at) * share + g * sub, sub), sub)

        bands = [(s, t) for s in range(1, na) for t in list(range(1, nb)) + [0]]
        bands += [(0, t) for t in list(range(1, nb)) + [0]]
        items = [(s, t, g) for s, t in bands for g in range(SUBS)]

        def item_chip(s, t):
            return chip_of(lax.rem(a + s, na), lax.rem(b + t, nb))

        def pair_copy(index, chip_at, g):
            return remote(
                part.at[band(chip_at, 1 - core, g)],
                recv_a.at[pl.ds(pl.multiple_of(chip_at * share + g * sub, sub), sub)],
                a_s,
                a_r.at[index],
                {"dp": partner},
            )

        def partner_chip(s, t):
            if na == nb:
                a_at, b_at = lax.rem(b + s, na), lax.rem(a + t, nb)
                return jnp.where(core == 1, b_at * na + a_at, a_at * na + b_at)
            return item_chip(s, t)

        def item_pair(index):
            s, t, g = items[index]
            return pair_copy(index, partner_chip(s, t), g)

        def item_out(s, t, g):
            at = ((s - 1) * nb + t) * SUBS + g
            to = dp_of(lax.rem(a + s, na), b)
            return remote(send_b.at[at], recv_b.at[at], b_s, b_r.at[at], {"dp": to})

        def item_last(t, g):
            at = (t - 1) * SUBS + g
            to = dp_of(a, lax.rem(b + t, nb))
            return remote(send_c.at[at], recv_c.at[at], c_s, c_r.at[at], {"dp": to})

        def pair_sum(index):
            s, t, g = items[index]
            chip_to = item_chip(s, t)
            item_pair(index).wait_recv()
            return (
                part[band(chip_to, core, g)].astype(F32)
                + recv_a[pl.ds(pl.multiple_of(chip_to * share + g * sub, sub), sub)].astype(F32)
            )

        def reduce_pair():
            for index, (s, t, g) in enumerate(items):
                if g == 0:
                    weight_rows((partner_chip(s, t) * 2 + 1 - core) * share, share)
                item_pair(index).start()

        def reduce_first():
            for index, (s, t, g) in enumerate(items):
                if g == 0:
                    weight_rows((item_chip(s, t) * 2 + core) * share, share)
                if s > 0:
                    send_b[((s - 1) * nb + t) * SUBS + g] = pair_sum(index).astype(BF16)
                    item_out(s, t, g).start()

        def item_total(index):
            s, t, g = items[index]
            total = pair_sum(index)
            for s_from in range(1, na):
                item_out(s_from, t, g).wait_recv()
                total = total + recv_b[((s_from - 1) * nb + t) * SUBS + g].astype(F32)
            return total

        def reduce_second():
            for index, (s, t, g) in enumerate(items):
                if s == 0 and t > 0:
                    send_c[(t - 1) * SUBS + g] = item_total(index).astype(BF16)
                    item_last(t, g).start()

        def reduce_own():
            for index, (s, t, g) in enumerate(items):
                if s == t == 0:
                    w_grad_ref[0, pl.ds(g * sub, sub)] = item_total(index)
            for t in range(1, nb):
                for g in range(SUBS):
                    item_last(t, g).wait_recv()
                    w_grad_ref[0, pl.ds(g * sub, sub)] += recv_c[(t - 1) * SUBS + g].astype(F32)

        def add_far(q):
            far_hop(q).wait_recv()
            for third in range(3):
                at = pl.ds(third * hid + q * unit, unit)
                w_grad_ref[0, :, at] += far_d[q, :, third * unit : (third + 1) * unit].astype(F32)

        own_rows()
        take(0)
        take(1)
        pass_on(0)
        take(2)
        if is_inner:
            near_copy(*g_args).start()
        pass_on(1)
        pass_last(0)
        kept_terms(0)
        pass_on(2)
        if is_inner:
            pass_last(1)
            kept_terms(1)
            pass_terms(0)
            pass_last(2)
            kept_terms(2)
            near_forward()
            near_backward()
            cross_forward(2)
            cross_backward(2)
            pass_terms(1)
            pass_terms(2)
            cross_forward(3)
            reduce_pair()
            reduce_first()
            kept_band(0)
            add_hop(0)
            kept_band(1)
            add_hop(1)
            cross_backward(3)
            reduce_second()
            kept_band(2)
            add_hop(2)
            kept_backward()
            reduce_own()
        else:
            near_forward()
            pass_last(1)
            kept_terms(1)
            pass_terms(0)
            reduce_pair()
            kept_band(0)
            pass_last(2)
            kept_terms(2)
            pass_terms(1)
            kept_band(1)
            reduce_first()
            pass_terms(2)
            kept_band(2)
            near_backward()
            kept_backward()
            reduce_second()
            reduce_own()
            for q in range(slices):
                add_far(q)

        bytes_of(arrived.at[both], rt_s, rt_r).wait_recv()
        in_grad_ref[...] = jnp.dot(table_t, arrived[...], preferred_element_type=F32).astype(BF16)

        bytes_of(send_x, to_s, near_r).wait_send()
        bands_in.wait_send()
        bytes_of(terms.at[:, pl.ds(0, 3 * cap)], tm_s, tm_r.at[0]).wait_send()
        bytes_of(terms.at[:, pl.ds(0, 4 * cap)], fw_s, fw_r.at[0]).wait_send()
        bytes_of(w2_ref.at[:, pl.ds(0, 3 * share)], ag_s, ag_r.at[0]).wait_send()
        bytes_of(w2_ref.at[:, pl.ds(0, 4 * share)], pf_s, pf_r.at[0]).wait_send()
        bytes_of(stage, w_s, w_r.at[0]).wait_send()
        bytes_of(send_d, d_s, d_r.at[0]).wait_send()
        bytes_of(ret.at[pl.ds(0, (3 if is_inner else 1) * cap)], rt_s, rt_r).wait_send()
        bytes_of(recv_a, a_s, a_r.at[0]).wait_send()
        bytes_of(send_b, b_s, b_r.at[0]).wait_send()
        bytes_of(send_c, c_s, c_r.at[0]).wait_send()

    pl.when(inner)(lambda: run(True))
    pl.when(outer)(lambda: run(False))


def local(n_expert, n_dp, tokens, out_grad, gate_prob, routing, expert_weights):
    tok, width = tokens.shape
    full = expert_weights.shape[2]
    hid = full // 3
    cap = max(16, 2 * tok // n_expert)
    slots = n_expert * cap
    share = width // n_dp
    _, _, _, na, nb = plan(n_expert, n_dp)
    sub = share // SUBS
    chips = na * nb
    n_b, n_c = max(1, (na - 1) * nb) * SUBS, max(1, nb - 1) * SUBS
    dma = pltpu.SemaphoreType.DMA
    vmem = pl.BlockSpec(memory_space=pltpu.VMEM)
    weights, rows = pltpu.VMEM((width, full), BF16), pltpu.VMEM((slots, width), BF16)
    scratch = [weights] + [rows] * 6
    scratch += [
        pltpu.VMEM((slots, 2 * hid), BF16),
        pltpu.VMEM((slots, hid), BF16),
        pltpu.VMEM((width, full), BF16),
        pltpu.VMEM((chips * share, full), BF16),
        pltpu.VMEM((n_b, sub, full), BF16),
        pltpu.VMEM((n_b, sub, full), BF16),
        pltpu.VMEM((n_c, sub, full), BF16),
        pltpu.VMEM((n_c, sub, full), BF16),
    ]
    sems = [dma] + [dma((n_expert,))] * 6 + [dma((chips * SUBS,))] * 2
    sems += [dma((n_b,))] * 2 + [dma((n_c,))] * 2
    kernel, ins = body, [vmem] * 4
    if paired(width, hid, n_expert, n_dp):
        kernel = paired_body
        slices, third = SLICES, full // SLICES
        scratch.insert(1, pltpu.VMEM((slices, width, third), BF16))
        scratch += [pltpu.VMEM((slices, share, third), BF16)]
        scratch += [pltpu.VMEM((n_dp * cap, share), BF16)] * 2
        scratch += [pltpu.VMEM((slices, n_dp * cap, third), BF16)]
        scratch += [pltpu.VMEM((slices, share, third), F32)]
        scratch += [pltpu.VMEM((slices, share, third), BF16)] * 3
        scratch += [pltpu.VMEM((tok, width), BF16)] * 2
        scratch += [pltpu.VMEM((1, tok), F32), pltpu.VMEM((1, tok), jnp.int32)]
        each = dma((slices,))
        sems = [dma, dma((4,)), each, dma, dma, dma((2,)), dma, dma]
        sems += [dma, dma((chips * SUBS,)), dma, dma((n_b,)), dma, dma((n_c,)), dma, dma]
        sems += [dma, each] * 3 + [dma, each, each] + [dma, each] * 2
        ins = [pl.BlockSpec(memory_space=pl.ANY)] * 4
    early = pl.pallas_call(
        functools.partial(kernel, n_expert, n_dp, cap),
        out_shape=(pltpu.VMEM((tok, width), BF16), pltpu.VMEM((1, share, full), F32)),
        in_specs=ins + [pl.BlockSpec(memory_space=pl.ANY)],
        out_specs=(vmem, vmem),
        scratch_shapes=scratch + sems,
        compiler_params=pltpu.CompilerParams(
            collective_id=0, has_side_effects=True, vmem_limit_bytes=60 * 1024 * 1024
        ),
        name="moe_backward",
    )(tokens, out_grad, gate_prob.reshape(1, tok), routing.reshape(1, tok), expert_weights)
    return pl.pallas_call(
        write_out,
        out_shape=(
            jax.ShapeDtypeStruct((tok, width), BF16),
            jax.ShapeDtypeStruct((1, share, full), F32),
        ),
        in_specs=[vmem] * 2,
        out_specs=(pl.BlockSpec(memory_space=pl.ANY),) * 2,
        scratch_shapes=[dma((2,))],
        name="write_out",
    )(*[pltpu.with_memory_space_constraint(value, pltpu.VMEM) for value in early])


def write_out(in_grad_ref, w_grad_ref, in_grad_out, w_grad_out, sem):
    moves = [
        pltpu.make_async_copy(in_grad_ref, in_grad_out, sem.at[0]),
        pltpu.make_async_copy(w_grad_ref, w_grad_out, sem.at[1]),
    ]
    for move in moves:
        move.start()
    for move in moves:
        move.wait()


def solution(mesh):
    tokens_spec = P(("dp", "expert"), None)
    return jax.shard_map(
        functools.partial(local, mesh.shape["expert"], mesh.shape["dp"]),
        mesh=mesh,
        in_specs=(tokens_spec, tokens_spec, tokens_spec, tokens_spec, P("expert", None, None)),
        out_specs=(tokens_spec, P("expert", "dp", None)),
        check_vma=False,
    )
```

```python
import functools
import math
import jax
import jax.numpy as jnp
from jax import lax
from jax.experimental import pallas as pl
from jax.experimental.pallas import tpu as pltpu
from jax.sharding import PartitionSpec as P

MESH = pl.DeviceIdType.MESH
F32 = jnp.float32
BF16 = jnp.bfloat16
SUBS = 2
SLICES = 3
PIECES = 4


def xor(value, step):
    total, bit = 0, 1
    result = value
    while bit <= step:
        if step & bit:
            result = result + bit - 2 * bit * (lax.rem(lax.div(value, bit), 2))
        bit *= 2
    return result


def plan(n_expert, n_dp):
    half, quarter = n_expert // 2, n_expert // 4
    near = list(range(1, half))
    across = list(range(n_expert - 1, half + quarter - 1, -1))
    last = list(range(half + quarter - 1, half - 1, -1))
    chips = n_dp // 2
    side = math.isqrt(chips)
    while chips % side:
        side -= 1
    return near, across, last, chips // side, side


def body(
    n_expert,
    n_dp,
    cap,
    tokens_ref,
    out_grad_ref,
    gate_ref,
    route_ref,
    w_hbm,
    in_grad_ref,
    w_grad_ref,
    w_ref,
    send_x,
    send_g,
    recv_x,
    recv_g,
    ret,
    arrived,
    pair,
    hidden,
    part,
    recv_a,
    send_b,
    recv_b,
    send_c,
    recv_c,
    w_sem,
    dx_s,
    dx_r,
    dg_s,
    dg_r,
    rt_s,
    rt_r,
    a_s,
    a_r,
    b_s,
    b_r,
    c_s,
    c_r,
):
    near, across, last, na, nb = plan(n_expert, n_dp)
    far = across + last
    me = lax.axis_index("expert")
    dp = lax.axis_index("dp")
    tok, width = tokens_ref.shape
    hid = w_ref.shape[1] // 3
    slots = n_expert * cap
    quarter_rows = slots // 4
    share = width // n_dp
    sub = share // SUBS
    grad_scale = float(tok * n_dp) ** (-0.5)
    core = lax.rem(dp, 2)
    chip = lax.div(dp, 2)
    pos_hi, pos_lo = lax.div(chip, na), lax.rem(chip, na)
    if na == nb:
        a = jnp.where(core == 0, pos_lo, pos_hi)
        b = jnp.where(core == 0, pos_hi, pos_lo)
    else:
        a, b = pos_lo, pos_hi

    def chip_of(a_at, b_at):
        plain = b_at * na + a_at
        if na == nb:
            return jnp.where(core == 0, plain, a_at * na + b_at)
        return plain

    def dp_of(a_at, b_at):
        return chip_of(a_at, b_at) * 2 + core

    w_copy = pltpu.make_async_copy(w_hbm.at[0], w_ref, w_sem)
    w_copy.start()

    barrier = pltpu.get_barrier_semaphore()
    partner = dp + 1 - 2 * core
    greeted = 0
    for k in near + far:
        pl.semaphore_signal(barrier, inc=1, device_id={"expert": xor(me, k)}, device_id_type=MESH)
        greeted += 1
    pl.semaphore_signal(barrier, inc=1, device_id={"dp": partner}, device_id_type=MESH)
    greeted += 1
    for s in range(1, na):
        pl.semaphore_signal(
            barrier, inc=1, device_id={"dp": dp_of(lax.rem(a + s, na), b)}, device_id_type=MESH
        )
        greeted += 1
    for t in range(1, nb):
        pl.semaphore_signal(
            barrier, inc=1, device_id={"dp": dp_of(a, lax.rem(b + t, nb))}, device_id_type=MESH
        )
        greeted += 1

    row_i = lax.broadcasted_iota(jnp.int32, (tok, tok), 0)
    col_i = lax.broadcasted_iota(jnp.int32, (tok, tok), 1)

    def column(row):
        return jnp.sum(jnp.where(row_i == col_i, row, 0.0), axis=1, keepdims=True)

    route_row = route_ref[...].astype(F32)
    route_col = column(route_row)
    same = route_col == route_row
    pos_row = jnp.sum(jnp.where(same & (row_i < col_i), 1.0, 0.0), axis=0, keepdims=True)
    pos_col = jnp.sum(jnp.where(same & (col_i < row_i), 1.0, 0.0), axis=1, keepdims=True)
    slot_row = route_row * cap + pos_row
    slot_col = route_col * cap + pos_col
    slot_at = lax.broadcasted_iota(jnp.int32, (slots, tok), 0).astype(F32)
    table = jnp.where(slot_at == slot_row, 1.0, 0.0).astype(BF16)
    slot_of = lax.broadcasted_iota(jnp.int32, (tok, slots), 1).astype(F32)
    table_t = jnp.where(slot_of == slot_col, 1.0, 0.0).astype(BF16)

    send_x[...] = jnp.dot(table, tokens_ref[...], preferred_element_type=F32).astype(BF16)
    scaled = (column(gate_ref[...]) * out_grad_ref[...].astype(F32)).astype(BF16)
    send_g[...] = jnp.dot(table, scaled, preferred_element_type=F32).astype(BF16)

    def rows_of(index):
        return pl.ds(pl.multiple_of(index * cap, cap), cap)

    pl.semaphore_wait(barrier, greeted)

    def dispatch(k, src, dst, s_sem, r_sem):
        peer = xor(me, k)
        return pltpu.make_async_remote_copy(
            src_ref=src.at[rows_of(peer)],
            dst_ref=dst.at[rows_of(me)],
            send_sem=s_sem.at[k],
            recv_sem=r_sem.at[k],
            device_id={"expert": peer},
            device_id_type=MESH,
        )

    x_copies = {k: dispatch(k, send_x, recv_x, dx_s, dx_r) for k in near + far}
    g_copies = {k: dispatch(k, send_g, recv_g, dg_s, dg_r) for k in near + far}
    returns = {k: dispatch(k, ret, arrived, rt_s, rt_r) for k in near + far}
    for k in near + far:
        x_copies[k].start()
        g_copies[k].start()

    recv_x[rows_of(me)] = send_x[rows_of(me)]
    recv_g[rows_of(me)] = send_g[rows_of(me)]
    w_copy.wait()

    mine = lax.div(me, n_expert // 4)

    def forward(start, size):
        rows = pl.ds(pl.multiple_of(start, cap), size)
        x = recv_x[rows]
        pre_gate = jnp.dot(x, w_ref[:, :hid], preferred_element_type=F32)
        pre_up = jnp.dot(x, w_ref[:, hid : 2 * hid], preferred_element_type=F32)
        grad_hidden = jnp.dot(recv_g[rows], w_ref[:, 2 * hid :], preferred_element_type=F32)
        sig = jax.nn.sigmoid(pre_gate)
        active = pre_gate * sig
        hidden[rows] = (active * pre_up).astype(BF16)
        grad_gate = grad_hidden * pre_up * (sig * (1.0 + pre_gate * (1.0 - sig)))
        pair[rows, :hid] = grad_gate.astype(BF16)
        pair[rows, hid:] = (grad_hidden * active).astype(BF16)

    def backward(start, size):
        rows = pl.ds(pl.multiple_of(start, cap), size)
        tile = min(512, width)

        @pl.loop(0, width // tile)
        def _(j):
            at = pl.ds(pl.multiple_of(j * tile, tile), tile)
            ret[rows, at] = lax.dot_general(
                pair[rows],
                w_ref[at, : 2 * hid],
                (((1,), (1,)), ((), ())),
                preferred_element_type=F32,
            ).astype(BF16)

    near_half = (lax.div(mine, 2) * 2 * quarter_rows, 2 * quarter_rows)
    across_quarter = (xor(mine, 3) * quarter_rows, quarter_rows)
    last_quarter = (xor(mine, 2) * quarter_rows, quarter_rows)
    for k in near:
        x_copies[k].wait_recv()
        g_copies[k].wait_recv()
    forward(*near_half)
    backward(*near_half)
    for k in near:
        returns[k].start()
    arrived[rows_of(me)] = ret[rows_of(me)]
    for k in across:
        x_copies[k].wait_recv()
        g_copies[k].wait_recv()
    forward(*across_quarter)
    backward(*across_quarter)
    for k in last:
        x_copies[k].wait_recv()
        g_copies[k].wait_recv()
    for k in across:
        returns[k].start()
    forward(*last_quarter)

    def weight_rows(start, size):
        at = pl.ds(pl.multiple_of(start, size), size)
        contract = (((0,), (0,)), ((), ()))
        part[at, : 2 * hid] = (
            grad_scale
            * lax.dot_general(recv_x[:, at], pair[...], contract, preferred_element_type=F32)
        ).astype(BF16)
        part[at, 2 * hid :] = (
            grad_scale
            * lax.dot_general(recv_g[:, at], hidden[...], contract, preferred_element_type=F32)
        ).astype(BF16)

    def band(chip_at, core_at, g):
        return pl.ds(pl.multiple_of((chip_at * 2 + core_at) * share + g * sub, sub), sub)

    bands = [(s, t) for s in range(1, na) for t in list(range(1, nb)) + [0]]
    bands += [(0, t) for t in list(range(1, nb)) + [0]]
    items = [(s, t, g) for s, t in bands for g in range(SUBS)]

    def item_chip(s, t):
        return chip_of(lax.rem(a + s, na), lax.rem(b + t, nb))

    banded = share % 128 == 0
    if not banded:

        @pl.loop(0, width // 256)
        def _(j):
            weight_rows(j * 256, 256)

    def pair_copy(index, chip_at, g):
        rows = band(chip_at, 1 - core, g)
        return pltpu.make_async_remote_copy(
            src_ref=part.at[rows],
            dst_ref=recv_a.at[pl.ds(pl.multiple_of(chip_at * share + g * sub, sub), sub)],
            send_sem=a_s.at[index],
            recv_sem=a_r.at[index],
            device_id={"dp": partner},
            device_id_type=MESH,
        )

    def partner_chip(s, t):
        if na == nb:
            a_at, b_at = lax.rem(b + s, na), lax.rem(a + t, nb)
            return jnp.where(core == 1, b_at * na + a_at, a_at * na + b_at)
        return item_chip(s, t)

    a_copies = []
    for index, (s, t, g) in enumerate(items):
        chip_at = partner_chip(s, t)
        if banded and g == 0:
            weight_rows((chip_at * 2 + 1 - core) * share, share)
        copy = pair_copy(index, chip_at, g)
        copy.start()
        a_copies.append(copy)

    backward(*last_quarter)
    for k in last:
        returns[k].start()

    def pair_sum(index, s, t, g):
        chip_at = item_chip(s, t)
        a_copies[index].wait_recv()
        return (
            part[band(chip_at, core, g)].astype(F32)
            + recv_a[pl.ds(pl.multiple_of(chip_at * share + g * sub, sub), sub)].astype(F32)
        )

    if banded:
        for s, t in bands:
            weight_rows((item_chip(s, t) * 2 + core) * share, share)

    b_copies = {}
    for index, (s, t, g) in enumerate(items):
        if s == 0:
            continue
        at = ((s - 1) * nb + t) * SUBS + g
        send_b[at] = pair_sum(index, s, t, g).astype(BF16)
        copy = pltpu.make_async_remote_copy(
            src_ref=send_b.at[at],
            dst_ref=recv_b.at[at],
            send_sem=b_s.at[at],
            recv_sem=b_r.at[at],
            device_id={"dp": dp_of(lax.rem(a + s, na), b)},
            device_id_type=MESH,
        )
        copy.start()
        b_copies[s, t, g] = copy
    c_copies = {}
    for index, (s, t, g) in enumerate(items):
        if s > 0:
            continue
        total = pair_sum(index, s, t, g)
        for s_from in range(1, na):
            b_copies[s_from, t, g].wait_recv()
            total = total + recv_b[((s_from - 1) * nb + t) * SUBS + g].astype(F32)
        if t > 0:
            at = (t - 1) * SUBS + g
            send_c[at] = total.astype(BF16)
            copy = pltpu.make_async_remote_copy(
                src_ref=send_c.at[at],
                dst_ref=recv_c.at[at],
                send_sem=c_s.at[at],
                recv_sem=c_r.at[at],
                device_id={"dp": dp_of(a, lax.rem(b + t, nb))},
                device_id_type=MESH,
            )
            copy.start()
            c_copies[t, g] = copy
        else:
            w_grad_ref[0, pl.ds(g * sub, sub)] = total
    for t in range(1, nb):
        for g in range(SUBS):
            c_copies[t, g].wait_recv()
            w_grad_ref[0, pl.ds(g * sub, sub)] += recv_c[(t - 1) * SUBS + g].astype(F32)

    for k in near + far:
        returns[k].wait_recv()
    in_grad_ref[...] = jnp.dot(table_t, arrived[...], preferred_element_type=F32).astype(BF16)

    for k in near + far:
        x_copies[k].wait_send()
        g_copies[k].wait_send()
        returns[k].wait_send()
    for copy in a_copies + list(b_copies.values()) + list(c_copies.values()):
        copy.wait_send()


def paired(width, hid, n_expert, n_dp):
    chips_a, chips_b = plan(n_expert, n_dp)[3:]
    return n_expert == 4 and chips_a == chips_b == 2 and width % (128 * n_dp) == hid % (128 * SLICES) == 0


def paired_body(
    n_expert,
    n_dp,
    cap,
    tokens_hbm,
    out_grad_hbm,
    gate_hbm,
    route_hbm,
    w_hbm,
    in_grad_ref,
    w_grad_ref,
    w_ref,
    w2_ref,
    send_x,
    send_g,
    recv_x,
    recv_g,
    ret,
    arrived,
    pair,
    hidden,
    part,
    recv_a,
    send_b,
    recv_b,
    send_c,
    recv_c,
    stage,
    band_x,
    band_g,
    terms,
    held_d,
    send_d,
    near_d,
    far_d,
    tokens_ref,
    out_grad_ref,
    gate_ref,
    route_ref,
    across,
    w_sem,
    in_sem,
    st_sem,
    to_s,
    near_r,
    cross_r,
    rt_s,
    rt_r,
    a_s,
    a_r,
    b_s,
    b_r,
    c_s,
    c_r,
    bd_s,
    bd_r,
    tm_s,
    tm_r,
    fw_s,
    fw_r,
    w_s,
    w_r,
    ag_s,
    ag_r,
    rl_r,
    pf_s,
    pf_r,
    d_s,
    d_r,
):
    _, _, _, na, nb = plan(n_expert, n_dp)
    chips = na * nb
    me = lax.axis_index("expert")
    dp = lax.axis_index("dp")
    half = lax.div(me, 2)
    inner = (me == 1) | (me == n_expert - 2)
    outer = jnp.logical_not(inner)
    near = me + 1 - 2 * lax.rem(me, 2)
    mirror = n_expert - 1 - me
    inner_far = 2 - half
    outer_far = 3 - 3 * half
    tok, width = tokens_hbm.shape
    hid = w_ref.shape[1] // 3
    slots = n_expert * cap
    share = width // n_dp
    sub = share // SUBS
    grad_scale = float(tok * n_dp) ** (-0.5)
    core = lax.rem(dp, 2)
    chip = lax.div(dp, 2)
    partner = dp + 1 - 2 * core
    pos_hi, pos_lo = lax.div(chip, na), lax.rem(chip, na)
    if na == nb:
        a = jnp.where(core == 0, pos_lo, pos_hi)
        b = jnp.where(core == 0, pos_hi, pos_lo)
    else:
        a, b = pos_lo, pos_hi

    def chip_of(a_at, b_at):
        plain = b_at * na + a_at
        if na == nb:
            return jnp.where(core == 0, plain, a_at * na + b_at)
        return plain

    def dp_of(a_at, b_at):
        return chip_of(a_at, b_at) * 2 + core

    def columns_of(index):
        return pl.ds(pl.multiple_of(index * share, share), share)

    w_copy = pltpu.make_async_copy(w_hbm.at[0], w_ref, w_sem)
    slices = w2_ref.shape[0]
    unit = hid // slices

    def stage_copy(q, third):
        return pltpu.make_async_copy(
            w_hbm.at[0, columns_of(dp), pl.ds(third * hid + q * unit, unit)],
            stage.at[q, :, pl.ds(third * unit, unit)],
            st_sem.at[q],
        )

    barrier = pltpu.get_barrier_semaphore()
    for peer in (near, inner_far):
        pl.semaphore_signal(barrier, inc=1, device_id={"expert": peer}, device_id_type=MESH)

    @pl.when(inner)
    def _():
        pl.semaphore_signal(barrier, inc=1, device_id={"expert": outer_far}, device_id_type=MESH)

    beside_dp = [partner] + [xor(chip, c) * 2 + k for c in (1, 2) for k in (0, 1)]
    for peer in beside_dp:
        pl.semaphore_signal(barrier, inc=1, device_id={"dp": peer}, device_id_type=MESH)

    @pl.when(outer)
    def _():
        for q in range(slices):
            for third in range(3):
                stage_copy(q, third).start()

    loads = [
        pltpu.make_async_copy(src, dst, in_sem.at[n])
        for n, (src, dst) in enumerate(
            (
                (route_hbm, route_ref),
                (gate_hbm, gate_ref),
                (tokens_hbm, tokens_ref),
                (out_grad_hbm, out_grad_ref),
            )
        )
    ]
    for load in loads:
        load.start()
    w_copy.start()

    def rows_of(index):
        return pl.ds(index * cap, cap)

    kept = rows_of(3)

    def rows_from(index):
        return pl.ds(pl.multiple_of(index * cap, cap), cap)

    def remote(src, dst, s_sem, r_sem, device):
        return pltpu.make_async_remote_copy(
            src_ref=src,
            dst_ref=dst,
            send_sem=s_sem,
            recv_sem=r_sem,
            device_id=device,
            device_id_type=MESH,
        )

    pl.semaphore_wait(barrier, jnp.where(inner, 3, 2) + len(beside_dp))
    pl.semaphore_signal(
        across, inc=1, device_id={"dp": xor(chip, 1) * 2 + core}, device_id_type=MESH
    )

    def weight_out(q):
        dst = w2_ref.at[q, columns_of(dp)]
        return remote(stage.at[q], dst, w_s, w_r.at[q], {"expert": inner_far})

    @pl.when(outer)
    def _():
        for q in range(slices):
            pltpu.make_async_copy(stage.at[q], stage.at[q], st_sem.at[q]).wait()
            weight_out(q).start()

    row_i = lax.broadcasted_iota(jnp.int32, (tok, tok), 0)
    col_i = lax.broadcasted_iota(jnp.int32, (tok, tok), 1)

    def column(row):
        return jnp.sum(jnp.where(row_i == col_i, row, 0.0), axis=1, keepdims=True)

    loads[0].wait()
    route = route_ref[...]
    block = jnp.where(route == near, 1, jnp.where(route == inner_far, 2, 3))
    route_row = jnp.where(route == me, 0, block).astype(F32)
    route_col = column(route_row)
    same = route_col == route_row
    pos_row = jnp.sum(jnp.where(same & (row_i < col_i), 1.0, 0.0), axis=0, keepdims=True)
    pos_col = jnp.sum(jnp.where(same & (col_i < row_i), 1.0, 0.0), axis=1, keepdims=True)
    slot_row = route_row * cap + pos_row
    slot_col = route_col * cap + pos_col
    slot_at = lax.broadcasted_iota(jnp.int32, (slots, tok), 0).astype(F32)
    table = jnp.where(slot_at == slot_row, 1.0, 0.0).astype(BF16)
    slot_of = lax.broadcasted_iota(jnp.int32, (tok, slots), 1).astype(F32)
    table_t = jnp.where(slot_of == slot_col, 1.0, 0.0).astype(BF16)

    loads[2].wait()
    send_x[...] = jnp.dot(table, tokens_ref[...], preferred_element_type=F32).astype(BF16)
    loads[1].wait()
    loads[3].wait()
    scaled = (column(gate_ref[...]) * out_grad_ref[...].astype(F32)).astype(BF16)
    send_g[...] = jnp.dot(table, scaled, preferred_element_type=F32).astype(BF16)

    def run(is_inner):
        cross_at = 2 if is_inner else 3

        def near_copy(src, dst):
            return remote(
                src.at[rows_of(1)], dst.at[rows_of(1)], to_s, near_r, {"expert": near}
            )

        def cross_copy(src, dst):
            return remote(
                src.at[rows_of(2)],
                dst.at[rows_of(cross_at)],
                to_s,
                cross_r.at[cross_at - 2],
                {"expert": inner_far},
            )

        def bytes_of(ref, s_sem, r_sem):
            return remote(ref, ref, s_sem, r_sem, {"expert": near})

        both = pl.ds(0, 2 * cap)
        x_args = (send_x, recv_x)
        g_args = (send_g, recv_g)

        def return_copy(index):
            peer = {1: near, 2: mirror, 3: outer_far}[index]
            home = rows_of(min(index, 2))
            return remote(
                ret.at[rows_of(index)],
                arrived.at[home],
                rt_s,
                rt_r,
                {"expert": peer},
            )

        first = jnp.where(core == 0, 1, 2)

        def beside(c):
            return xor(chip, c)

        chip_first = jnp.where(core == 0, beside(1), beside(2))
        chip_second = jnp.where(core == 0, beside(2), beside(1))

        def weight_on(q):
            at = w2_ref.at[q, columns_of(dp)]
            return remote(at, at, w_s, w_r.at[q], {"expert": near})

        def spread(c, q):
            at = w2_ref.at[q, columns_of(dp)]
            return remote(at, at, ag_s, ag_r.at[q], {"dp": beside(c) * 2 + core})

        def relay(q):
            at = w2_ref.at[q, columns_of(chip_first * 2 + core)]
            return remote(at, at, ag_s, rl_r.at[q], {"dp": chip_second * 2 + core})

        def hand_over(c, q):
            at = w2_ref.at[q, columns_of(beside(c) * 2 + core)]
            return remote(at, at, pf_s, pf_r.at[q], {"dp": partner})

        def band_copy(j, src, dst):
            peer = lax.rem(dp + j, n_dp)
            return remote(
                src.at[kept, columns_of(peer)], dst.at[rows_from(dp)], bd_s, bd_r, {"dp": peer}
            )

        bands_in = bytes_of(recv_x.at[pl.ds(0, 2 * (n_dp - 1) * cap // n_dp)], bd_s, bd_r)

        def term_copy(c, q):
            at = terms.at[q, rows_from(dp)]
            return remote(at, at, tm_s, tm_r.at[q], {"dp": beside(c) * 2 + core})

        def term_over(c, q):
            at = terms.at[q, rows_from(beside(c) * 2 + core)]
            return remote(at, at, fw_s, fw_r.at[q], {"dp": partner})

        if is_inner:
            near_copy(*x_args).start()
        cross_copy(*x_args).start()
        cross_copy(*g_args).start()
        if not is_inner:
            near_copy(*x_args).start()
            near_copy(*g_args).start()
        pl.semaphore_wait(across, 1)
        for j in range(1, n_dp):
            band_copy(j, send_x, band_x).start()
            band_copy(j, send_g, band_g).start()

        recv_x[rows_of(0)] = send_x[rows_of(0)]
        recv_g[rows_of(0)] = send_g[rows_of(0)]
        band_x[rows_from(dp)] = send_x[kept, columns_of(dp)]
        band_g[rows_from(dp)] = send_g[kept, columns_of(dp)]

        def forward(x, g, weights):
            third = weights.shape[1] // 3
            pre_gate = jnp.dot(x, weights[:, :third], preferred_element_type=F32)
            pre_up = jnp.dot(x, weights[:, third : 2 * third], preferred_element_type=F32)
            grad_hidden = jnp.dot(g, weights[:, 2 * third :], preferred_element_type=F32)
            sig = jax.nn.sigmoid(pre_gate)
            active = pre_gate * sig
            grad_gate = grad_hidden * pre_up * (sig * (1.0 + pre_gate * (1.0 - sig)))
            return (
                grad_gate.astype(BF16),
                (grad_hidden * active).astype(BF16),
                (active * pre_up).astype(BF16),
            )

        def forward_rows(start, size):
            rows = pl.ds(start, size)
            grad_gate, grad_up, kept_hidden = forward(recv_x[rows], recv_g[rows], w_ref)
            pair[rows, :hid] = grad_gate
            pair[rows, hid:] = grad_up
            hidden[rows] = kept_hidden

        def columns(pieces, dst, rows):
            tile = min(512, width)

            @pl.loop(0, width // tile)
            def _(j):
                at = pl.ds(pl.multiple_of(j * tile, tile), tile)
                total = 0.0
                for grads, weights in pieces:
                    total = total + lax.dot_general(
                        grads(), weights(at), (((1,), (1,)), ((), ())), preferred_element_type=F32
                    )
                dst[rows, at] = total.astype(BF16)

        def backward_rows(start, size):
            rows = pl.ds(start, size)
            columns([(lambda: pair[rows], lambda at: w_ref[at, : 2 * hid])], ret, rows)

        contract = (((0,), (0,)), ((), ()))
        mine = rows_from(dp)

        def kept_forward(q):
            grad_gate, grad_up, kept_hidden = forward(send_x[kept], send_g[kept], w2_ref.at[q])
            terms[q, mine, :unit] = grad_gate
            terms[q, mine, unit : 2 * unit] = grad_up
            terms[q, mine, 2 * unit :] = kept_hidden

        def kept_grad(q):
            first = lax.dot_general(
                band_x[...], terms[q, :, : 2 * unit], contract, preferred_element_type=F32
            )
            second = lax.dot_general(
                band_g[...], terms[q, :, 2 * unit :], contract, preferred_element_type=F32
            )
            return grad_scale * jnp.concatenate([first, second], axis=1)

        def near_hop(q):
            return remote(send_d.at[q], near_d.at[q], d_s, d_r.at[q], {"expert": near})

        def far_hop(q):
            return remote(send_d.at[q], far_d.at[q], d_s, d_r.at[q], {"expert": outer_far})

        def take(q):
            weight_on(q).wait_recv()
            if is_inner:
                weight_on(q).start()
            for c in (1, 2):
                spread(c, q).start()
            hand_over(0, q).start()

        def pass_on(q):
            bytes_of(w2_ref.at[q, pl.ds(0, 2 * share)], ag_s, ag_r.at[q]).wait_recv()
            relay(q).start()
            for c in (1, 2):
                hand_over(c, q).start()

        def pass_last(q):
            relay(q).wait_recv()
            hand_over(3, q).start()

        def kept_terms(q):
            bytes_of(w2_ref.at[q, pl.ds(0, 4 * share)], pf_s, pf_r.at[q]).wait_recv()
            kept_forward(q)
            for c in range(1, 4):
                term_copy(c, q).start()
            term_over(0, q).start()

        def pass_terms(q):
            bytes_of(terms.at[q, pl.ds(0, 3 * cap)], tm_s, tm_r.at[q]).wait_recv()
            for c in range(1, 4):
                term_over(c, q).start()

        def kept_band(q):
            if q == 0:
                bands_in.wait_recv()
            bytes_of(terms.at[q, pl.ds(0, 4 * cap)], fw_s, fw_r.at[q]).wait_recv()
            held_d[q] = kept_grad(q)
            if not is_inner:
                send_d[q] = held_d[q].astype(BF16)
                near_hop(q).start()

        def own_rows():
            w_copy.wait()
            forward_rows(0, cap)
            backward_rows(0, cap)
            arrived[rows_of(0)] = ret[rows_of(0)]

        def near_arrival():
            bytes_of(recv_x.at[both], to_s, near_r).wait_recv()

        def cross_arrival(index):
            bytes_of(recv_x.at[both], to_s, cross_r.at[index - 2]).wait_recv()

        def return_rows(start, size):
            backward_rows(start * cap, size * cap)
            for index in range(start, start + size):
                return_copy(index).start()

        def kept_backward():
            pieces = [
                (lambda q=q: terms[q, mine, : 2 * unit], lambda at, q=q: w2_ref[q, at, : 2 * unit])
                for q in range(slices)
            ]
            columns(pieces, arrived, kept)

        def add_hop(q):
            near_hop(q).wait_recv()
            send_d[q] = (held_d[q] + near_d[q].astype(F32)).astype(BF16)
            far_hop(q).start()

        rows_in = slots if is_inner else 2 * cap

        def weight_rows(start, size):
            at = pl.ds(pl.multiple_of(start, size), size)
            part[at, : 2 * hid] = (
                grad_scale
                * lax.dot_general(
                    recv_x[:rows_in, at], pair[:rows_in], contract, preferred_element_type=F32
                )
            ).astype(BF16)
            part[at, 2 * hid :] = (
                grad_scale
                * lax.dot_general(
                    recv_g[:rows_in, at], hidden[:rows_in], contract, preferred_element_type=F32
                )
            ).astype(BF16)

        def band(chip_at, core_at, g):
            return pl.ds(pl.multiple_of((chip_at * 2 + core_at) * share + g * sub, sub), sub)

        bands = [(s, t) for s in range(1, na) for t in list(range(1, nb)) + [0]]
        bands += [(0, t) for t in list(range(1, nb)) + [0]]
        items = [(s, t, g) for s, t in bands for g in range(SUBS)]

        def item_chip(s, t):
            return chip_of(lax.rem(a + s, na), lax.rem(b + t, nb))

        def pair_copy(index, chip_at, g):
            return remote(
                part.at[band(chip_at, 1 - core, g)],
                recv_a.at[pl.ds(pl.multiple_of(chip_at * share + g * sub, sub), sub)],
                a_s,
                a_r.at[index],
                {"dp": partner},
            )

        def partner_chip(s, t):
            if na == nb:
                a_at, b_at = lax.rem(b + s, na), lax.rem(a + t, nb)
                return jnp.where(core == 1, b_at * na + a_at, a_at * na + b_at)
            return item_chip(s, t)

        def item_pair(index):
            s, t, g = items[index]
            return pair_copy(index, partner_chip(s, t), g)

        def item_out(s, t, g):
            at = ((s - 1) * nb + t) * SUBS + g
            to = dp_of(lax.rem(a + s, na), b)
            return remote(send_b.at[at], recv_b.at[at], b_s, b_r.at[at], {"dp": to})

        def item_last(t, g):
            at = (t - 1) * SUBS + g
            to = dp_of(a, lax.rem(b + t, nb))
            return remote(send_c.at[at], recv_c.at[at], c_s, c_r.at[at], {"dp": to})

        def pair_sum(index):
            s, t, g = items[index]
            chip_to = item_chip(s, t)
            item_pair(index).wait_recv()
            return (
                part[band(chip_to, core, g)].astype(F32)
                + recv_a[pl.ds(pl.multiple_of(chip_to * share + g * sub, sub), sub)].astype(F32)
            )

        sent = [index for index, (s, t, g) in enumerate(items) if s > 0]
        rest = [index for index, (s, t, g) in enumerate(items) if s == 0]

        def reduce_pair(which):
            for index in which:
                s, t, g = items[index]
                if g == 0:
                    weight_rows((partner_chip(s, t) * 2 + 1 - core) * share, share)
                item_pair(index).start()

        def reduce_first(which):
            for index in which:
                s, t, g = items[index]
                if g == 0:
                    weight_rows((item_chip(s, t) * 2 + core) * share, share)
                if s > 0:
                    send_b[((s - 1) * nb + t) * SUBS + g] = pair_sum(index).astype(BF16)
                    item_out(s, t, g).start()

        def item_total(index):
            s, t, g = items[index]
            total = pair_sum(index)
            for s_from in range(1, na):
                item_out(s_from, t, g).wait_recv()
                total = total + recv_b[((s_from - 1) * nb + t) * SUBS + g].astype(F32)
            return total

        def reduce_second():
            for index, (s, t, g) in enumerate(items):
                if s == 0 and t > 0:
                    send_c[(t - 1) * SUBS + g] = item_total(index).astype(BF16)
                    item_last(t, g).start()

        def reduce_own():
            for index, (s, t, g) in enumerate(items):
                if s == t == 0:
                    w_grad_ref[0, pl.ds(g * sub, sub)] = item_total(index)
            for t in range(1, nb):
                for g in range(SUBS):
                    item_last(t, g).wait_recv()
                    w_grad_ref[0, pl.ds(g * sub, sub)] += recv_c[(t - 1) * SUBS + g].astype(F32)

        def add_far(q):
            far_hop(q).wait_recv()
            for third in range(3):
                at = pl.ds(third * hid + q * unit, unit)
                w_grad_ref[0, :, at] += far_d[q, :, third * unit : (third + 1) * unit].astype(F32)

        own_rows()
        take(0)
        take(1)
        pass_on(0)
        take(2)
        if is_inner:
            near_copy(*g_args).start()
        pass_on(1)
        pass_last(0)
        kept_terms(0)
        pass_on(2)
        if is_inner:
            pass_last(1)
            kept_terms(1)
            pass_terms(0)
            pass_last(2)
            kept_terms(2)
            cross_arrival(3)
            forward_rows(3 * cap, cap)
            return_rows(3, 1)
            pass_terms(1)
            pass_terms(2)
            kept_band(0)
            kept_band(1)
            near_arrival()
            cross_arrival(2)
            forward_rows(cap, 2 * cap)
            reduce_pair(sent)
            reduce_first(sent)
            add_hop(0)
            return_rows(1, 2)
            reduce_pair(rest)
            reduce_first(rest)
            add_hop(1)
            kept_band(2)
            reduce_second()
            add_hop(2)
            kept_backward()
            reduce_own()
        else:
            near_arrival()
            forward_rows(cap, cap)
            pass_last(1)
            pass_terms(0)
            kept_terms(1)
            kept_band(0)
            pass_last(2)
            reduce_pair(sent + rest)
            kept_terms(2)
            pass_terms(1)
            kept_band(1)
            reduce_first(sent + rest)
            pass_terms(2)
            kept_band(2)
            return_rows(1, 1)
            kept_backward()
            reduce_second()
            reduce_own()
            for q in range(slices - 1):
                add_far(q)

        bytes_of(arrived.at[both], rt_s, rt_r).wait_recv()
        in_grad_ref[...] = jnp.dot(table_t, arrived[...], preferred_element_type=F32).astype(BF16)
        if not is_inner:
            add_far(slices - 1)

        bytes_of(send_x, to_s, near_r).wait_send()
        bands_in.wait_send()
        bytes_of(terms.at[:, pl.ds(0, 3 * cap)], tm_s, tm_r.at[0]).wait_send()
        bytes_of(terms.at[:, pl.ds(0, 4 * cap)], fw_s, fw_r.at[0]).wait_send()
        bytes_of(w2_ref.at[:, pl.ds(0, 3 * share)], ag_s, ag_r.at[0]).wait_send()
        bytes_of(w2_ref.at[:, pl.ds(0, 4 * share)], pf_s, pf_r.at[0]).wait_send()
        bytes_of(stage, w_s, w_r.at[0]).wait_send()
        bytes_of(send_d, d_s, d_r.at[0]).wait_send()
        bytes_of(ret.at[pl.ds(0, (3 if is_inner else 1) * cap)], rt_s, rt_r).wait_send()
        bytes_of(recv_a, a_s, a_r.at[0]).wait_send()
        bytes_of(send_b, b_s, b_r.at[0]).wait_send()
        bytes_of(send_c, c_s, c_r.at[0]).wait_send()

    pl.when(inner)(lambda: run(True))
    pl.when(outer)(lambda: run(False))


def local(n_expert, n_dp, tokens, out_grad, gate_prob, routing, expert_weights):
    tok, width = tokens.shape
    full = expert_weights.shape[2]
    hid = full // 3
    cap = max(16, 2 * tok // n_expert)
    slots = n_expert * cap
    share = width // n_dp
    _, _, _, na, nb = plan(n_expert, n_dp)
    sub = share // SUBS
    chips = na * nb
    n_b, n_c = max(1, (na - 1) * nb) * SUBS, max(1, nb - 1) * SUBS
    dma = pltpu.SemaphoreType.DMA
    vmem = pl.BlockSpec(memory_space=pltpu.VMEM)
    weights, rows = pltpu.VMEM((width, full), BF16), pltpu.VMEM((slots, width), BF16)
    scratch = [weights] + [rows] * 6
    scratch += [
        pltpu.VMEM((slots, 2 * hid), BF16),
        pltpu.VMEM((slots, hid), BF16),
        pltpu.VMEM((width, full), BF16),
        pltpu.VMEM((chips * share, full), BF16),
        pltpu.VMEM((n_b, sub, full), BF16),
        pltpu.VMEM((n_b, sub, full), BF16),
        pltpu.VMEM((n_c, sub, full), BF16),
        pltpu.VMEM((n_c, sub, full), BF16),
    ]
    sems = [dma] + [dma((n_expert,))] * 6 + [dma((chips * SUBS,))] * 2
    sems += [dma((n_b,))] * 2 + [dma((n_c,))] * 2
    kernel, ins = body, [vmem] * 4
    if paired(width, hid, n_expert, n_dp):
        kernel = paired_body
        slices, third = SLICES, full // SLICES
        scratch.insert(1, pltpu.VMEM((slices, width, third), BF16))
        scratch += [pltpu.VMEM((slices, share, third), BF16)]
        scratch += [pltpu.VMEM((n_dp * cap, share), BF16)] * 2
        scratch += [pltpu.VMEM((slices, n_dp * cap, third), BF16)]
        scratch += [pltpu.VMEM((slices, share, third), F32)]
        scratch += [pltpu.VMEM((slices, share, third), BF16)] * 3
        scratch += [pltpu.VMEM((tok, width), BF16)] * 2
        scratch += [pltpu.VMEM((1, tok), F32), pltpu.VMEM((1, tok), jnp.int32)]
        each = dma((slices,))
        sems = [pltpu.SemaphoreType.REGULAR, dma, dma((4,)), each, dma, dma, dma((2,)), dma, dma]
        sems += [dma, dma((chips * SUBS,)), dma, dma((n_b,)), dma, dma((n_c,)), dma, dma]
        sems += [dma, each] * 3 + [dma, each, each] + [dma, each] * 2
        ins = [pl.BlockSpec(memory_space=pl.ANY)] * 4
    early = pl.pallas_call(
        functools.partial(kernel, n_expert, n_dp, cap),
        out_shape=(pltpu.VMEM((tok, width), BF16), pltpu.VMEM((1, share, full), F32)),
        in_specs=ins + [pl.BlockSpec(memory_space=pl.ANY)],
        out_specs=(vmem, vmem),
        scratch_shapes=scratch + sems,
        compiler_params=pltpu.CompilerParams(
            collective_id=0, has_side_effects=True, vmem_limit_bytes=60 * 1024 * 1024
        ),
        name="moe_backward",
    )(tokens, out_grad, gate_prob.reshape(1, tok), routing.reshape(1, tok), expert_weights)
    return pl.pallas_call(
        write_out,
        out_shape=(
            jax.ShapeDtypeStruct((tok, width), BF16),
            jax.ShapeDtypeStruct((1, share, full), F32),
        ),
        in_specs=[vmem] * 2,
        out_specs=(pl.BlockSpec(memory_space=pl.ANY),) * 2,
        scratch_shapes=[dma((2,))],
        name="write_out",
    )(*[pltpu.with_memory_space_constraint(value, pltpu.VMEM) for value in early])


def write_out(in_grad_ref, w_grad_ref, in_grad_out, w_grad_out, sem):
    moves = [
        pltpu.make_async_copy(in_grad_ref, in_grad_out, sem.at[0]),
        pltpu.make_async_copy(w_grad_ref, w_grad_out, sem.at[1]),
    ]
    for move in moves:
        move.start()
    for move in moves:
        move.wait()


def solution(mesh):
    tokens_spec = P(("dp", "expert"), None)
    return jax.shard_map(
        functools.partial(local, mesh.shape["expert"], mesh.shape["dp"]),
        mesh=mesh,
        in_specs=(tokens_spec, tokens_spec, tokens_spec, tokens_spec, P("expert", None, None)),
        out_specs=(tokens_spec, P("expert", "dp", None)),
        check_vma=False,
    )
```

```python
import functools
import math
import jax
import jax.numpy as jnp
from jax import lax
from jax.experimental import pallas as pl
from jax.experimental.pallas import tpu as pltpu
from jax.sharding import PartitionSpec as P

MESH = pl.DeviceIdType.MESH
F32 = jnp.float32
BF16 = jnp.bfloat16
SUBS = 2
SLICES = 3
PIECES = 4


def xor(value, step):
    total, bit = 0, 1
    result = value
    while bit <= step:
        if step & bit:
            result = result + bit - 2 * bit * (lax.rem(lax.div(value, bit), 2))
        bit *= 2
    return result


def plan(n_expert, n_dp):
    half, quarter = n_expert // 2, n_expert // 4
    near = list(range(1, half))
    across = list(range(n_expert - 1, half + quarter - 1, -1))
    last = list(range(half + quarter - 1, half - 1, -1))
    chips = n_dp // 2
    side = math.isqrt(chips)
    while chips % side:
        side -= 1
    return near, across, last, chips // side, side


def body(
    n_expert,
    n_dp,
    cap,
    tokens_ref,
    out_grad_ref,
    gate_ref,
    route_ref,
    w_hbm,
    in_grad_ref,
    w_grad_ref,
    w_ref,
    send_x,
    send_g,
    recv_x,
    recv_g,
    ret,
    arrived,
    pair,
    hidden,
    part,
    recv_a,
    send_b,
    recv_b,
    send_c,
    recv_c,
    w_sem,
    dx_s,
    dx_r,
    dg_s,
    dg_r,
    rt_s,
    rt_r,
    a_s,
    a_r,
    b_s,
    b_r,
    c_s,
    c_r,
):
    near, across, last, na, nb = plan(n_expert, n_dp)
    far = across + last
    me = lax.axis_index("expert")
    dp = lax.axis_index("dp")
    tok, width = tokens_ref.shape
    hid = w_ref.shape[1] // 3
    slots = n_expert * cap
    quarter_rows = slots // 4
    share = width // n_dp
    sub = share // SUBS
    grad_scale = float(tok * n_dp) ** (-0.5)
    core = lax.rem(dp, 2)
    chip = lax.div(dp, 2)
    pos_hi, pos_lo = lax.div(chip, na), lax.rem(chip, na)
    if na == nb:
        a = jnp.where(core == 0, pos_lo, pos_hi)
        b = jnp.where(core == 0, pos_hi, pos_lo)
    else:
        a, b = pos_lo, pos_hi

    def chip_of(a_at, b_at):
        plain = b_at * na + a_at
        if na == nb:
            return jnp.where(core == 0, plain, a_at * na + b_at)
        return plain

    def dp_of(a_at, b_at):
        return chip_of(a_at, b_at) * 2 + core

    w_copy = pltpu.make_async_copy(w_hbm.at[0], w_ref, w_sem)
    w_copy.start()

    barrier = pltpu.get_barrier_semaphore()
    partner = dp + 1 - 2 * core
    greeted = 0
    for k in near + far:
        pl.semaphore_signal(barrier, inc=1, device_id={"expert": xor(me, k)}, device_id_type=MESH)
        greeted += 1
    pl.semaphore_signal(barrier, inc=1, device_id={"dp": partner}, device_id_type=MESH)
    greeted += 1
    for s in range(1, na):
        pl.semaphore_signal(
            barrier, inc=1, device_id={"dp": dp_of(lax.rem(a + s, na), b)}, device_id_type=MESH
        )
        greeted += 1
    for t in range(1, nb):
        pl.semaphore_signal(
            barrier, inc=1, device_id={"dp": dp_of(a, lax.rem(b + t, nb))}, device_id_type=MESH
        )
        greeted += 1

    row_i = lax.broadcasted_iota(jnp.int32, (tok, tok), 0)
    col_i = lax.broadcasted_iota(jnp.int32, (tok, tok), 1)

    def column(row):
        return jnp.sum(jnp.where(row_i == col_i, row, 0.0), axis=1, keepdims=True)

    route_row = route_ref[...].astype(F32)
    route_col = column(route_row)
    same = route_col == route_row
    pos_row = jnp.sum(jnp.where(same & (row_i < col_i), 1.0, 0.0), axis=0, keepdims=True)
    pos_col = jnp.sum(jnp.where(same & (col_i < row_i), 1.0, 0.0), axis=1, keepdims=True)
    slot_row = route_row * cap + pos_row
    slot_col = route_col * cap + pos_col
    slot_at = lax.broadcasted_iota(jnp.int32, (slots, tok), 0).astype(F32)
    table = jnp.where(slot_at == slot_row, 1.0, 0.0).astype(BF16)
    slot_of = lax.broadcasted_iota(jnp.int32, (tok, slots), 1).astype(F32)
    table_t = jnp.where(slot_of == slot_col, 1.0, 0.0).astype(BF16)

    send_x[...] = jnp.dot(table, tokens_ref[...], preferred_element_type=F32).astype(BF16)
    scaled = (column(gate_ref[...]) * out_grad_ref[...].astype(F32)).astype(BF16)
    send_g[...] = jnp.dot(table, scaled, preferred_element_type=F32).astype(BF16)

    def rows_of(index):
        return pl.ds(pl.multiple_of(index * cap, cap), cap)

    pl.semaphore_wait(barrier, greeted)

    def dispatch(k, src, dst, s_sem, r_sem):
        peer = xor(me, k)
        return pltpu.make_async_remote_copy(
            src_ref=src.at[rows_of(peer)],
            dst_ref=dst.at[rows_of(me)],
            send_sem=s_sem.at[k],
            recv_sem=r_sem.at[k],
            device_id={"expert": peer},
            device_id_type=MESH,
        )

    x_copies = {k: dispatch(k, send_x, recv_x, dx_s, dx_r) for k in near + far}
    g_copies = {k: dispatch(k, send_g, recv_g, dg_s, dg_r) for k in near + far}
    returns = {k: dispatch(k, ret, arrived, rt_s, rt_r) for k in near + far}
    for k in near + far:
        x_copies[k].start()
        g_copies[k].start()

    recv_x[rows_of(me)] = send_x[rows_of(me)]
    recv_g[rows_of(me)] = send_g[rows_of(me)]
    w_copy.wait()

    mine = lax.div(me, n_expert // 4)

    def forward(start, size):
        rows = pl.ds(pl.multiple_of(start, cap), size)
        x = recv_x[rows]
        pre_gate = jnp.dot(x, w_ref[:, :hid], preferred_element_type=F32)
        pre_up = jnp.dot(x, w_ref[:, hid : 2 * hid], preferred_element_type=F32)
        grad_hidden = jnp.dot(recv_g[rows], w_ref[:, 2 * hid :], preferred_element_type=F32)
        sig = jax.nn.sigmoid(pre_gate)
        active = pre_gate * sig
        hidden[rows] = (active * pre_up).astype(BF16)
        grad_gate = grad_hidden * pre_up * (sig * (1.0 + pre_gate * (1.0 - sig)))
        pair[rows, :hid] = grad_gate.astype(BF16)
        pair[rows, hid:] = (grad_hidden * active).astype(BF16)

    def backward(start, size):
        rows = pl.ds(pl.multiple_of(start, cap), size)
        tile = min(512, width)

        @pl.loop(0, width // tile)
        def _(j):
            at = pl.ds(pl.multiple_of(j * tile, tile), tile)
            ret[rows, at] = lax.dot_general(
                pair[rows],
                w_ref[at, : 2 * hid],
                (((1,), (1,)), ((), ())),
                preferred_element_type=F32,
            ).astype(BF16)

    near_half = (lax.div(mine, 2) * 2 * quarter_rows, 2 * quarter_rows)
    across_quarter = (xor(mine, 3) * quarter_rows, quarter_rows)
    last_quarter = (xor(mine, 2) * quarter_rows, quarter_rows)
    for k in near:
        x_copies[k].wait_recv()
        g_copies[k].wait_recv()
    forward(*near_half)
    backward(*near_half)
    for k in near:
        returns[k].start()
    arrived[rows_of(me)] = ret[rows_of(me)]
    for k in across:
        x_copies[k].wait_recv()
        g_copies[k].wait_recv()
    forward(*across_quarter)
    backward(*across_quarter)
    for k in last:
        x_copies[k].wait_recv()
        g_copies[k].wait_recv()
    for k in across:
        returns[k].start()
    forward(*last_quarter)

    def weight_rows(start, size):
        at = pl.ds(pl.multiple_of(start, size), size)
        contract = (((0,), (0,)), ((), ()))
        part[at, : 2 * hid] = (
            grad_scale
            * lax.dot_general(recv_x[:, at], pair[...], contract, preferred_element_type=F32)
        ).astype(BF16)
        part[at, 2 * hid :] = (
            grad_scale
            * lax.dot_general(recv_g[:, at], hidden[...], contract, preferred_element_type=F32)
        ).astype(BF16)

    def band(chip_at, core_at, g):
        return pl.ds(pl.multiple_of((chip_at * 2 + core_at) * share + g * sub, sub), sub)

    bands = [(s, t) for s in range(1, na) for t in list(range(1, nb)) + [0]]
    bands += [(0, t) for t in list(range(1, nb)) + [0]]
    items = [(s, t, g) for s, t in bands for g in range(SUBS)]

    def item_chip(s, t):
        return chip_of(lax.rem(a + s, na), lax.rem(b + t, nb))

    banded = share % 128 == 0
    if not banded:

        @pl.loop(0, width // 256)
        def _(j):
            weight_rows(j * 256, 256)

    def pair_copy(index, chip_at, g):
        rows = band(chip_at, 1 - core, g)
        return pltpu.make_async_remote_copy(
            src_ref=part.at[rows],
            dst_ref=recv_a.at[pl.ds(pl.multiple_of(chip_at * share + g * sub, sub), sub)],
            send_sem=a_s.at[index],
            recv_sem=a_r.at[index],
            device_id={"dp": partner},
            device_id_type=MESH,
        )

    def partner_chip(s, t):
        if na == nb:
            a_at, b_at = lax.rem(b + s, na), lax.rem(a + t, nb)
            return jnp.where(core == 1, b_at * na + a_at, a_at * na + b_at)
        return item_chip(s, t)

    a_copies = []
    for index, (s, t, g) in enumerate(items):
        chip_at = partner_chip(s, t)
        if banded and g == 0:
            weight_rows((chip_at * 2 + 1 - core) * share, share)
        copy = pair_copy(index, chip_at, g)
        copy.start()
        a_copies.append(copy)

    backward(*last_quarter)
    for k in last:
        returns[k].start()

    def pair_sum(index, s, t, g):
        chip_at = item_chip(s, t)
        a_copies[index].wait_recv()
        return (
            part[band(chip_at, core, g)].astype(F32)
            + recv_a[pl.ds(pl.multiple_of(chip_at * share + g * sub, sub), sub)].astype(F32)
        )

    if banded:
        for s, t in bands:
            weight_rows((item_chip(s, t) * 2 + core) * share, share)

    b_copies = {}
    for index, (s, t, g) in enumerate(items):
        if s == 0:
            continue
        at = ((s - 1) * nb + t) * SUBS + g
        send_b[at] = pair_sum(index, s, t, g).astype(BF16)
        copy = pltpu.make_async_remote_copy(
            src_ref=send_b.at[at],
            dst_ref=recv_b.at[at],
            send_sem=b_s.at[at],
            recv_sem=b_r.at[at],
            device_id={"dp": dp_of(lax.rem(a + s, na), b)},
            device_id_type=MESH,
        )
        copy.start()
        b_copies[s, t, g] = copy
    c_copies = {}
    for index, (s, t, g) in enumerate(items):
        if s > 0:
            continue
        total = pair_sum(index, s, t, g)
        for s_from in range(1, na):
            b_copies[s_from, t, g].wait_recv()
            total = total + recv_b[((s_from - 1) * nb + t) * SUBS + g].astype(F32)
        if t > 0:
            at = (t - 1) * SUBS + g
            send_c[at] = total.astype(BF16)
            copy = pltpu.make_async_remote_copy(
                src_ref=send_c.at[at],
                dst_ref=recv_c.at[at],
                send_sem=c_s.at[at],
                recv_sem=c_r.at[at],
                device_id={"dp": dp_of(a, lax.rem(b + t, nb))},
                device_id_type=MESH,
            )
            copy.start()
            c_copies[t, g] = copy
        else:
            w_grad_ref[0, pl.ds(g * sub, sub)] = total
    for t in range(1, nb):
        for g in range(SUBS):
            c_copies[t, g].wait_recv()
            w_grad_ref[0, pl.ds(g * sub, sub)] += recv_c[(t - 1) * SUBS + g].astype(F32)

    for k in near + far:
        returns[k].wait_recv()
    in_grad_ref[...] = jnp.dot(table_t, arrived[...], preferred_element_type=F32).astype(BF16)

    for k in near + far:
        x_copies[k].wait_send()
        g_copies[k].wait_send()
        returns[k].wait_send()
    for copy in a_copies + list(b_copies.values()) + list(c_copies.values()):
        copy.wait_send()


def paired(width, hid, n_expert, n_dp):
    chips_a, chips_b = plan(n_expert, n_dp)[3:]
    return n_expert == 4 and chips_a == chips_b == 2 and width % (128 * n_dp) == hid % (128 * SLICES) == 0


def paired_body(
    n_expert,
    n_dp,
    cap,
    tokens_hbm,
    out_grad_hbm,
    gate_hbm,
    route_hbm,
    w_hbm,
    in_grad_ref,
    w_grad_ref,
    w_ref,
    w2_ref,
    send_x,
    send_g,
    recv_x,
    recv_g,
    ret,
    arrived,
    pair,
    hidden,
    part,
    recv_a,
    send_b,
    recv_b,
    send_c,
    recv_c,
    stage,
    band_x,
    band_g,
    terms,
    held_d,
    send_d,
    near_d,
    far_d,
    tokens_ref,
    out_grad_ref,
    gate_ref,
    route_ref,
    across,
    w_sem,
    in_sem,
    st_sem,
    to_s,
    near_r,
    cross_r,
    rt_s,
    rt_r,
    a_s,
    a_r,
    b_s,
    b_r,
    c_s,
    c_r,
    bd_s,
    bd_r,
    tm_s,
    tm_r,
    fw_s,
    fw_r,
    w_s,
    w_r,
    ag_s,
    ag_r,
    rl_r,
    pf_s,
    pf_r,
    d_s,
    d_r,
):
    _, _, _, na, nb = plan(n_expert, n_dp)
    chips = na * nb
    me = lax.axis_index("expert")
    dp = lax.axis_index("dp")
    half = lax.div(me, 2)
    inner = (me == 1) | (me == n_expert - 2)
    outer = jnp.logical_not(inner)
    near = me + 1 - 2 * lax.rem(me, 2)
    mirror = n_expert - 1 - me
    inner_far = 2 - half
    outer_far = 3 - 3 * half
    tok, width = tokens_hbm.shape
    hid = w_ref.shape[1] // 3
    slots = n_expert * cap
    share = width // n_dp
    sub = share // SUBS
    grad_scale = float(tok * n_dp) ** (-0.5)
    core = lax.rem(dp, 2)
    chip = lax.div(dp, 2)
    partner = dp + 1 - 2 * core
    pos_hi, pos_lo = lax.div(chip, na), lax.rem(chip, na)
    if na == nb:
        a = jnp.where(core == 0, pos_lo, pos_hi)
        b = jnp.where(core == 0, pos_hi, pos_lo)
    else:
        a, b = pos_lo, pos_hi

    def chip_of(a_at, b_at):
        plain = b_at * na + a_at
        if na == nb:
            return jnp.where(core == 0, plain, a_at * na + b_at)
        return plain

    def dp_of(a_at, b_at):
        return chip_of(a_at, b_at) * 2 + core

    def columns_of(index):
        return pl.ds(pl.multiple_of(index * share, share), share)

    w_copy = pltpu.make_async_copy(w_hbm.at[0], w_ref, w_sem)
    slices = w2_ref.shape[0]
    unit = hid // slices

    def stage_copy(q, third):
        return pltpu.make_async_copy(
            w_hbm.at[0, columns_of(dp), pl.ds(third * hid + q * unit, unit)],
            stage.at[q, :, pl.ds(third * unit, unit)],
            st_sem.at[q],
        )

    barrier = pltpu.get_barrier_semaphore()
    for peer in (near, inner_far):
        pl.semaphore_signal(barrier, inc=1, device_id={"expert": peer}, device_id_type=MESH)

    @pl.when(inner)
    def _():
        pl.semaphore_signal(barrier, inc=1, device_id={"expert": outer_far}, device_id_type=MESH)

    beside_dp = [partner] + [xor(chip, c) * 2 + k for c in (1, 2) for k in (0, 1)]
    for peer in beside_dp:
        pl.semaphore_signal(barrier, inc=1, device_id={"dp": peer}, device_id_type=MESH)

    @pl.when(outer)
    def _():
        for q in range(slices):
            for third in range(3):
                stage_copy(q, third).start()

    loads = [
        pltpu.make_async_copy(src, dst, in_sem.at[n])
        for n, (src, dst) in enumerate(
            (
                (route_hbm, route_ref),
                (gate_hbm, gate_ref),
                (tokens_hbm, tokens_ref),
                (out_grad_hbm, out_grad_ref),
            )
        )
    ]
    for load in loads:
        load.start()
    w_copy.start()

    def rows_of(index):
        return pl.ds(index * cap, cap)

    kept = rows_of(3)

    def rows_from(index):
        return pl.ds(pl.multiple_of(index * cap, cap), cap)

    def remote(src, dst, s_sem, r_sem, device):
        return pltpu.make_async_remote_copy(
            src_ref=src,
            dst_ref=dst,
            send_sem=s_sem,
            recv_sem=r_sem,
            device_id=device,
            device_id_type=MESH,
        )

    pl.semaphore_wait(barrier, jnp.where(inner, 3, 2) + len(beside_dp))
    pl.semaphore_signal(
        across, inc=1, device_id={"dp": xor(chip, 1) * 2 + core}, device_id_type=MESH
    )

    def weight_out(q):
        dst = w2_ref.at[q, columns_of(dp)]
        return remote(stage.at[q], dst, w_s, w_r.at[q], {"expert": inner_far})

    @pl.when(outer)
    def _():
        for q in range(slices):
            pltpu.make_async_copy(stage.at[q], stage.at[q], st_sem.at[q]).wait()
            weight_out(q).start()

    row_i = lax.broadcasted_iota(jnp.int32, (tok, tok), 0)
    col_i = lax.broadcasted_iota(jnp.int32, (tok, tok), 1)

    def column(row):
        return jnp.sum(jnp.where(row_i == col_i, row, 0.0), axis=1, keepdims=True)

    loads[0].wait()
    route = route_ref[...]
    block = jnp.where(route == near, 1, jnp.where(route == inner_far, 2, 3))
    route_row = jnp.where(route == me, 0, block).astype(F32)
    route_col = column(route_row)
    same = route_col == route_row
    pos_row = jnp.sum(jnp.where(same & (row_i < col_i), 1.0, 0.0), axis=0, keepdims=True)
    pos_col = jnp.sum(jnp.where(same & (col_i < row_i), 1.0, 0.0), axis=1, keepdims=True)
    slot_row = route_row * cap + pos_row
    slot_col = route_col * cap + pos_col
    slot_at = lax.broadcasted_iota(jnp.int32, (slots, tok), 0).astype(F32)
    table = jnp.where(slot_at == slot_row, 1.0, 0.0).astype(BF16)
    slot_of = lax.broadcasted_iota(jnp.int32, (tok, slots), 1).astype(F32)
    table_t = jnp.where(slot_of == slot_col, 1.0, 0.0).astype(BF16)

    loads[2].wait()
    send_x[...] = jnp.dot(table, tokens_ref[...], preferred_element_type=F32).astype(BF16)
    loads[1].wait()
    loads[3].wait()
    scaled = (column(gate_ref[...]) * out_grad_ref[...].astype(F32)).astype(BF16)
    send_g[...] = jnp.dot(table, scaled, preferred_element_type=F32).astype(BF16)

    def run(is_inner):
        cross_at = 2 if is_inner else 3

        def near_copy(src, dst):
            return remote(
                src.at[rows_of(1)], dst.at[rows_of(1)], to_s, near_r, {"expert": near}
            )

        def cross_copy(src, dst):
            return remote(
                src.at[rows_of(2)],
                dst.at[rows_of(cross_at)],
                to_s,
                cross_r.at[cross_at - 2],
                {"expert": inner_far},
            )

        def bytes_of(ref, s_sem, r_sem):
            return remote(ref, ref, s_sem, r_sem, {"expert": near})

        both = pl.ds(0, 2 * cap)
        x_args = (send_x, recv_x)
        g_args = (send_g, recv_g)

        def return_copy(index):
            peer = {1: near, 2: mirror, 3: outer_far}[index]
            home = rows_of(min(index, 2))
            return remote(
                ret.at[rows_of(index)],
                arrived.at[home],
                rt_s,
                rt_r,
                {"expert": peer},
            )

        first = jnp.where(core == 0, 1, 2)

        def beside(c):
            return xor(chip, c)

        chip_first = jnp.where(core == 0, beside(1), beside(2))
        chip_second = jnp.where(core == 0, beside(2), beside(1))

        def weight_on(q):
            at = w2_ref.at[q, columns_of(dp)]
            return remote(at, at, w_s, w_r.at[q], {"expert": near})

        def spread(c, q):
            at = w2_ref.at[q, columns_of(dp)]
            return remote(at, at, ag_s, ag_r.at[q], {"dp": beside(c) * 2 + core})

        def relay(q):
            at = w2_ref.at[q, columns_of(chip_first * 2 + core)]
            return remote(at, at, ag_s, rl_r.at[q], {"dp": chip_second * 2 + core})

        def hand_over(c, q):
            at = w2_ref.at[q, columns_of(beside(c) * 2 + core)]
            return remote(at, at, pf_s, pf_r.at[q], {"dp": partner})

        def band_copy(j, src, dst):
            peer = lax.rem(dp + j, n_dp)
            return remote(
                src.at[kept, columns_of(peer)], dst.at[rows_from(dp)], bd_s, bd_r, {"dp": peer}
            )

        bands_in = bytes_of(recv_x.at[pl.ds(0, 2 * (n_dp - 1) * cap // n_dp)], bd_s, bd_r)

        def term_copy(c, q):
            at = terms.at[q, rows_from(dp)]
            return remote(at, at, tm_s, tm_r.at[q], {"dp": beside(c) * 2 + core})

        def term_over(c, q):
            at = terms.at[q, rows_from(beside(c) * 2 + core)]
            return remote(at, at, fw_s, fw_r.at[q], {"dp": partner})

        if is_inner:
            near_copy(*x_args).start()
        cross_copy(*x_args).start()
        cross_copy(*g_args).start()
        if not is_inner:
            near_copy(*x_args).start()
            near_copy(*g_args).start()
        pl.semaphore_wait(across, 1)
        for j in range(1, n_dp):
            band_copy(j, send_x, band_x).start()
            band_copy(j, send_g, band_g).start()

        recv_x[rows_of(0)] = send_x[rows_of(0)]
        recv_g[rows_of(0)] = send_g[rows_of(0)]
        band_x[rows_from(dp)] = send_x[kept, columns_of(dp)]
        band_g[rows_from(dp)] = send_g[kept, columns_of(dp)]

        def forward(x, g, weights):
            third = weights.shape[1] // 3
            pre_gate = jnp.dot(x, weights[:, :third], preferred_element_type=F32)
            pre_up = jnp.dot(x, weights[:, third : 2 * third], preferred_element_type=F32)
            grad_hidden = jnp.dot(g, weights[:, 2 * third :], preferred_element_type=F32)
            sig = jax.nn.sigmoid(pre_gate)
            active = pre_gate * sig
            grad_gate = grad_hidden * pre_up * (sig * (1.0 + pre_gate * (1.0 - sig)))
            return (
                grad_gate.astype(BF16),
                (grad_hidden * active).astype(BF16),
                (active * pre_up).astype(BF16),
            )

        def forward_rows(start, size):
            rows = pl.ds(start, size)
            grad_gate, grad_up, kept_hidden = forward(recv_x[rows], recv_g[rows], w_ref)
            pair[rows, :hid] = grad_gate
            pair[rows, hid:] = grad_up
            hidden[rows] = kept_hidden

        def columns(pieces, dst, rows):
            tile = min(512, width)

            @pl.loop(0, width // tile)
            def _(j):
                at = pl.ds(pl.multiple_of(j * tile, tile), tile)
                total = 0.0
                for grads, weights in pieces:
                    total = total + lax.dot_general(
                        grads(), weights(at), (((1,), (1,)), ((), ())), preferred_element_type=F32
                    )
                dst[rows, at] = total.astype(BF16)

        def backward_rows(start, size):
            rows = pl.ds(start, size)
            columns([(lambda: pair[rows], lambda at: w_ref[at, : 2 * hid])], ret, rows)

        contract = (((0,), (0,)), ((), ()))
        mine = rows_from(dp)

        def kept_forward(q):
            grad_gate, grad_up, kept_hidden = forward(send_x[kept], send_g[kept], w2_ref.at[q])
            terms[q, mine, :unit] = grad_gate
            terms[q, mine, unit : 2 * unit] = grad_up
            terms[q, mine, 2 * unit :] = kept_hidden

        def kept_grad(q):
            first = lax.dot_general(
                band_x[...], terms[q, :, : 2 * unit], contract, preferred_element_type=F32
            )
            second = lax.dot_general(
                band_g[...], terms[q, :, 2 * unit :], contract, preferred_element_type=F32
            )
            return grad_scale * jnp.concatenate([first, second], axis=1)

        def near_hop(q):
            return remote(send_d.at[q], near_d.at[q], d_s, d_r.at[q], {"expert": near})

        def far_hop(q):
            return remote(send_d.at[q], far_d.at[q], d_s, d_r.at[q], {"expert": outer_far})

        def take(q):
            weight_on(q).wait_recv()
            if is_inner:
                weight_on(q).start()
            for c in (1, 2):
                spread(c, q).start()
            hand_over(0, q).start()

        def pass_on(q):
            bytes_of(w2_ref.at[q, pl.ds(0, 2 * share)], ag_s, ag_r.at[q]).wait_recv()
            relay(q).start()
            for c in (1, 2):
                hand_over(c, q).start()

        def pass_last(q):
            relay(q).wait_recv()
            hand_over(3, q).start()

        def kept_terms(q):
            bytes_of(w2_ref.at[q, pl.ds(0, 4 * share)], pf_s, pf_r.at[q]).wait_recv()
            kept_forward(q)
            for c in range(1, 4):
                term_copy(c, q).start()
            term_over(0, q).start()

        def pass_terms(q):
            bytes_of(terms.at[q, pl.ds(0, 3 * cap)], tm_s, tm_r.at[q]).wait_recv()
            for c in range(1, 4):
                term_over(c, q).start()

        def kept_band(q):
            if q == 0:
                bands_in.wait_recv()
            bytes_of(terms.at[q, pl.ds(0, 4 * cap)], fw_s, fw_r.at[q]).wait_recv()
            held_d[q] = kept_grad(q)
            if not is_inner:
                send_d[q] = held_d[q].astype(BF16)
                near_hop(q).start()

        def own_rows():
            w_copy.wait()
            forward_rows(0, cap)
            backward_rows(0, cap)
            arrived[rows_of(0)] = ret[rows_of(0)]

        def near_arrival():
            bytes_of(recv_x.at[both], to_s, near_r).wait_recv()

        def cross_arrival(index):
            bytes_of(recv_x.at[both], to_s, cross_r.at[index - 2]).wait_recv()

        def kept_backward():
            pieces = [
                (lambda q=q: terms[q, mine, : 2 * unit], lambda at, q=q: w2_ref[q, at, : 2 * unit])
                for q in range(slices)
            ]
            columns(pieces, arrived, kept)

        def add_hop(q):
            near_hop(q).wait_recv()
            send_d[q] = (held_d[q] + near_d[q].astype(F32)).astype(BF16)
            far_hop(q).start()

        rows_in = slots if is_inner else 2 * cap

        def weight_rows(start, size):
            at = pl.ds(pl.multiple_of(start, size), size)
            part[at, : 2 * hid] = (
                grad_scale
                * lax.dot_general(
                    recv_x[:rows_in, at], pair[:rows_in], contract, preferred_element_type=F32
                )
            ).astype(BF16)
            part[at, 2 * hid :] = (
                grad_scale
                * lax.dot_general(
                    recv_g[:rows_in, at], hidden[:rows_in], contract, preferred_element_type=F32
                )
            ).astype(BF16)

        def band(chip_at, core_at, g):
            return pl.ds(pl.multiple_of((chip_at * 2 + core_at) * share + g * sub, sub), sub)

        bands = [(s, t) for s in range(1, na) for t in list(range(1, nb)) + [0]]
        bands += [(0, t) for t in list(range(1, nb)) + [0]]
        items = [(s, t, g) for s, t in bands for g in range(SUBS)]

        def item_chip(s, t):
            return chip_of(lax.rem(a + s, na), lax.rem(b + t, nb))

        def pair_copy(index, chip_at, g):
            return remote(
                part.at[band(chip_at, 1 - core, g)],
                recv_a.at[pl.ds(pl.multiple_of(chip_at * share + g * sub, sub), sub)],
                a_s,
                a_r.at[index],
                {"dp": partner},
            )

        def partner_chip(s, t):
            if na == nb:
                a_at, b_at = lax.rem(b + s, na), lax.rem(a + t, nb)
                return jnp.where(core == 1, b_at * na + a_at, a_at * na + b_at)
            return item_chip(s, t)

        def item_pair(index):
            s, t, g = items[index]
            return pair_copy(index, partner_chip(s, t), g)

        def item_out(s, t, g):
            at = ((s - 1) * nb + t) * SUBS + g
            to = dp_of(lax.rem(a + s, na), b)
            return remote(send_b.at[at], recv_b.at[at], b_s, b_r.at[at], {"dp": to})

        def item_last(t, g):
            at = (t - 1) * SUBS + g
            to = dp_of(a, lax.rem(b + t, nb))
            return remote(send_c.at[at], recv_c.at[at], c_s, c_r.at[at], {"dp": to})

        def pair_sum(index):
            s, t, g = items[index]
            chip_to = item_chip(s, t)
            item_pair(index).wait_recv()
            return (
                part[band(chip_to, core, g)].astype(F32)
                + recv_a[pl.ds(pl.multiple_of(chip_to * share + g * sub, sub), sub)].astype(F32)
            )

        sent = [index for index, (s, t, g) in enumerate(items) if s > 0]
        rest = [index for index, (s, t, g) in enumerate(items) if s == 0]

        def reduce_pair(which):
            for index in which:
                s, t, g = items[index]
                if g == 0:
                    weight_rows((partner_chip(s, t) * 2 + 1 - core) * share, share)
                item_pair(index).start()

        def reduce_first(which):
            for index in which:
                s, t, g = items[index]
                if g == 0:
                    weight_rows((item_chip(s, t) * 2 + core) * share, share)
                if s > 0:
                    send_b[((s - 1) * nb + t) * SUBS + g] = pair_sum(index).astype(BF16)
                    item_out(s, t, g).start()

        def item_total(index):
            s, t, g = items[index]
            total = pair_sum(index)
            for s_from in range(1, na):
                item_out(s_from, t, g).wait_recv()
                total = total + recv_b[((s_from - 1) * nb + t) * SUBS + g].astype(F32)
            return total

        def reduce_second():
            for index, (s, t, g) in enumerate(items):
                if s == 0 and t > 0:
                    send_c[(t - 1) * SUBS + g] = item_total(index).astype(BF16)
                    item_last(t, g).start()

        def reduce_own():
            for index, (s, t, g) in enumerate(items):
                if s == t == 0:
                    w_grad_ref[0, pl.ds(g * sub, sub)] = item_total(index)
            for t in range(1, nb):
                for g in range(SUBS):
                    item_last(t, g).wait_recv()
                    w_grad_ref[0, pl.ds(g * sub, sub)] += recv_c[(t - 1) * SUBS + g].astype(F32)

        def add_far(q):
            far_hop(q).wait_recv()
            for third in range(3):
                at = pl.ds(third * hid + q * unit, unit)
                w_grad_ref[0, :, at] += far_d[q, :, third * unit : (third + 1) * unit].astype(F32)

        own_rows()
        take(0)
        take(1)
        pass_on(0)
        take(2)
        if is_inner:
            near_copy(*g_args).start()
        pass_on(1)
        pass_last(0)
        kept_terms(0)
        pass_on(2)
        if is_inner:
            pass_last(1)
            kept_terms(1)
            pass_terms(0)
            pass_last(2)
            kept_terms(2)
            cross_arrival(3)
            forward_rows(3 * cap, cap)
            backward_rows(3 * cap, cap)
            return_copy(3).start()
            pass_terms(1)
            pass_terms(2)
            kept_band(0)
            kept_band(1)
            near_arrival()
            cross_arrival(2)
            forward_rows(cap, 2 * cap)
            reduce_pair(sent)
            backward_rows(cap, cap)
            return_copy(1).start()
            reduce_first(sent)
            add_hop(0)
            backward_rows(2 * cap, cap)
            reduce_pair(rest)
            reduce_first(rest)
            add_hop(1)
            kept_band(2)
            reduce_second()
            add_hop(2)
            return_copy(2).start()
            kept_backward()
            reduce_own()
        else:
            near_arrival()
            forward_rows(cap, cap)
            pass_last(1)
            pass_terms(0)
            kept_terms(1)
            kept_band(0)
            pass_last(2)
            reduce_pair(sent)
            kept_terms(2)
            reduce_first(sent)
            pass_terms(1)
            reduce_pair(rest)
            reduce_first(rest)
            kept_band(1)
            pass_terms(2)
            kept_band(2)
            backward_rows(cap, cap)
            return_copy(1).start()
            kept_backward()
            reduce_second()
            reduce_own()
            for q in range(slices - 1):
                add_far(q)

        bytes_of(arrived.at[both], rt_s, rt_r).wait_recv()
        in_grad_ref[...] = jnp.dot(table_t, arrived[...], preferred_element_type=F32).astype(BF16)
        if not is_inner:
            add_far(slices - 1)

        bytes_of(send_x, to_s, near_r).wait_send()
        bands_in.wait_send()
        bytes_of(terms.at[:, pl.ds(0, 3 * cap)], tm_s, tm_r.at[0]).wait_send()
        bytes_of(terms.at[:, pl.ds(0, 4 * cap)], fw_s, fw_r.at[0]).wait_send()
        bytes_of(w2_ref.at[:, pl.ds(0, 3 * share)], ag_s, ag_r.at[0]).wait_send()
        bytes_of(w2_ref.at[:, pl.ds(0, 4 * share)], pf_s, pf_r.at[0]).wait_send()
        bytes_of(stage, w_s, w_r.at[0]).wait_send()
        bytes_of(send_d, d_s, d_r.at[0]).wait_send()
        bytes_of(ret.at[pl.ds(0, (3 if is_inner else 1) * cap)], rt_s, rt_r).wait_send()
        bytes_of(recv_a, a_s, a_r.at[0]).wait_send()
        bytes_of(send_b, b_s, b_r.at[0]).wait_send()
        bytes_of(send_c, c_s, c_r.at[0]).wait_send()

    pl.when(inner)(lambda: run(True))
    pl.when(outer)(lambda: run(False))


def local(n_expert, n_dp, tokens, out_grad, gate_prob, routing, expert_weights):
    tok, width = tokens.shape
    full = expert_weights.shape[2]
    hid = full // 3
    cap = max(16, 2 * tok // n_expert)
    slots = n_expert * cap
    share = width // n_dp
    _, _, _, na, nb = plan(n_expert, n_dp)
    sub = share // SUBS
    chips = na * nb
    n_b, n_c = max(1, (na - 1) * nb) * SUBS, max(1, nb - 1) * SUBS
    dma = pltpu.SemaphoreType.DMA
    vmem = pl.BlockSpec(memory_space=pltpu.VMEM)
    weights, rows = pltpu.VMEM((width, full), BF16), pltpu.VMEM((slots, width), BF16)
    scratch = [weights] + [rows] * 6
    scratch += [
        pltpu.VMEM((slots, 2 * hid), BF16),
        pltpu.VMEM((slots, hid), BF16),
        pltpu.VMEM((width, full), BF16),
        pltpu.VMEM((chips * share, full), BF16),
        pltpu.VMEM((n_b, sub, full), BF16),
        pltpu.VMEM((n_b, sub, full), BF16),
        pltpu.VMEM((n_c, sub, full), BF16),
        pltpu.VMEM((n_c, sub, full), BF16),
    ]
    sems = [dma] + [dma((n_expert,))] * 6 + [dma((chips * SUBS,))] * 2
    sems += [dma((n_b,))] * 2 + [dma((n_c,))] * 2
    kernel, ins = body, [vmem] * 4
    if paired(width, hid, n_expert, n_dp):
        kernel = paired_body
        slices, third = SLICES, full // SLICES
        scratch.insert(1, pltpu.VMEM((slices, width, third), BF16))
        scratch += [pltpu.VMEM((slices, share, third), BF16)]
        scratch += [pltpu.VMEM((n_dp * cap, share), BF16)] * 2
        scratch += [pltpu.VMEM((slices, n_dp * cap, third), BF16)]
        scratch += [pltpu.VMEM((slices, share, third), F32)]
        scratch += [pltpu.VMEM((slices, share, third), BF16)] * 3
        scratch += [pltpu.VMEM((tok, width), BF16)] * 2
        scratch += [pltpu.VMEM((1, tok), F32), pltpu.VMEM((1, tok), jnp.int32)]
        each = dma((slices,))
        sems = [pltpu.SemaphoreType.REGULAR, dma, dma((4,)), each, dma, dma, dma((2,)), dma, dma]
        sems += [dma, dma((chips * SUBS,)), dma, dma((n_b,)), dma, dma((n_c,)), dma, dma]
        sems += [dma, each] * 3 + [dma, each, each] + [dma, each] * 2
        ins = [pl.BlockSpec(memory_space=pl.ANY)] * 4
    early = pl.pallas_call(
        functools.partial(kernel, n_expert, n_dp, cap),
        out_shape=(pltpu.VMEM((tok, width), BF16), pltpu.VMEM((1, share, full), F32)),
        in_specs=ins + [pl.BlockSpec(memory_space=pl.ANY)],
        out_specs=(vmem, vmem),
        scratch_shapes=scratch + sems,
        compiler_params=pltpu.CompilerParams(
            collective_id=0, has_side_effects=True, vmem_limit_bytes=60 * 1024 * 1024
        ),
        name="moe_backward",
    )(tokens, out_grad, gate_prob.reshape(1, tok), routing.reshape(1, tok), expert_weights)
    return pl.pallas_call(
        write_out,
        out_shape=(
            jax.ShapeDtypeStruct((tok, width), BF16),
            jax.ShapeDtypeStruct((1, share, full), F32),
        ),
        in_specs=[vmem] * 2,
        out_specs=(pl.BlockSpec(memory_space=pl.ANY),) * 2,
        scratch_shapes=[dma((2,))],
        name="write_out",
    )(*[pltpu.with_memory_space_constraint(value, pltpu.VMEM) for value in early])


def write_out(in_grad_ref, w_grad_ref, in_grad_out, w_grad_out, sem):
    moves = [
        pltpu.make_async_copy(in_grad_ref, in_grad_out, sem.at[0]),
        pltpu.make_async_copy(w_grad_ref, w_grad_out, sem.at[1]),
    ]
    for move in moves:
        move.start()
    for move in moves:
        move.wait()


def solution(mesh):
    tokens_spec = P(("dp", "expert"), None)
    return jax.shard_map(
        functools.partial(local, mesh.shape["expert"], mesh.shape["dp"]),
        mesh=mesh,
        in_specs=(tokens_spec, tokens_spec, tokens_spec, tokens_spec, P("expert", None, None)),
        out_specs=(tokens_spec, P("expert", "dp", None)),
        check_vma=False,
    )
```

```python
import functools
import math
import jax
import jax.numpy as jnp
from jax import lax
from jax.experimental import pallas as pl
from jax.experimental.pallas import tpu as pltpu
from jax.sharding import PartitionSpec as P

MESH = pl.DeviceIdType.MESH
F32 = jnp.float32
BF16 = jnp.bfloat16
SUBS = 2
SLICES = 3
PIECES = 4


def xor(value, step):
    total, bit = 0, 1
    result = value
    while bit <= step:
        if step & bit:
            result = result + bit - 2 * bit * (lax.rem(lax.div(value, bit), 2))
        bit *= 2
    return result


def plan(n_expert, n_dp):
    half, quarter = n_expert // 2, n_expert // 4
    near = list(range(1, half))
    across = list(range(n_expert - 1, half + quarter - 1, -1))
    last = list(range(half + quarter - 1, half - 1, -1))
    chips = n_dp // 2
    side = math.isqrt(chips)
    while chips % side:
        side -= 1
    return near, across, last, chips // side, side


def body(
    n_expert,
    n_dp,
    cap,
    tokens_ref,
    out_grad_ref,
    gate_ref,
    route_ref,
    w_hbm,
    in_grad_ref,
    w_grad_ref,
    w_ref,
    send_x,
    send_g,
    recv_x,
    recv_g,
    ret,
    arrived,
    pair,
    hidden,
    part,
    recv_a,
    send_b,
    recv_b,
    send_c,
    recv_c,
    w_sem,
    dx_s,
    dx_r,
    dg_s,
    dg_r,
    rt_s,
    rt_r,
    a_s,
    a_r,
    b_s,
    b_r,
    c_s,
    c_r,
):
    near, across, last, na, nb = plan(n_expert, n_dp)
    far = across + last
    me = lax.axis_index("expert")
    dp = lax.axis_index("dp")
    tok, width = tokens_ref.shape
    hid = w_ref.shape[1] // 3
    slots = n_expert * cap
    quarter_rows = slots // 4
    share = width // n_dp
    sub = share // SUBS
    grad_scale = float(tok * n_dp) ** (-0.5)
    core = lax.rem(dp, 2)
    chip = lax.div(dp, 2)
    pos_hi, pos_lo = lax.div(chip, na), lax.rem(chip, na)
    if na == nb:
        a = jnp.where(core == 0, pos_lo, pos_hi)
        b = jnp.where(core == 0, pos_hi, pos_lo)
    else:
        a, b = pos_lo, pos_hi

    def chip_of(a_at, b_at):
        plain = b_at * na + a_at
        if na == nb:
            return jnp.where(core == 0, plain, a_at * na + b_at)
        return plain

    def dp_of(a_at, b_at):
        return chip_of(a_at, b_at) * 2 + core

    w_copy = pltpu.make_async_copy(w_hbm.at[0], w_ref, w_sem)
    w_copy.start()

    barrier = pltpu.get_barrier_semaphore()
    partner = dp + 1 - 2 * core
    greeted = 0
    for k in near + far:
        pl.semaphore_signal(barrier, inc=1, device_id={"expert": xor(me, k)}, device_id_type=MESH)
        greeted += 1
    pl.semaphore_signal(barrier, inc=1, device_id={"dp": partner}, device_id_type=MESH)
    greeted += 1
    for s in range(1, na):
        pl.semaphore_signal(
            barrier, inc=1, device_id={"dp": dp_of(lax.rem(a + s, na), b)}, device_id_type=MESH
        )
        greeted += 1
    for t in range(1, nb):
        pl.semaphore_signal(
            barrier, inc=1, device_id={"dp": dp_of(a, lax.rem(b + t, nb))}, device_id_type=MESH
        )
        greeted += 1

    row_i = lax.broadcasted_iota(jnp.int32, (tok, tok), 0)
    col_i = lax.broadcasted_iota(jnp.int32, (tok, tok), 1)

    def column(row):
        return jnp.sum(jnp.where(row_i == col_i, row, 0.0), axis=1, keepdims=True)

    route_row = route_ref[...].astype(F32)
    route_col = column(route_row)
    same = route_col == route_row
    pos_row = jnp.sum(jnp.where(same & (row_i < col_i), 1.0, 0.0), axis=0, keepdims=True)
    pos_col = jnp.sum(jnp.where(same & (col_i < row_i), 1.0, 0.0), axis=1, keepdims=True)
    slot_row = route_row * cap + pos_row
    slot_col = route_col * cap + pos_col
    slot_at = lax.broadcasted_iota(jnp.int32, (slots, tok), 0).astype(F32)
    table = jnp.where(slot_at == slot_row, 1.0, 0.0).astype(BF16)
    slot_of = lax.broadcasted_iota(jnp.int32, (tok, slots), 1).astype(F32)
    table_t = jnp.where(slot_of == slot_col, 1.0, 0.0).astype(BF16)

    send_x[...] = jnp.dot(table, tokens_ref[...], preferred_element_type=F32).astype(BF16)
    scaled = (column(gate_ref[...]) * out_grad_ref[...].astype(F32)).astype(BF16)
    send_g[...] = jnp.dot(table, scaled, preferred_element_type=F32).astype(BF16)

    def rows_of(index):
        return pl.ds(pl.multiple_of(index * cap, cap), cap)

    pl.semaphore_wait(barrier, greeted)

    def dispatch(k, src, dst, s_sem, r_sem):
        peer = xor(me, k)
        return pltpu.make_async_remote_copy(
            src_ref=src.at[rows_of(peer)],
            dst_ref=dst.at[rows_of(me)],
            send_sem=s_sem.at[k],
            recv_sem=r_sem.at[k],
            device_id={"expert": peer},
            device_id_type=MESH,
        )

    x_copies = {k: dispatch(k, send_x, recv_x, dx_s, dx_r) for k in near + far}
    g_copies = {k: dispatch(k, send_g, recv_g, dg_s, dg_r) for k in near + far}
    returns = {k: dispatch(k, ret, arrived, rt_s, rt_r) for k in near + far}
    for k in near + far:
        x_copies[k].start()
        g_copies[k].start()

    recv_x[rows_of(me)] = send_x[rows_of(me)]
    recv_g[rows_of(me)] = send_g[rows_of(me)]
    w_copy.wait()

    mine = lax.div(me, n_expert // 4)

    def forward(start, size):
        rows = pl.ds(pl.multiple_of(start, cap), size)
        x = recv_x[rows]
        pre_gate = jnp.dot(x, w_ref[:, :hid], preferred_element_type=F32)
        pre_up = jnp.dot(x, w_ref[:, hid : 2 * hid], preferred_element_type=F32)
        grad_hidden = jnp.dot(recv_g[rows], w_ref[:, 2 * hid :], preferred_element_type=F32)
        sig = jax.nn.sigmoid(pre_gate)
        active = pre_gate * sig
        hidden[rows] = (active * pre_up).astype(BF16)
        grad_gate = grad_hidden * pre_up * (sig * (1.0 + pre_gate * (1.0 - sig)))
        pair[rows, :hid] = grad_gate.astype(BF16)
        pair[rows, hid:] = (grad_hidden * active).astype(BF16)

    def backward(start, size):
        rows = pl.ds(pl.multiple_of(start, cap), size)
        tile = min(512, width)

        @pl.loop(0, width // tile)
        def _(j):
            at = pl.ds(pl.multiple_of(j * tile, tile), tile)
            ret[rows, at] = lax.dot_general(
                pair[rows],
                w_ref[at, : 2 * hid],
                (((1,), (1,)), ((), ())),
                preferred_element_type=F32,
            ).astype(BF16)

    near_half = (lax.div(mine, 2) * 2 * quarter_rows, 2 * quarter_rows)
    across_quarter = (xor(mine, 3) * quarter_rows, quarter_rows)
    last_quarter = (xor(mine, 2) * quarter_rows, quarter_rows)
    for k in near:
        x_copies[k].wait_recv()
        g_copies[k].wait_recv()
    forward(*near_half)
    backward(*near_half)
    for k in near:
        returns[k].start()
    arrived[rows_of(me)] = ret[rows_of(me)]
    for k in across:
        x_copies[k].wait_recv()
        g_copies[k].wait_recv()
    forward(*across_quarter)
    backward(*across_quarter)
    for k in last:
        x_copies[k].wait_recv()
        g_copies[k].wait_recv()
    for k in across:
        returns[k].start()
    forward(*last_quarter)

    def weight_rows(start, size):
        at = pl.ds(pl.multiple_of(start, size), size)
        contract = (((0,), (0,)), ((), ()))
        part[at, : 2 * hid] = (
            grad_scale
            * lax.dot_general(recv_x[:, at], pair[...], contract, preferred_element_type=F32)
        ).astype(BF16)
        part[at, 2 * hid :] = (
            grad_scale
            * lax.dot_general(recv_g[:, at], hidden[...], contract, preferred_element_type=F32)
        ).astype(BF16)

    def band(chip_at, core_at, g):
        return pl.ds(pl.multiple_of((chip_at * 2 + core_at) * share + g * sub, sub), sub)

    bands = [(s, t) for s in range(1, na) for t in list(range(1, nb)) + [0]]
    bands += [(0, t) for t in list(range(1, nb)) + [0]]
    items = [(s, t, g) for s, t in bands for g in range(SUBS)]

    def item_chip(s, t):
        return chip_of(lax.rem(a + s, na), lax.rem(b + t, nb))

    banded = share % 128 == 0
    if not banded:

        @pl.loop(0, width // 256)
        def _(j):
            weight_rows(j * 256, 256)

    def pair_copy(index, chip_at, g):
        rows = band(chip_at, 1 - core, g)
        return pltpu.make_async_remote_copy(
            src_ref=part.at[rows],
            dst_ref=recv_a.at[pl.ds(pl.multiple_of(chip_at * share + g * sub, sub), sub)],
            send_sem=a_s.at[index],
            recv_sem=a_r.at[index],
            device_id={"dp": partner},
            device_id_type=MESH,
        )

    def partner_chip(s, t):
        if na == nb:
            a_at, b_at = lax.rem(b + s, na), lax.rem(a + t, nb)
            return jnp.where(core == 1, b_at * na + a_at, a_at * na + b_at)
        return item_chip(s, t)

    a_copies = []
    for index, (s, t, g) in enumerate(items):
        chip_at = partner_chip(s, t)
        if banded and g == 0:
            weight_rows((chip_at * 2 + 1 - core) * share, share)
        copy = pair_copy(index, chip_at, g)
        copy.start()
        a_copies.append(copy)

    backward(*last_quarter)
    for k in last:
        returns[k].start()

    def pair_sum(index, s, t, g):
        chip_at = item_chip(s, t)
        a_copies[index].wait_recv()
        return (
            part[band(chip_at, core, g)].astype(F32)
            + recv_a[pl.ds(pl.multiple_of(chip_at * share + g * sub, sub), sub)].astype(F32)
        )

    if banded:
        for s, t in bands:
            weight_rows((item_chip(s, t) * 2 + core) * share, share)

    b_copies = {}
    for index, (s, t, g) in enumerate(items):
        if s == 0:
            continue
        at = ((s - 1) * nb + t) * SUBS + g
        send_b[at] = pair_sum(index, s, t, g).astype(BF16)
        copy = pltpu.make_async_remote_copy(
            src_ref=send_b.at[at],
            dst_ref=recv_b.at[at],
            send_sem=b_s.at[at],
            recv_sem=b_r.at[at],
            device_id={"dp": dp_of(lax.rem(a + s, na), b)},
            device_id_type=MESH,
        )
        copy.start()
        b_copies[s, t, g] = copy
    c_copies = {}
    for index, (s, t, g) in enumerate(items):
        if s > 0:
            continue
        total = pair_sum(index, s, t, g)
        for s_from in range(1, na):
            b_copies[s_from, t, g].wait_recv()
            total = total + recv_b[((s_from - 1) * nb + t) * SUBS + g].astype(F32)
        if t > 0:
            at = (t - 1) * SUBS + g
            send_c[at] = total.astype(BF16)
            copy = pltpu.make_async_remote_copy(
                src_ref=send_c.at[at],
                dst_ref=recv_c.at[at],
                send_sem=c_s.at[at],
                recv_sem=c_r.at[at],
                device_id={"dp": dp_of(a, lax.rem(b + t, nb))},
                device_id_type=MESH,
            )
            copy.start()
            c_copies[t, g] = copy
        else:
            w_grad_ref[0, pl.ds(g * sub, sub)] = total
    for t in range(1, nb):
        for g in range(SUBS):
            c_copies[t, g].wait_recv()
            w_grad_ref[0, pl.ds(g * sub, sub)] += recv_c[(t - 1) * SUBS + g].astype(F32)

    for k in near + far:
        returns[k].wait_recv()
    in_grad_ref[...] = jnp.dot(table_t, arrived[...], preferred_element_type=F32).astype(BF16)

    for k in near + far:
        x_copies[k].wait_send()
        g_copies[k].wait_send()
        returns[k].wait_send()
    for copy in a_copies + list(b_copies.values()) + list(c_copies.values()):
        copy.wait_send()


def paired(width, hid, n_expert, n_dp):
    chips_a, chips_b = plan(n_expert, n_dp)[3:]
    return n_expert == 4 and chips_a == chips_b == 2 and width % (128 * n_dp) == hid % (128 * SLICES) == 0


def paired_body(
    n_expert,
    n_dp,
    cap,
    tokens_hbm,
    out_grad_hbm,
    gate_hbm,
    route_hbm,
    w_hbm,
    in_grad_ref,
    w_grad_ref,
    w_ref,
    w2_ref,
    send_x,
    send_g,
    recv_x,
    recv_g,
    ret,
    arrived,
    pair,
    hidden,
    part,
    recv_a,
    send_b,
    recv_b,
    send_c,
    recv_c,
    stage,
    band_x,
    band_g,
    terms,
    held_d,
    send_d,
    near_d,
    far_d,
    tokens_ref,
    out_grad_ref,
    gate_ref,
    route_ref,
    across,
    w_sem,
    in_sem,
    st_sem,
    to_s,
    near_r,
    cross_r,
    rt_s,
    rt_r,
    a_s,
    a_r,
    b_s,
    b_r,
    c_s,
    c_r,
    bd_s,
    bd_r,
    tm_s,
    tm_r,
    fw_s,
    fw_r,
    w_s,
    w_r,
    ag_s,
    ag_r,
    rl_r,
    pf_s,
    pf_r,
    d_s,
    d_r,
):
    _, _, _, na, nb = plan(n_expert, n_dp)
    chips = na * nb
    me = lax.axis_index("expert")
    dp = lax.axis_index("dp")
    half = lax.div(me, 2)
    inner = (me == 1) | (me == n_expert - 2)
    outer = jnp.logical_not(inner)
    near = me + 1 - 2 * lax.rem(me, 2)
    mirror = n_expert - 1 - me
    inner_far = 2 - half
    outer_far = 3 - 3 * half
    tok, width = tokens_hbm.shape
    hid = w_ref.shape[1] // 3
    slots = n_expert * cap
    share = width // n_dp
    sub = share // SUBS
    grad_scale = float(tok * n_dp) ** (-0.5)
    core = lax.rem(dp, 2)
    chip = lax.div(dp, 2)
    partner = dp + 1 - 2 * core
    pos_hi, pos_lo = lax.div(chip, na), lax.rem(chip, na)
    if na == nb:
        a = jnp.where(core == 0, pos_lo, pos_hi)
        b = jnp.where(core == 0, pos_hi, pos_lo)
    else:
        a, b = pos_lo, pos_hi

    def chip_of(a_at, b_at):
        plain = b_at * na + a_at
        if na == nb:
            return jnp.where(core == 0, plain, a_at * na + b_at)
        return plain

    def dp_of(a_at, b_at):
        return chip_of(a_at, b_at) * 2 + core

    def columns_of(index):
        return pl.ds(pl.multiple_of(index * share, share), share)

    w_copy = pltpu.make_async_copy(w_hbm.at[0], w_ref, w_sem)
    slices = w2_ref.shape[0]
    unit = hid // slices

    def stage_copy(q, third):
        return pltpu.make_async_copy(
            w_hbm.at[0, columns_of(dp), pl.ds(third * hid + q * unit, unit)],
            stage.at[q, :, pl.ds(third * unit, unit)],
            st_sem.at[q],
        )

    barrier = pltpu.get_barrier_semaphore()
    for peer in (near, inner_far):
        pl.semaphore_signal(barrier, inc=1, device_id={"expert": peer}, device_id_type=MESH)

    @pl.when(inner)
    def _():
        pl.semaphore_signal(barrier, inc=1, device_id={"expert": outer_far}, device_id_type=MESH)

    beside_dp = [partner] + [xor(chip, c) * 2 + k for c in (1, 2) for k in (0, 1)]
    for peer in beside_dp:
        pl.semaphore_signal(barrier, inc=1, device_id={"dp": peer}, device_id_type=MESH)

    @pl.when(outer)
    def _():
        for q in range(slices):
            for third in range(3):
                stage_copy(q, third).start()

    loads = [
        pltpu.make_async_copy(src, dst, in_sem.at[n])
        for n, (src, dst) in enumerate(
            (
                (route_hbm, route_ref),
                (gate_hbm, gate_ref),
                (tokens_hbm, tokens_ref),
                (out_grad_hbm, out_grad_ref),
            )
        )
    ]
    for load in loads:
        load.start()
    w_copy.start()

    def rows_of(index):
        return pl.ds(index * cap, cap)

    kept = rows_of(3)

    def rows_from(index):
        return pl.ds(pl.multiple_of(index * cap, cap), cap)

    def remote(src, dst, s_sem, r_sem, device):
        return pltpu.make_async_remote_copy(
            src_ref=src,
            dst_ref=dst,
            send_sem=s_sem,
            recv_sem=r_sem,
            device_id=device,
            device_id_type=MESH,
        )

    pl.semaphore_wait(barrier, jnp.where(inner, 3, 2) + len(beside_dp))
    pl.semaphore_signal(
        across, inc=1, device_id={"dp": xor(chip, 1) * 2 + core}, device_id_type=MESH
    )

    def weight_out(q):
        dst = w2_ref.at[q, columns_of(dp)]
        return remote(stage.at[q], dst, w_s, w_r.at[q], {"expert": inner_far})

    @pl.when(outer)
    def _():
        for q in range(slices):
            pltpu.make_async_copy(stage.at[q], stage.at[q], st_sem.at[q]).wait()
            weight_out(q).start()

    row_i = lax.broadcasted_iota(jnp.int32, (tok, tok), 0)
    col_i = lax.broadcasted_iota(jnp.int32, (tok, tok), 1)

    def column(row):
        return jnp.sum(jnp.where(row_i == col_i, row, 0.0), axis=1, keepdims=True)

    loads[0].wait()
    route = route_ref[...]
    block = jnp.where(route == near, 1, jnp.where(route == inner_far, 2, 3))
    route_row = jnp.where(route == me, 0, block).astype(F32)
    route_col = column(route_row)
    same = route_col == route_row
    pos_row = jnp.sum(jnp.where(same & (row_i < col_i), 1.0, 0.0), axis=0, keepdims=True)
    pos_col = jnp.sum(jnp.where(same & (col_i < row_i), 1.0, 0.0), axis=1, keepdims=True)
    slot_row = route_row * cap + pos_row
    slot_col = route_col * cap + pos_col
    slot_at = lax.broadcasted_iota(jnp.int32, (slots, tok), 0).astype(F32)
    table = jnp.where(slot_at == slot_row, 1.0, 0.0).astype(BF16)

    loads[2].wait()
    send_x[...] = jnp.dot(table, tokens_ref[...], preferred_element_type=F32).astype(BF16)
    loads[1].wait()
    loads[3].wait()
    scaled = (column(gate_ref[...]) * out_grad_ref[...].astype(F32)).astype(BF16)
    send_g[...] = jnp.dot(table, scaled, preferred_element_type=F32).astype(BF16)

    def run(is_inner):
        cross_at = 2 if is_inner else 3

        def near_copy(src, dst):
            return remote(
                src.at[rows_of(1)], dst.at[rows_of(1)], to_s, near_r, {"expert": near}
            )

        def cross_copy(src, dst):
            return remote(
                src.at[rows_of(2)],
                dst.at[rows_of(cross_at)],
                to_s,
                cross_r.at[cross_at - 2],
                {"expert": inner_far},
            )

        def bytes_of(ref, s_sem, r_sem):
            return remote(ref, ref, s_sem, r_sem, {"expert": near})

        both = pl.ds(0, 2 * cap)
        x_args = (send_x, recv_x)
        g_args = (send_g, recv_g)

        def return_copy(index):
            peer = {1: near, 2: mirror, 3: outer_far}[index]
            home = rows_of(min(index, 2))
            return remote(
                ret.at[rows_of(index)],
                arrived.at[home],
                rt_s,
                rt_r.at[min(index, 2) - 1],
                {"expert": peer},
            )

        first = jnp.where(core == 0, 1, 2)

        def beside(c):
            return xor(chip, c)

        chip_first = jnp.where(core == 0, beside(1), beside(2))
        chip_second = jnp.where(core == 0, beside(2), beside(1))

        def weight_on(q):
            at = w2_ref.at[q, columns_of(dp)]
            return remote(at, at, w_s, w_r.at[q], {"expert": near})

        def spread(c, q):
            at = w2_ref.at[q, columns_of(dp)]
            return remote(at, at, ag_s, ag_r.at[q], {"dp": beside(c) * 2 + core})

        def relay(q):
            at = w2_ref.at[q, columns_of(chip_first * 2 + core)]
            return remote(at, at, ag_s, rl_r.at[q], {"dp": chip_second * 2 + core})

        def hand_over(c, q):
            at = w2_ref.at[q, columns_of(beside(c) * 2 + core)]
            return remote(at, at, pf_s, pf_r.at[q], {"dp": partner})

        def band_copy(j, src, dst):
            peer = lax.rem(dp + j, n_dp)
            return remote(
                src.at[kept, columns_of(peer)], dst.at[rows_from(dp)], bd_s, bd_r, {"dp": peer}
            )

        bands_in = bytes_of(recv_x.at[pl.ds(0, 2 * (n_dp - 1) * cap // n_dp)], bd_s, bd_r)

        def term_copy(c, q):
            at = terms.at[q, rows_from(dp)]
            return remote(at, at, tm_s, tm_r.at[q], {"dp": beside(c) * 2 + core})

        def term_over(c, q):
            at = terms.at[q, rows_from(beside(c) * 2 + core)]
            return remote(at, at, fw_s, fw_r.at[q], {"dp": partner})

        if is_inner:
            near_copy(*x_args).start()
        cross_copy(*x_args).start()
        cross_copy(*g_args).start()
        if not is_inner:
            near_copy(*x_args).start()
            near_copy(*g_args).start()
        pl.semaphore_wait(across, 1)
        for j in range(1, n_dp):
            band_copy(j, send_x, band_x).start()
            band_copy(j, send_g, band_g).start()

        recv_x[rows_of(0)] = send_x[rows_of(0)]
        recv_g[rows_of(0)] = send_g[rows_of(0)]
        band_x[rows_from(dp)] = send_x[kept, columns_of(dp)]
        band_g[rows_from(dp)] = send_g[kept, columns_of(dp)]

        def forward(x, g, weights):
            third = weights.shape[1] // 3
            pre_gate = jnp.dot(x, weights[:, :third], preferred_element_type=F32)
            pre_up = jnp.dot(x, weights[:, third : 2 * third], preferred_element_type=F32)
            grad_hidden = jnp.dot(g, weights[:, 2 * third :], preferred_element_type=F32)
            sig = jax.nn.sigmoid(pre_gate)
            active = pre_gate * sig
            grad_gate = grad_hidden * pre_up * (sig * (1.0 + pre_gate * (1.0 - sig)))
            return (
                grad_gate.astype(BF16),
                (grad_hidden * active).astype(BF16),
                (active * pre_up).astype(BF16),
            )

        def forward_rows(start, size):
            rows = pl.ds(start, size)
            grad_gate, grad_up, kept_hidden = forward(recv_x[rows], recv_g[rows], w_ref)
            pair[rows, :hid] = grad_gate
            pair[rows, hid:] = grad_up
            hidden[rows] = kept_hidden

        def columns(pieces, dst, rows):
            tile = min(512, width)

            @pl.loop(0, width // tile)
            def _(j):
                at = pl.ds(pl.multiple_of(j * tile, tile), tile)
                total = 0.0
                for grads, weights in pieces:
                    total = total + lax.dot_general(
                        grads(), weights(at), (((1,), (1,)), ((), ())), preferred_element_type=F32
                    )
                dst[rows, at] = total.astype(BF16)

        def backward_rows(start, size):
            rows = pl.ds(start, size)
            columns([(lambda: pair[rows], lambda at: w_ref[at, : 2 * hid])], ret, rows)

        contract = (((0,), (0,)), ((), ()))
        mine = rows_from(dp)

        def kept_forward(q):
            grad_gate, grad_up, kept_hidden = forward(send_x[kept], send_g[kept], w2_ref.at[q])
            terms[q, mine, :unit] = grad_gate
            terms[q, mine, unit : 2 * unit] = grad_up
            terms[q, mine, 2 * unit :] = kept_hidden

        def kept_grad(q):
            first = lax.dot_general(
                band_x[...], terms[q, :, : 2 * unit], contract, preferred_element_type=F32
            )
            second = lax.dot_general(
                band_g[...], terms[q, :, 2 * unit :], contract, preferred_element_type=F32
            )
            return grad_scale * jnp.concatenate([first, second], axis=1)

        def near_hop(q):
            return remote(send_d.at[q], near_d.at[q], d_s, d_r.at[q], {"expert": near})

        def far_hop(q):
            return remote(send_d.at[q], far_d.at[q], d_s, d_r.at[q], {"expert": outer_far})

        def take(q):
            weight_on(q).wait_recv()
            if is_inner:
                weight_on(q).start()
            for c in (1, 2):
                spread(c, q).start()
            hand_over(0, q).start()

        def pass_on(q):
            bytes_of(w2_ref.at[q, pl.ds(0, 2 * share)], ag_s, ag_r.at[q]).wait_recv()
            relay(q).start()
            for c in (1, 2):
                hand_over(c, q).start()

        def pass_last(q):
            relay(q).wait_recv()
            hand_over(3, q).start()

        def kept_terms(q):
            bytes_of(w2_ref.at[q, pl.ds(0, 4 * share)], pf_s, pf_r.at[q]).wait_recv()
            kept_forward(q)
            for c in range(1, 4):
                term_copy(c, q).start()
            term_over(0, q).start()

        def pass_terms(q):
            bytes_of(terms.at[q, pl.ds(0, 3 * cap)], tm_s, tm_r.at[q]).wait_recv()
            for c in range(1, 4):
                term_over(c, q).start()

        def kept_band(q):
            if q == 0:
                bands_in.wait_recv()
            bytes_of(terms.at[q, pl.ds(0, 4 * cap)], fw_s, fw_r.at[q]).wait_recv()
            held_d[q] = kept_grad(q)
            if not is_inner:
                send_d[q] = held_d[q].astype(BF16)
                near_hop(q).start()

        def own_rows():
            w_copy.wait()
            forward_rows(0, cap)
            backward_rows(0, cap)
            arrived[rows_of(0)] = ret[rows_of(0)]

        def near_arrival():
            bytes_of(recv_x.at[both], to_s, near_r).wait_recv()

        def cross_arrival(index):
            bytes_of(recv_x.at[both], to_s, cross_r.at[index - 2]).wait_recv()

        def home_rows(start, size):
            at = lax.broadcasted_iota(jnp.int32, (tok, size * cap), 1).astype(F32) + start * cap
            pick = jnp.where(at == slot_col, 1.0, 0.0).astype(BF16)
            rows = arrived[start * cap : (start + size) * cap]
            return jnp.dot(pick, rows, preferred_element_type=F32).astype(BF16)

        def await_home(index):
            bytes_of(arrived.at[rows_of(index)], rt_s, rt_r.at[index - 1]).wait_recv()

        def home_early():
            if is_inner:
                await_home(1)
                in_grad_ref[...] = home_rows(0, 2) + home_rows(3, 1)
            else:
                await_home(2)
                in_grad_ref[...] = home_rows(0, 1) + home_rows(2, 2)

        def kept_backward():
            pieces = [
                (lambda q=q: terms[q, mine, : 2 * unit], lambda at, q=q: w2_ref[q, at, : 2 * unit])
                for q in range(slices)
            ]
            columns(pieces, arrived, kept)

        def add_hop(q):
            near_hop(q).wait_recv()
            send_d[q] = (held_d[q] + near_d[q].astype(F32)).astype(BF16)
            far_hop(q).start()

        rows_in = slots if is_inner else 2 * cap

        def weight_rows(start, size):
            at = pl.ds(pl.multiple_of(start, size), size)
            part[at, : 2 * hid] = (
                grad_scale
                * lax.dot_general(
                    recv_x[:rows_in, at], pair[:rows_in], contract, preferred_element_type=F32
                )
            ).astype(BF16)
            part[at, 2 * hid :] = (
                grad_scale
                * lax.dot_general(
                    recv_g[:rows_in, at], hidden[:rows_in], contract, preferred_element_type=F32
                )
            ).astype(BF16)

        def band(chip_at, core_at, g):
            return pl.ds(pl.multiple_of((chip_at * 2 + core_at) * share + g * sub, sub), sub)

        bands = [(s, t) for s in range(1, na) for t in list(range(1, nb)) + [0]]
        bands += [(0, t) for t in list(range(1, nb)) + [0]]
        items = [(s, t, g) for s, t in bands for g in range(SUBS)]

        def item_chip(s, t):
            return chip_of(lax.rem(a + s, na), lax.rem(b + t, nb))

        def pair_copy(index, chip_at, g):
            return remote(
                part.at[band(chip_at, 1 - core, g)],
                recv_a.at[pl.ds(pl.multiple_of(chip_at * share + g * sub, sub), sub)],
                a_s,
                a_r.at[index],
                {"dp": partner},
            )

        def partner_chip(s, t):
            if na == nb:
                a_at, b_at = lax.rem(b + s, na), lax.rem(a + t, nb)
                return jnp.where(core == 1, b_at * na + a_at, a_at * na + b_at)
            return item_chip(s, t)

        def item_pair(index):
            s, t, g = items[index]
            return pair_copy(index, partner_chip(s, t), g)

        def item_out(s, t, g):
            at = ((s - 1) * nb + t) * SUBS + g
            to = dp_of(lax.rem(a + s, na), b)
            return remote(send_b.at[at], recv_b.at[at], b_s, b_r.at[at], {"dp": to})

        def item_last(t, g):
            at = (t - 1) * SUBS + g
            to = dp_of(a, lax.rem(b + t, nb))
            return remote(send_c.at[at], recv_c.at[at], c_s, c_r.at[at], {"dp": to})

        def pair_sum(index):
            s, t, g = items[index]
            chip_to = item_chip(s, t)
            item_pair(index).wait_recv()
            return (
                part[band(chip_to, core, g)].astype(F32)
                + recv_a[pl.ds(pl.multiple_of(chip_to * share + g * sub, sub), sub)].astype(F32)
            )

        sent = [index for index, (s, t, g) in enumerate(items) if s > 0]
        rest = [index for index, (s, t, g) in enumerate(items) if s == 0]

        def reduce_pair(which):
            for index in which:
                s, t, g = items[index]
                if g == 0:
                    weight_rows((partner_chip(s, t) * 2 + 1 - core) * share, share)
                item_pair(index).start()

        def reduce_first(which):
            for index in which:
                s, t, g = items[index]
                if g == 0:
                    weight_rows((item_chip(s, t) * 2 + core) * share, share)
                if s > 0:
                    send_b[((s - 1) * nb + t) * SUBS + g] = pair_sum(index).astype(BF16)
                    item_out(s, t, g).start()

        def item_total(index):
            s, t, g = items[index]
            total = pair_sum(index)
            for s_from in range(1, na):
                item_out(s_from, t, g).wait_recv()
                total = total + recv_b[((s_from - 1) * nb + t) * SUBS + g].astype(F32)
            return total

        def reduce_second():
            for index, (s, t, g) in enumerate(items):
                if s == 0 and t > 0:
                    send_c[(t - 1) * SUBS + g] = item_total(index).astype(BF16)
                    item_last(t, g).start()

        def reduce_own():
            for index, (s, t, g) in enumerate(items):
                if s == t == 0:
                    w_grad_ref[0, pl.ds(g * sub, sub)] = item_total(index)
            for t in range(1, nb):
                for g in range(SUBS):
                    item_last(t, g).wait_recv()
                    w_grad_ref[0, pl.ds(g * sub, sub)] += recv_c[(t - 1) * SUBS + g].astype(F32)

        def add_far(q):
            far_hop(q).wait_recv()
            for third in range(3):
                at = pl.ds(third * hid + q * unit, unit)
                w_grad_ref[0, :, at] += far_d[q, :, third * unit : (third + 1) * unit].astype(F32)

        own_rows()
        take(0)
        take(1)
        pass_on(0)
        take(2)
        if is_inner:
            near_copy(*g_args).start()
        pass_on(1)
        pass_last(0)
        kept_terms(0)
        pass_on(2)
        if is_inner:
            pass_last(1)
            kept_terms(1)
            pass_terms(0)
            pass_last(2)
            kept_terms(2)
            cross_arrival(3)
            forward_rows(3 * cap, cap)
            backward_rows(3 * cap, cap)
            return_copy(3).start()
            pass_terms(1)
            pass_terms(2)
            kept_band(0)
            kept_band(1)
            near_arrival()
            cross_arrival(2)
            forward_rows(cap, 2 * cap)
            reduce_pair(sent)
            backward_rows(cap, cap)
            return_copy(1).start()
            reduce_first(sent)
            add_hop(0)
            backward_rows(2 * cap, cap)
            reduce_pair(rest)
            reduce_first(rest)
            add_hop(1)
            kept_band(2)
            reduce_second()
            add_hop(2)
            return_copy(2).start()
            kept_backward()
            home_early()
            reduce_own()
        else:
            near_arrival()
            forward_rows(cap, cap)
            pass_last(1)
            pass_terms(0)
            kept_terms(1)
            kept_band(0)
            pass_last(2)
            reduce_pair(sent)
            kept_terms(2)
            reduce_first(sent)
            pass_terms(1)
            reduce_pair(rest)
            reduce_first(rest)
            kept_band(1)
            pass_terms(2)
            kept_band(2)
            backward_rows(cap, cap)
            return_copy(1).start()
            kept_backward()
            reduce_second()
            home_early()
            reduce_own()
            for q in range(slices):
                add_far(q)

        late = 2 if is_inner else 1
        await_home(late)
        in_grad_ref[...] += home_rows(late, 1)

        bytes_of(send_x, to_s, near_r).wait_send()
        bands_in.wait_send()
        bytes_of(terms.at[:, pl.ds(0, 3 * cap)], tm_s, tm_r.at[0]).wait_send()
        bytes_of(terms.at[:, pl.ds(0, 4 * cap)], fw_s, fw_r.at[0]).wait_send()
        bytes_of(w2_ref.at[:, pl.ds(0, 3 * share)], ag_s, ag_r.at[0]).wait_send()
        bytes_of(w2_ref.at[:, pl.ds(0, 4 * share)], pf_s, pf_r.at[0]).wait_send()
        bytes_of(stage, w_s, w_r.at[0]).wait_send()
        bytes_of(send_d, d_s, d_r.at[0]).wait_send()
        bytes_of(ret.at[pl.ds(0, (3 if is_inner else 1) * cap)], rt_s, rt_r.at[0]).wait_send()
        bytes_of(recv_a, a_s, a_r.at[0]).wait_send()
        bytes_of(send_b, b_s, b_r.at[0]).wait_send()
        bytes_of(send_c, c_s, c_r.at[0]).wait_send()

    pl.when(inner)(lambda: run(True))
    pl.when(outer)(lambda: run(False))


def local(n_expert, n_dp, tokens, out_grad, gate_prob, routing, expert_weights):
    tok, width = tokens.shape
    full = expert_weights.shape[2]
    hid = full // 3
    cap = max(16, 2 * tok // n_expert)
    slots = n_expert * cap
    share = width // n_dp
    _, _, _, na, nb = plan(n_expert, n_dp)
    sub = share // SUBS
    chips = na * nb
    n_b, n_c = max(1, (na - 1) * nb) * SUBS, max(1, nb - 1) * SUBS
    dma = pltpu.SemaphoreType.DMA
    vmem = pl.BlockSpec(memory_space=pltpu.VMEM)
    weights, rows = pltpu.VMEM((width, full), BF16), pltpu.VMEM((slots, width), BF16)
    scratch = [weights] + [rows] * 6
    scratch += [
        pltpu.VMEM((slots, 2 * hid), BF16),
        pltpu.VMEM((slots, hid), BF16),
        pltpu.VMEM((width, full), BF16),
        pltpu.VMEM((chips * share, full), BF16),
        pltpu.VMEM((n_b, sub, full), BF16),
        pltpu.VMEM((n_b, sub, full), BF16),
        pltpu.VMEM((n_c, sub, full), BF16),
        pltpu.VMEM((n_c, sub, full), BF16),
    ]
    sems = [dma] + [dma((n_expert,))] * 6 + [dma((chips * SUBS,))] * 2
    sems += [dma((n_b,))] * 2 + [dma((n_c,))] * 2
    kernel, ins = body, [vmem] * 4
    if paired(width, hid, n_expert, n_dp):
        kernel = paired_body
        slices, third = SLICES, full // SLICES
        scratch.insert(1, pltpu.VMEM((slices, width, third), BF16))
        scratch += [pltpu.VMEM((slices, share, third), BF16)]
        scratch += [pltpu.VMEM((n_dp * cap, share), BF16)] * 2
        scratch += [pltpu.VMEM((slices, n_dp * cap, third), BF16)]
        scratch += [pltpu.VMEM((slices, share, third), F32)]
        scratch += [pltpu.VMEM((slices, share, third), BF16)] * 3
        scratch += [pltpu.VMEM((tok, width), BF16)] * 2
        scratch += [pltpu.VMEM((1, tok), F32), pltpu.VMEM((1, tok), jnp.int32)]
        each = dma((slices,))
        sems = [pltpu.SemaphoreType.REGULAR, dma, dma((4,)), each, dma, dma]
        sems += [dma((2,)), dma, dma((2,))]
        sems += [dma, dma((chips * SUBS,)), dma, dma((n_b,)), dma, dma((n_c,)), dma, dma]
        sems += [dma, each] * 3 + [dma, each, each] + [dma, each] * 2
        ins = [pl.BlockSpec(memory_space=pl.ANY)] * 4
    early = pl.pallas_call(
        functools.partial(kernel, n_expert, n_dp, cap),
        out_shape=(pltpu.VMEM((tok, width), BF16), pltpu.VMEM((1, share, full), F32)),
        in_specs=ins + [pl.BlockSpec(memory_space=pl.ANY)],
        out_specs=(vmem, vmem),
        scratch_shapes=scratch + sems,
        compiler_params=pltpu.CompilerParams(
            collective_id=0, has_side_effects=True, vmem_limit_bytes=60 * 1024 * 1024
        ),
        name="moe_backward",
    )(tokens, out_grad, gate_prob.reshape(1, tok), routing.reshape(1, tok), expert_weights)
    return pl.pallas_call(
        write_out,
        out_shape=(
            jax.ShapeDtypeStruct((tok, width), BF16),
            jax.ShapeDtypeStruct((1, share, full), F32),
        ),
        in_specs=[vmem] * 2,
        out_specs=(pl.BlockSpec(memory_space=pl.ANY),) * 2,
        scratch_shapes=[dma((2,))],
        name="write_out",
    )(*[pltpu.with_memory_space_constraint(value, pltpu.VMEM) for value in early])


def write_out(in_grad_ref, w_grad_ref, in_grad_out, w_grad_out, sem):
    moves = [
        pltpu.make_async_copy(in_grad_ref, in_grad_out, sem.at[0]),
        pltpu.make_async_copy(w_grad_ref, w_grad_out, sem.at[1]),
    ]
    for move in moves:
        move.start()
    for move in moves:
        move.wait()


def solution(mesh):
    tokens_spec = P(("dp", "expert"), None)
    return jax.shard_map(
        functools.partial(local, mesh.shape["expert"], mesh.shape["dp"]),
        mesh=mesh,
        in_specs=(tokens_spec, tokens_spec, tokens_spec, tokens_spec, P("expert", None, None)),
        out_specs=(tokens_spec, P("expert", "dp", None)),
        check_vma=False,
    )
```
